512 devices in a mesh: grp: 2 (over y), seq: 128 (over z, x), head: 2 (over core).
Axes of the slice: x: 8, y: 2, z: 16, core: 2. Of those that a mesh axis runs over, the one named last changes fastest.
The devices are a block of a 8x8x16 slice.
Arguments:
- queries: bfloat16 [98304, 768], P(('grp', 'seq'), 'head'), parts along dimension 0, may hold values from -6 to 6
- key_rows: bfloat16 [98304, 768], P(('grp', 'seq'), 'head'), parts along dimension 0, may hold values from -6 to 6
- value_rows: bfloat16 [98304, 768], P(('grp', 'seq'), 'head'), parts along dimension 0, may hold values from -6 to 6
- gate_input: bfloat16 [98304, 768], P(('grp', 'seq'), 'head'), parts along dimension 0, may hold values from -6 to 6
- norm_gain: float32 [768], P('head'), may hold values from 0.5 to 1.5
Outputs:
- retained: bfloat16 [98304, 768], P(('grp', 'seq'), 'head'), parts along dimension 0
- final_state: float32 [256, 6, 128], P(('grp', 'seq'), 'head'), parts along dimension 0
The draws below stay inside these ranges and needn't reach their ends.
There are 2 independent parts, one for each index of `grp`. The reference program is written for one: setup_inputs(seed, part) draws one part's arguments, and reference() takes and returns one part's arrays. A program takes and returns all parts, laid end to end along the dimension named above; an argument that names none is the same for every part. Nothing has to cross between parts.
All inputs are finite; a program needn't handle non-finite values.
Results may differ from the reference program's by a relative error of at most 0.0056.
Values sent between devices are 32-bit elements; how exact they have to be, the bound alone decides.
A program may use at most 128 MiB of HBM per device.

```python
import jax
import jax.numpy as jnp
from jax import lax

ALL_HEADS = 10
HEADS = 6
DH = 128
TOK_DEV = 384
LENGTH = 49152
N_SEQ = 128


def level_of(key, shape, shards, smallest, top_value):
    loudness, own = 1.0, jax.random.fold_in(key, 6)
    for position, blocks in shards:
        steps = jnp.exp(jax.random.uniform(jax.random.fold_in(own, position), (blocks,), jnp.float32, smallest / len(shards), top_value / len(shards)))
        loudness = loudness * jnp.repeat(steps, shape[position] // blocks).reshape([-1 if axis == position else 1 for axis in range(len(shape))])
    return loudness


def normal_values(key, dims, spread, most, pieces=(), kind=jnp.bfloat16):
    values = jax.random.normal(key, dims, jnp.float32) * spread
    if len(pieces) > 0:
        values = level_of(key, dims, pieces, -0.22, 0.18) * values
    return jnp.clip(values, min=-most, max=most).astype(kind)


def setup_inputs(seed: int = 0, part: int = 0) -> dict:
    key_of = jax.random.split(jax.random.key(seed), 6)
    part_splits = jax.random.split(jax.random.fold_in(key_of[5], part), 6)
    queries = normal_values(part_splits[0], (LENGTH, HEADS * DH), 1.0, 6.0, ((0, 128), (1, 2)))
    key_rows = normal_values(part_splits[1], (LENGTH, HEADS * DH), 1.0, 6.0, ((0, 128), (1, 2)))
    value_rows = normal_values(part_splits[2], (LENGTH, HEADS * DH), 1.0, 6.0, ((0, 128), (1, 2)))
    gate_input = normal_values(part_splits[3], (LENGTH, HEADS * DH), 1.0, 6.0, ((0, 128), (1, 2)))
    norm_gain = jnp.clip(1.0 + 0.1 * jax.random.normal(key_of[4], (HEADS * DH,), jnp.float32), 0.5, 1.5)
    return dict(queries=queries, key_rows=key_rows, value_rows=value_rows, gate_input=gate_input, norm_gain=norm_gain)


def reference(queries, key_rows, value_rows, gate_input, norm_gain):
    key_scale = DH ** (-0.5)
    head_ids = (ALL_HEADS - HEADS + jnp.arange(HEADS, dtype=jnp.int32)).astype(jnp.float32)
    log_decay = jnp.log1p(-jnp.exp2(-5.0 - head_ids))
    places = jnp.arange(TOK_DEV, dtype=jnp.float32)
    offsets = places[:, None] - places[None, :]
    causal = offsets >= 0
    decays = jnp.where(causal[None], jnp.exp(jnp.where(causal, offsets, 0.0)[None] * log_decay[:, None, None]), 0.0)
    tail_decay = jnp.exp((TOK_DEV - 1 - places)[:, None] * log_decay[None, :])
    lead_decay = jnp.exp((places + 1)[:, None] * log_decay[None, :])
    block_decay = jnp.exp(TOK_DEV * log_decay)
    gain_split = norm_gain.reshape(HEADS, DH)
    split_shape = (N_SEQ, TOK_DEV, HEADS, DH)
    highest = lax.Precision.HIGHEST

    def block_step(carried, block_data):
        query_split, key_split, value_split, gate_split = block_data
        query_wide = query_split.astype(jnp.float32)
        key_wide = key_split.astype(jnp.float32)
        value_wide = value_split.astype(jnp.float32)
        scores = jnp.einsum('thd,shd->hts', query_wide, key_wide, precision=highest) * key_scale
        weights = lax.optimization_barrier((scores * decays).astype(jnp.bfloat16)).astype(jnp.float32)
        inner_term = jnp.einsum('hts,shd->thd', weights, value_wide, precision=highest)
        keys_decayed = lax.optimization_barrier((key_wide * key_scale * tail_decay[:, :, None]).astype(jnp.bfloat16)).astype(jnp.float32)
        local_state = jnp.einsum('shi,shj->ihj', keys_decayed, value_wide, precision=highest)
        state_low = lax.optimization_barrier(carried.astype(jnp.bfloat16)).astype(jnp.float32)
        outer_term = jnp.einsum('thi,ihj->thj', query_wide, state_low, precision=highest) * lead_decay[:, :, None]
        mixture = inner_term + outer_term
        centred = mixture - lax.optimization_barrier(jnp.mean(mixture, axis=-1, keepdims=True))
        variance = lax.optimization_barrier(jnp.mean(centred * centred, axis=-1, keepdims=True))
        normed = centred * lax.rsqrt(variance + 1e-05) * gain_split
        result = (normed * jax.nn.silu(gate_split.astype(jnp.float32))).astype(jnp.bfloat16)
        updated = block_decay[None, :, None] * carried + local_state
        return (updated, result.reshape(TOK_DEV, HEADS * DH))
    initial = jnp.zeros((DH, HEADS, DH), jnp.float32)
    blocks = (queries.reshape(split_shape), key_rows.reshape(split_shape), value_rows.reshape(split_shape), gate_input.reshape(split_shape))
    final_state, outputs = lax.scan(block_step, initial, blocks)
    return (outputs.reshape(N_SEQ * TOK_DEV, HEADS * DH), final_state)
```

```python
import functools
import math

import jax
import jax.numpy as jnp
import numpy as np
from jax import lax
from jax.experimental import pallas as pl
from jax.experimental.pallas import tpu as pltpu
from jax.sharding import PartitionSpec as P

ALL_HEADS = 10
HEADS = 6
DH = 128
NX = 8
MESH = pl.DeviceIdType.MESH
F32 = jnp.float32
BF16 = jnp.bfloat16
SUB = 128


def log_decays(shards):
    per = HEADS // shards
    ids = ALL_HEADS - HEADS + np.arange(HEADS, dtype=np.float64)
    table = np.log1p(-np.exp2(-5.0 - ids)).reshape(shards, per)
    return [[float(np.float32(v)) for v in row] for row in table]


def kernel(
    table, nz,
    q_hbm, k_hbm, v_hbm, g_hbm, gain_ref,
    out_hbm, fin_ref,
    q_v, k_v, v_v, g_v, out_v,
    st, sx, rx, xp, rtot, rz, win, rw, cb, rc, carr, inner, gs, fs, fr,
    load_sem, store_sem, xs_sem, xr_sem, as_sem, ar_sem, ws_sem, wr_sem, bs_sem, br_sem, fs_sem, fr_sem, relay,
):
    tokens = q_v.shape[0]
    nh = q_v.shape[1] // DH
    rows = DH // NX
    nb = tokens // SUB
    scale = DH ** (-0.5)
    me = lax.axis_index("seq")
    z = lax.div(me, NX)
    x = lax.rem(me, NX)
    hd = lax.axis_index("head")

    lds = []
    for h in range(nh):
        ld = jnp.float32(table[0][h])
        for s in range(1, len(table)):
            ld = jnp.where(hd == s, jnp.float32(table[s][h]), ld)
        lds.append(ld)

    def at(zz, xx):
        return {"seq": zz * NX + xx}

    def zwrap(d):
        return lax.rem(z + (d % nz), nz)

    def xwrap(d):
        return lax.rem(x + (d % NX), NX)

    def load(src, dst, i, h):
        cols = pl.ds(h * DH, DH)
        return pltpu.make_async_copy(src.at[:, cols], dst.at[:, cols], load_sem.at[i, h])

    for h in range(nh):
        load(k_hbm, k_v, 0, h).start()
        load(v_hbm, v_v, 1, h).start()
    for h in range(nh):
        load(q_hbm, q_v, 2, h).start()
        load(g_hbm, g_v, 3, h).start()

    barrier = pltpu.get_barrier_semaphore()
    for d in range(1, NX):
        pl.semaphore_signal(barrier, inc=1, device_id=at(z, xwrap(d)), device_id_type=MESH)
    near = (1, -1, 2, -2, 3, -3)
    for d in near:
        pl.semaphore_signal(barrier, inc=1, device_id=at(zwrap(d), x), device_id_type=MESH)

    zero = jnp.zeros((nh, rows, DH), F32)

    @pl.when(z < 2)
    def _():
        rz[:, 0] = zero

    @pl.when(z < 1)
    def _():
        rz[:, 1] = zero

    @pl.when(z != 3)
    def _():
        rz[:, 3] = zero

    for j in range(4):
        @pl.when(z < 2 + 4 * j)
        def _(j=j):
            rw[:, j] = zero

    def r_iota(n):
        return lax.broadcasted_iota(jnp.int32, (n, DH), 0).astype(F32)

    def x_copy(h, d):
        to = xwrap(d)
        return pltpu.make_async_remote_copy(
            sx.at[h, to], rx.at[h, x], xs_sem.at[h, d], xr_sem.at[h, d],
            device_id=at(z, to), device_id_type=MESH)

    def x_wait(h, d):
        src = xwrap(-d)
        return pltpu.make_async_remote_copy(
            sx.at[h, src], rx.at[h, src], xs_sem.at[h, d], xr_sem.at[h, d],
            device_id=at(z, src), device_id_type=MESH)

    def b_copy(h, d):
        to = xwrap(d)
        return pltpu.make_async_remote_copy(
            cb.at[h, to], rc.at[h, x], bs_sem.at[h, d], br_sem.at[h, d],
            device_id=at(z, to), device_id_type=MESH)

    def b_wait(h, d):
        src = xwrap(-d)
        return pltpu.make_async_remote_copy(
            cb.at[h, src], rc.at[h, src], bs_sem.at[h, d], br_sem.at[h, d],
            device_id=at(z, src), device_id_type=MESH)

    last_c = nz - 3
    raw = (
        (0, 2, z <= last_c - 2),
        (3, 3, z == 0),
        (1, 1, z <= last_c - 1),
        (2, -1, (z >= 1) & (z <= last_c + 1)),
    )
    raw_in = ((0, (z >= 2) & (z <= last_c)), (3, z == 3), (1, (z >= 1) & (z <= last_c)), (2, z <= last_c))

    def a_copy(h, slot, d):
        return pltpu.make_async_remote_copy(
            rtot.at[h], rz.at[h, slot], as_sem.at[h, slot], ar_sem.at[h, slot],
            device_id=at(zwrap(d), x), device_id_type=MESH)

    def w_copy(h, j):
        return pltpu.make_async_remote_copy(
            win.at[h], rw.at[h, j], ws_sem.at[h, j], wr_sem.at[h, j],
            device_id=at(zwrap(2 + 4 * j), x), device_id_type=MESH)

    def f_copy(zz):
        return pltpu.make_async_remote_copy(
            fs.at[zz], fr, fs_sem.at[zz], fr_sem,
            device_id=at(zz, x), device_id_type=MESH)

    far = (4, 3, 5, 2, 6, 1, 7)

    for h in range(nh):
        cols = pl.ds(h * DH, DH)
        tail = jnp.exp((tokens - 1 - r_iota(tokens)) * lds[h])
        load(k_hbm, k_v, 0, h).wait()
        load(v_hbm, v_v, 1, h).wait()
        kd = (k_v[:, cols].astype(F32) * scale * tail).astype(BF16)
        st[h] = lax.dot_general(kd, v_v[:, cols], (((0,), (0,)), ((), ())), preferred_element_type=F32)
        for xx in range(NX):
            sx[h, xx] = st[h, pl.ds(xx, rows, stride=NX), :]
        if h == 0:
            pl.semaphore_wait(barrier, NX - 1 + len(near))
        for d in far:
            x_copy(h, d).start()
        rx[h, x] = sx[h, x]
        if h == 0:
            for d in (3, -3):
                pl.semaphore_signal(relay, inc=1, device_id=at(zwrap(d), x), device_id_type=MESH)

    ri = lax.broadcasted_iota(jnp.int32, (SUB, SUB), 0)
    ci = lax.broadcasted_iota(jnp.int32, (SUB, SUB), 1)

    def inner_of(h):
        cols = pl.ds(h * DH, DH)
        load(q_hbm, q_v, 2, h).wait()
        base = jnp.exp((ri - ci).astype(F32) * lds[h]) * scale
        diag = jnp.where(ri >= ci, base, 0.0)
        for i in range(nb):
            qi = q_v[pl.ds(i * SUB, SUB), cols]
            parts = []
            for j in range(i + 1):
                s = lax.dot_general(qi, k_v[pl.ds(j * SUB, SUB), cols], (((1,), (1,)), ((), ())),
                                    preferred_element_type=F32)
                if j == i:
                    w = jnp.where(ri >= ci, s * diag, 0.0)
                else:
                    w = s * (base * jnp.exp(lds[h] * float((i - j) * SUB)))
                parts.append(w.astype(BF16))
            w = parts[0] if i == 0 else jnp.concatenate(parts, axis=1)
            inner[h, pl.ds(i * SUB, SUB), :] = jnp.dot(
                w, v_v[pl.ds(0, (i + 1) * SUB), cols], preferred_element_type=F32)

    def gate_of(h):
        cols = pl.ds(h * DH, DH)
        load(g_hbm, g_v, 3, h).wait()
        gain = gain_ref[:, cols]
        u = g_v[:, cols].astype(F32)
        gs[h] = u / (1.0 + jnp.exp(-u)) * gain

    inner_of(0)

    for h in range(nh):
        d1 = jnp.exp(lds[h] * float(tokens))
        for d in far:
            x_wait(h, d).wait_recv()
        acc = rx[h, 0]
        for xx in range(1, NX):
            xp[h, xx] = acc
            acc = acc * d1 + rx[h, xx]
        rtot[h] = acc
        for slot, d, ok in raw:
            @pl.when(ok)
            def _(slot=slot, d=d, h=h):
                a_copy(h, slot, d).start()

    inner_of(1)

    pl.semaphore_wait(relay, 2)

    @pl.when(z <= last_c)
    def _():
        for h in range(nh):
            dd = [jnp.exp(lds[h] * float(tokens * NX * k)) for k in range(5)]
            for slot, ok in raw_in:
                @pl.when(ok)
                def _(slot=slot, h=h):
                    a_copy(h, slot, 0).wait_recv()
            win[h] = (rz[h, 2] + dd[1] * rtot[h] + dd[2] * rz[h, 1]
                      + dd[3] * rz[h, 0] + dd[4] * rz[h, 3])
            for j in (1, 2, 3, 0):
                @pl.when(z + 2 + 4 * j < nz)
                def _(j=j, h=h):
                    w_copy(h, j).start()

    inner_of(2)
    for h in range(nh):
        gate_of(h)

    for h in range(nh):
        for j in range(4):
            @pl.when(z >= 2 + 4 * j)
            def _(j=j, h=h):
                w_copy(h, j).wait_recv()

        @pl.when(z == 1)
        def _(h=h):
            rw[h, 0] = rz[h, 1]
        ee = rw[h, 0]
        for j in range(1, 4):
            ee = ee + rw[h, j] * jnp.exp(lds[h] * float(tokens * NX * 4 * j))
        cb[h, 0] = ee
        for xx in range(1, NX):
            cb[h, xx] = xp[h, xx] + ee * jnp.exp(lds[h] * float(tokens * xx))
        for d in far:
            b_copy(h, d).start()
        rc[h, x] = cb[h, x]

        @pl.when(z == nz - 1)
        def _(h=h, ee=ee):
            fs[:, h, :] = ee * jnp.exp(lds[h] * float(tokens * NX)) + rtot[h]

    @pl.when(z == nz - 1)
    def _():
        for zz in range(nz - 1):
            f_copy(zz).start()
        fin_ref[0] = fs[nz - 1]

    for h in range(nh):
        cols = pl.ds(h * DH, DH)
        lead = jnp.exp((r_iota(SUB) + 1.0) * lds[h])
        for d in far:
            b_wait(h, d).wait_recv()
        for xx in range(NX):
            carr[h, pl.ds(xx, rows, stride=NX), :] = rc[h, xx]
        low = carr[h].astype(BF16)
        for i in range(nb):
            rs = pl.ds(i * SUB, SUB)
            o = jnp.dot(q_v[rs, cols], low, preferred_element_type=F32)
            mix = inner[h, rs, :] + o * (lead * jnp.exp(lds[h] * float(i * SUB)))
            mean = jnp.sum(mix, axis=1, keepdims=True) * (1.0 / DH)
            cen = mix - mean
            var = jnp.sum(cen * cen, axis=1, keepdims=True) * (1.0 / DH)
            out_v[rs, cols] = (cen * lax.rsqrt(var + 1e-05) * gs[h, rs, :]).astype(BF16)
        pltpu.make_async_copy(out_v.at[:, cols], out_hbm.at[:, cols], store_sem.at[h]).start()

    @pl.when(z < nz - 1)
    def _():
        f_copy(0).wait_recv()
        fin_ref[0] = fr[...]

    @pl.when(z == nz - 1)
    def _():
        for zz in range(nz - 1):
            f_copy(zz).wait_send()

    for h in range(nh):
        for d in far:
            x_copy(h, d).wait_send()
            b_copy(h, d).wait_send()
        for slot, d, ok in raw:
            @pl.when(ok)
            def _(slot=slot, d=d, h=h):
                a_copy(h, slot, d).wait_send()
        for j in range(4):
            @pl.when((z <= last_c) & (z + 2 + 4 * j < nz))
            def _(j=j, h=h):
                w_copy(h, j).wait_send()
        cols = pl.ds(h * DH, DH)
        pltpu.make_async_copy(out_v.at[:, cols], out_hbm.at[:, cols], store_sem.at[h]).wait()


def body(table, nz, queries, key_rows, value_rows, gate_input, norm_gain):
    tokens, width = queries.shape
    nh = width // DH
    rows = DH // NX
    anyspace = pl.BlockSpec(memory_space=pl.ANY)
    vmem = pl.BlockSpec(memory_space=pltpu.VMEM)
    dma = pltpu.SemaphoreType.DMA
    wide = pltpu.VMEM((tokens, width), BF16)
    eight = pltpu.VMEM((nh, NX, rows, DH), F32)
    four = pltpu.VMEM((nh, 4, rows, DH), F32)
    one = pltpu.VMEM((nh, rows, DH), F32)
    square = pltpu.VMEM((nh, DH, DH), F32)
    tall = pltpu.VMEM((nh, tokens, DH), F32)
    return pl.pallas_call(
        functools.partial(kernel, table, nz),
        out_shape=(
            jax.ShapeDtypeStruct((tokens, width), BF16),
            jax.ShapeDtypeStruct((1, nh, DH), F32),
        ),
        in_specs=[anyspace, anyspace, anyspace, anyspace, vmem],
        out_specs=(anyspace, vmem),
        scratch_shapes=[
            wide, wide, wide, wide, wide,
            square, eight, eight, eight, one, four, one, four, eight, eight, square, tall, tall,
            pltpu.VMEM((nz, nh, DH), F32), pltpu.VMEM((nh, DH), F32),
            dma((4, nh)), dma((nh,)), dma((nh, NX)), dma((nh, NX)), dma((nh, 4)), dma((nh, 4)),
            dma((nh, 4)), dma((nh, 4)), dma((nh, NX)), dma((nh, NX)), dma((nz,)), dma,
            pltpu.SemaphoreType.REGULAR,
        ],
        compiler_params=pltpu.CompilerParams(collective_id=0, has_side_effects=True),
        name="retention",
    )(queries, key_rows, value_rows, gate_input, norm_gain.reshape(1, width))


def solution(mesh):
    table = log_decays(mesh.shape["head"])
    rows = ("grp", "seq")
    placed = (P(rows, "head"),) * 4 + (P("head"),)
    return jax.shard_map(
        functools.partial(body, table, mesh.shape["seq"] // NX),
        mesh=mesh,
        in_specs=placed,
        out_specs=(P(rows, "head"), P(rows, "head", None)),
        check_vma=False,
    )
```

```python
import functools
import math

import jax
import jax.numpy as jnp
import numpy as np
from jax import lax
from jax.experimental import pallas as pl
from jax.experimental.pallas import tpu as pltpu
from jax.sharding import PartitionSpec as P

ALL_HEADS = 10
HEADS = 6
DH = 128
NX = 8
MESH = pl.DeviceIdType.MESH
F32 = jnp.float32
BF16 = jnp.bfloat16
SUB = 128


def log_decays(shards):
    per = HEADS // shards
    ids = ALL_HEADS - HEADS + np.arange(HEADS, dtype=np.float64)
    table = np.log1p(-np.exp2(-5.0 - ids)).reshape(shards, per)
    return [[float(np.float32(v)) for v in row] for row in table]


def kernel(
    table, nz,
    q_hbm, k_hbm, v_hbm, g_hbm, gain_hbm,
    out_ref, fin_ref,
    q_v, k_v, v_v, g_v, gain_v,
    st, sx, rx, xp, rtot, rz, win, rw, cb, rc, carr, inner, gs, fs, fr,
    load_sem, gain_sem, xs_sem, xr_sem, as_sem, ar_sem, ws_sem, wr_sem, bs_sem, br_sem, fs_sem, fr_sem, ready,
):
    tokens = q_v.shape[0]
    nh = q_v.shape[1] // DH
    rows = DH // NX
    nb = tokens // SUB
    scale = DH ** (-0.5)
    me = lax.axis_index("seq")
    z = lax.div(me, NX)
    x = lax.rem(me, NX)
    hd = lax.axis_index("head")
    last_c = nz - 3

    lds = []
    for h in range(nh):
        ld = jnp.float32(table[0][h])
        for s in range(1, len(table)):
            ld = jnp.where(hd == s, jnp.float32(table[s][h]), ld)
        lds.append(ld)

    def at(zz, xx):
        return {"seq": zz * NX + xx}

    def xwrap(d):
        return lax.rem(x + (d % NX), NX)

    def load(src, dst, i, h):
        cols = pl.ds(h * DH, DH)
        return pltpu.make_async_copy(src.at[:, cols], dst.at[:, cols], load_sem.at[i, h])

    def gain_load():
        return pltpu.make_async_copy(gain_hbm, gain_v, gain_sem)

    for h in range(nh):
        load(k_hbm, k_v, 0, h).start()
        load(v_hbm, v_v, 1, h).start()

    barrier = pltpu.get_barrier_semaphore()
    for d in range(1, NX):
        pl.semaphore_signal(barrier, inc=1, device_id=at(z, xwrap(d)), device_id_type=MESH)
    for zz in range(1, nz):
        @pl.when(z < zz)
        def _(zz=zz):
            pl.semaphore_signal(barrier, inc=1, device_id=at(zz, x), device_id_type=MESH)

    for h in range(nh):
        load(q_hbm, q_v, 2, h).start()
        load(g_hbm, g_v, 3, h).start()
    gain_load().start()

    zero = jnp.zeros((nh, rows, DH), F32)

    @pl.when(z < 2)
    def _():
        rz[:, 0] = zero

    @pl.when(z < 1)
    def _():
        rz[:, 1] = zero

    @pl.when(z != 3)
    def _():
        rz[:, 3] = zero

    for j in range(4):
        @pl.when(z < 2 + 4 * j)
        def _(j=j):
            rw[:, j] = zero

    for zz in range(nz):
        @pl.when(zz <= z)
        def _(zz=zz):
            fr[zz] = jnp.zeros((nh, DH), F32)

    def r_iota(n):
        return lax.broadcasted_iota(jnp.int32, (n, DH), 0).astype(F32)

    def x_copy(h, d):
        to = xwrap(d)
        return pltpu.make_async_remote_copy(
            sx.at[h, to], rx.at[h, x], xs_sem.at[h, d], xr_sem.at[h, d],
            device_id=at(z, to), device_id_type=MESH)

    def x_wait(h, d):
        src = xwrap(-d)
        return pltpu.make_async_remote_copy(
            sx.at[h, src], rx.at[h, src], xs_sem.at[h, d], xr_sem.at[h, d],
            device_id=at(z, src), device_id_type=MESH)

    def b_copy(h, d):
        to = xwrap(d)
        return pltpu.make_async_remote_copy(
            cb.at[h, to], rc.at[h, x], bs_sem.at[h, d], br_sem.at[h, d],
            device_id=at(z, to), device_id_type=MESH)

    def b_wait(h, d):
        src = xwrap(-d)
        return pltpu.make_async_remote_copy(
            cb.at[h, src], rc.at[h, src], bs_sem.at[h, d], br_sem.at[h, d],
            device_id=at(z, src), device_id_type=MESH)

    raw = (
        (2, -1, (z >= 1) & (z <= last_c + 1)),
        (1, 1, z <= last_c - 1),
        (0, 2, z <= last_c - 2),
        (3, 3, z == 0),
    )
    raw_in = ((0, (z >= 2) & (z <= last_c)), (3, z == 3), (1, (z >= 1) & (z <= last_c)), (2, z <= last_c))

    def a_copy(h, slot, d):
        return pltpu.make_async_remote_copy(
            rtot.at[h], rz.at[h, slot], as_sem.at[h, slot], ar_sem.at[h, slot],
            device_id=at(z + d, x), device_id_type=MESH)

    def w_copy(h, j):
        return pltpu.make_async_remote_copy(
            win.at[h], rw.at[h, j], ws_sem.at[h, j], wr_sem.at[h, j],
            device_id=at(z + (2 + 4 * j), x), device_id_type=MESH)

    def f_copy(zz):
        return pltpu.make_async_remote_copy(
            fs.at[zz], fr.at[z], fs_sem.at[zz], fr_sem.at[z],
            device_id=at(zz, x), device_id_type=MESH)

    def f_wait(zz):
        return pltpu.make_async_remote_copy(
            fs.at[zz], fr.at[zz], fs_sem.at[zz], fr_sem.at[zz],
            device_id=at(zz, x), device_id_type=MESH)

    readies = ((1, (z >= 1) & (z <= last_c)), (2, z >= 2), (3, z == 3)) + tuple(
        (2 + 4 * j, z >= 2 + 4 * j) for j in range(1, 4))
    slot_of = {d: i for i, (d, _) in enumerate(readies)}

    def ready_wait(d):
        pl.semaphore_wait(ready.at[slot_of[d]], 1)

    far = (4, 3, 5, 2, 6, 1, 7)

    for h in range(nh):
        cols = pl.ds(h * DH, DH)
        tail = jnp.exp((tokens - 1 - r_iota(tokens)) * lds[h]) * scale
        with jax.named_scope(f"load{h}"):
            load(k_hbm, k_v, 0, h).wait()
            load(v_hbm, v_v, 1, h).wait()
        with jax.named_scope(f"state{h}"):
            kd = (k_v[:, cols].astype(F32) * tail).astype(BF16)
            st[h] = lax.dot_general(kd, v_v[:, cols], (((0,), (0,)), ((), ())), preferred_element_type=F32)
            for xx in range(NX):
                sx[h, xx] = st[h, pl.ds(xx, rows, stride=NX), :]
        if h == 0:
            with jax.named_scope("barrier"):
                pl.semaphore_wait(barrier, NX - 1 + z)
        for d in far:
            x_copy(h, d).start()
        rx[h, x] = sx[h, x]
    for d, ok in readies:
        @pl.when(ok)
        def _(d=d):
            pl.semaphore_signal(ready.at[slot_of[d]], inc=1, device_id=at(z - d, x), device_id_type=MESH)

    ri = lax.broadcasted_iota(jnp.int32, (SUB, SUB), 0)
    ci = lax.broadcasted_iota(jnp.int32, (SUB, SUB), 1)

    def inner_of(h):
        cols = pl.ds(h * DH, DH)
        load(q_hbm, q_v, 2, h).wait()
        base = jnp.exp((ri - ci).astype(F32) * lds[h]) * scale
        for i in range(nb):
            qi = q_v[pl.ds(i * SUB, SUB), cols]
            parts = []
            for j in range(i + 1):
                s = lax.dot_general(qi, k_v[pl.ds(j * SUB, SUB), cols], (((1,), (1,)), ((), ())),
                                    preferred_element_type=F32)
                if j == i:
                    w = jnp.where(ri >= ci, s * base, 0.0)
                else:
                    w = s * (base * jnp.exp(lds[h] * float((i - j) * SUB)))
                parts.append(w.astype(BF16))
            w = parts[0] if i == 0 else jnp.concatenate(parts, axis=1)
            inner[h, pl.ds(i * SUB, SUB), :] = jnp.dot(
                w, v_v[pl.ds(0, (i + 1) * SUB), cols], preferred_element_type=F32)

    def gate_of(h):
        cols = pl.ds(h * DH, DH)
        load(g_hbm, g_v, 3, h).wait()
        gain = gain_v[pl.ds(h * DH, DH)].reshape(1, DH)
        u = g_v[:, cols].astype(F32)
        gs[h] = u / (1.0 + jnp.exp(-u)) * gain

    def local_work():
        with jax.named_scope("local"):
            gain_load().wait()
            for h in range(nh):
                inner_of(h)
                gate_of(h)

    for h in range(nh):
        d1 = jnp.exp(lds[h] * float(tokens))
        with jax.named_scope(f"xwait{h}"):
            for d in far:
                x_wait(h, d).wait_recv()
        with jax.named_scope(f"prefix{h}"):
            acc = rx[h, 0]
            for xx in range(1, NX):
                xp[h, xx] = acc
                acc = acc * d1 + rx[h, xx]
            rtot[h] = acc
            fs[:, h, :] = acc * jnp.exp((nz - 1 - z).astype(F32) * (lds[h] * float(tokens * NX)))

    for zz in range(nz - 1):
        @pl.when(z > zz)
        def _(zz=zz):
            f_copy(zz).start()
    for slot, d, ok in raw:
        @pl.when(ok)
        def _(slot=slot, d=d):
            if d > 0:
                ready_wait(d)
            for h in range(nh):
                a_copy(h, slot, d).start()

    early = (z >= 1) & (z < nz // 2)

    @pl.when(early)
    def _():
        local_work()

    @pl.when(z <= last_c)
    def _():
        with jax.named_scope("windows"):
            @pl.when(z > last_c - 2)
            def _():
                ready_wait(2)
            for h in range(nh):
                dd = [jnp.exp(lds[h] * float(tokens * NX * k)) for k in range(5)]
                for slot, ok in raw_in:
                    @pl.when(ok)
                    def _(slot=slot, h=h):
                        pltpu.make_async_remote_copy(
                            rtot.at[h], rz.at[h, slot], as_sem.at[h, slot], ar_sem.at[h, slot],
                            device_id=at(z, x), device_id_type=MESH).wait_recv()
                win[h] = (rz[h, 2] + dd[1] * rtot[h] + dd[2] * rz[h, 1]
                          + dd[3] * rz[h, 0] + dd[4] * rz[h, 3])
                w_copy(h, 0).start()

    for h in range(nh):
        with jax.named_scope(f"wwait{h}"):
            for j in range(4):
                @pl.when(z >= 2 + 4 * j)
                def _(j=j, h=h):
                    pltpu.make_async_remote_copy(
                        win.at[h], rw.at[h, j], ws_sem.at[h, j], wr_sem.at[h, j],
                        device_id=at(z, x), device_id_type=MESH).wait_recv()

            @pl.when(z == 1)
            def _(h=h):
                rw[h, 0] = rz[h, 1]
        ee = rw[h, 0]
        for j in range(1, 4):
            ee = ee + rw[h, j] * jnp.exp(lds[h] * float(tokens * NX * 4 * j))
        cb[h, 0] = ee
        for xx in range(1, NX):
            cb[h, xx] = xp[h, xx] + ee * jnp.exp(lds[h] * float(tokens * xx))
        for d in far:
            b_copy(h, d).start()
        rc[h, x] = cb[h, x]

    @pl.when(jnp.logical_not(early))
    def _():
        local_work()

    for h in range(nh):
        cols = pl.ds(h * DH, DH)
        lead = jnp.exp((r_iota(SUB) + 1.0) * lds[h])
        with jax.named_scope(f"bwait{h}"):
            for d in far:
                b_wait(h, d).wait_recv()
        with jax.named_scope(f"outer{h}"):
            for xx in range(NX):
                carr[h, pl.ds(xx, rows, stride=NX), :] = rc[h, xx]
            low = carr[h].astype(BF16)
            for i in range(nb):
                rs = pl.ds(i * SUB, SUB)
                o = jnp.dot(q_v[rs, cols], low, preferred_element_type=F32)
                mix = inner[h, rs, :] + o * (lead * jnp.exp(lds[h] * float(i * SUB)))
                mean = jnp.sum(mix, axis=1, keepdims=True) * (1.0 / DH)
                cen = mix - mean
                var = jnp.sum(cen * cen, axis=1, keepdims=True) * (1.0 / DH)
                out_ref[rs, cols] = (cen * lax.rsqrt(var + 1e-05) * gs[h, rs, :]).astype(BF16)

    for j in range(1, 4):
        @pl.when(z + 2 + 4 * j < nz)
        def _(j=j):
            ready_wait(2 + 4 * j)
            for h in range(nh):
                w_copy(h, j).start()

    ahead = (nz - 1 - z).astype(F32)
    mine = []
    for h in range(nh):
        one = lds[h] * float(tokens * NX)
        mine.append(jnp.exp((ahead + 1.0) * one) * cb[h, 0, pl.ds(z, 1), :]
                    + jnp.exp(ahead * one) * rtot[h, pl.ds(z, 1), :])
    with jax.named_scope("fwait"):
        for zz in range(1, nz):
            @pl.when(z < zz)
            def _(zz=zz):
                f_wait(zz).wait_recv()
    for h in range(nh):
        fin_ref[h] = mine[h] + jnp.sum(fr[:, h, :], axis=0, keepdims=True)

    with jax.named_scope("ends"):
        for zz in range(nz - 1):
            @pl.when(z > zz)
            def _(zz=zz):
                f_copy(zz).wait_send()
        for h in range(nh):
            for d in far:
                x_copy(h, d).wait_send()
                b_copy(h, d).wait_send()
        for slot, d, ok in raw:
            @pl.when(ok)
            def _(slot=slot, d=d):
                for h in range(nh):
                    a_copy(h, slot, d).wait_send()
        for j in range(4):
            @pl.when(z + 2 + 4 * j < nz)
            def _(j=j):
                for h in range(nh):
                    w_copy(h, j).wait_send()


def body(table, nz, queries, key_rows, value_rows, gate_input, norm_gain):
    tokens, width = queries.shape
    nh = width // DH
    rows = DH // NX
    anyspace = pl.BlockSpec(memory_space=pl.ANY)
    vmem = pl.BlockSpec(memory_space=pltpu.VMEM)
    dma = pltpu.SemaphoreType.DMA
    wide = pltpu.VMEM((tokens, width), BF16)
    eight = pltpu.VMEM((nh, NX, rows, DH), F32)
    four = pltpu.VMEM((nh, 4, rows, DH), F32)
    one = pltpu.VMEM((nh, rows, DH), F32)
    square = pltpu.VMEM((nh, DH, DH), F32)
    tall = pltpu.VMEM((nh, tokens, DH), F32)
    retained, final = pl.pallas_call(
        functools.partial(kernel, table, nz),
        out_shape=(pltpu.VMEM((tokens, width), BF16), pltpu.VMEM((nh, 1, DH), F32)),
        in_specs=[anyspace] * 5,
        out_specs=(vmem, vmem),
        scratch_shapes=[
            wide, wide, wide, wide, pltpu.VMEM((width,), F32),
            square, eight, eight, eight, one, four, one, four, eight, eight, square, tall, tall,
            pltpu.VMEM((nz, nh, DH), F32), pltpu.VMEM((nz, nh, DH), F32),
            dma((4, nh)), dma, dma((nh, NX)), dma((nh, NX)), dma((nh, 4)), dma((nh, 4)),
            dma((nh, 4)), dma((nh, 4)), dma((nh, NX)), dma((nh, NX)), dma((nz,)), dma((nz,)),
            pltpu.SemaphoreType.REGULAR((6,)),
        ],
        compiler_params=pltpu.CompilerParams(collective_id=0, has_side_effects=True),
        name="retention",
    )(queries, key_rows, value_rows, gate_input, norm_gain)
    return retained, final.reshape(1, nh, DH)


def solution(mesh):
    table = log_decays(mesh.shape["head"])
    rows = ("grp", "seq")
    placed = (P(rows, "head"),) * 4 + (P("head"),)
    return jax.shard_map(
        functools.partial(body, table, mesh.shape["seq"] // NX),
        mesh=mesh,
        in_specs=placed,
        out_specs=(P(rows, "head"), P(rows, "head", None)),
        check_vma=False,
    )
```

```python
import functools
import math

import jax
import jax.numpy as jnp
import numpy as np
from jax import lax
from jax.experimental import pallas as pl
from jax.experimental.pallas import tpu as pltpu
from jax.sharding import PartitionSpec as P

ALL_HEADS = 10
HEADS = 6
DH = 128
NX = 8
MESH = pl.DeviceIdType.MESH
F32 = jnp.float32
BF16 = jnp.bfloat16
SUB = 128


def log_decays(shards):
    per = HEADS // shards
    ids = ALL_HEADS - HEADS + np.arange(HEADS, dtype=np.float64)
    table = np.log1p(-np.exp2(-5.0 - ids)).reshape(shards, per)
    return [[float(np.float32(v)) for v in row] for row in table]


def kernel(
    table, nz,
    q_hbm, k_hbm, v_hbm, g_hbm, gain_hbm,
    out_ref, fin_ref,
    q_v, k_v, v_v, g_v, gain_v,
    st, sx, rx, xp, rtot, rz, win, rw, cb, rc, carr, inner, gs, fs, fr, es, er,
    kv_sem, in_sem, xs_sem, xr_sem, as_sem, ar_sem, ws_sem, wr_sem, bs_sem, br_sem, fs_sem, fr_sem, es_sem, er_sem, ready, xready,
):
    tokens = q_v.shape[0]
    nh = q_v.shape[1] // DH
    rows = DH // NX
    nb = tokens // SUB
    scale = DH ** (-0.5)
    me = lax.axis_index("seq")
    z = lax.div(me, NX)
    x = lax.rem(me, NX)
    hd = lax.axis_index("head")
    plane = (lax.axis_index("grp") == 0) & (hd == 0)
    column = plane & (x == 0)
    first = column & (z == 0)
    inner_col = column & (z > 0) & (z < nz - 1)
    last_c = nz - 3

    lds = []
    for h in range(nh):
        ld = jnp.float32(table[0][h])
        for s in range(1, len(table)):
            ld = jnp.where(hd == s, jnp.float32(table[s][h]), ld)
        lds.append(ld)

    def at(zz, xx):
        return {"seq": zz * NX + xx}

    def xwrap(d):
        return lax.rem(x + (d % NX), NX)

    def load(src, dst, h):
        cols = pl.ds(h * DH, DH)
        return pltpu.make_async_copy(src.at[:, cols], dst.at[:, cols], kv_sem.at[h])

    def kv_wait(h):
        two = pl.ds(0, 2 * DH)
        pltpu.make_async_copy(k_hbm.at[:, two], k_v.at[:, two], kv_sem.at[h]).wait()

    whole = (
        pltpu.make_async_copy(q_hbm, q_v, in_sem.at[0]),
        pltpu.make_async_copy(g_hbm, g_v, in_sem.at[1]),
        pltpu.make_async_copy(gain_hbm, gain_v, in_sem.at[2]),
    )

    for h in range(nh):
        load(k_hbm, k_v, h).start()
        load(v_hbm, v_v, h).start()

    def key_of(xx):
        k = jnp.where(xx < NX // 2, xx, 3 * NX // 2 - 1 - xx)
        return jnp.where((xx == 0) & (z == 0) & plane, NX, k)

    def x_of(k):
        if k == NX:
            return 0
        return k if k < NX // 2 else 3 * NX // 2 - 1 - k

    key = key_of(x)

    barrier = pltpu.get_barrier_semaphore()
    for d in range(1, NX):
        @pl.when(key_of(xwrap(d)) > key)
        def _(d=d):
            pl.semaphore_signal(barrier, inc=1, device_id=at(z, xwrap(d)), device_id_type=MESH)
    last = z == nz - 1
    express = ((0, 0), (1, 0), (0, 1))

    def tell_later():
        for zz in range(1, nz):
            ok = z < zz
            if zz < nz - 1:
                ok = ok & jnp.logical_not(first)

            @pl.when(ok)
            def _(zz=zz):
                pl.semaphore_signal(barrier, inc=1, device_id=at(zz, x), device_id_type=MESH)

    @pl.when(z > 0)
    def _():
        tell_later()

    @pl.when(inner_col)
    def _():
        pl.semaphore_signal(barrier, inc=1, device_id=at(0, x), device_id_type=MESH)
    owed = jnp.where(plane, NX - 1 - jnp.where(x == 0, 0, 1), NX - 1)
    count = key + z + jnp.where(last, owed + NX - 1, jnp.where(z == nz - 2, owed, 0))
    count = jnp.where((z == 0) & plane, key - 1, count)
    count = jnp.where(first, NX + nz - 3, count) - jnp.where(inner_col, 1, 0)
    with jax.named_scope("barrier"):
        @pl.when(count > 0)
        def _():
            pl.semaphore_wait(barrier, count)
    for d in range(1, NX):
        @pl.when(key_of(xwrap(d)) < key)
        def _(d=d):
            pl.semaphore_signal(xready.at[NX - d], inc=1, device_id=at(z, xwrap(d)), device_id_type=MESH)

    @pl.when(z == 0)
    def _():
        tell_later()

    @pl.when(first)
    def _():
        for zz in range(1, nz - 1):
            pl.semaphore_signal(xready.at[0], inc=1, device_id=at(zz, x), device_id_type=MESH)
    for j, k in express:
        @pl.when((z == j) & jnp.logical_not(first))
        def _(k=k):
            for d in range(1, NX):
                pl.semaphore_signal(barrier, inc=1, device_id=at(nz - 1 - k, xwrap(d)), device_id_type=MESH)
    for c in whole:
        c.start()

    def r_iota(n):
        return lax.broadcasted_iota(jnp.int32, (n, DH), 0).astype(F32)

    def x_copy(h, to):
        return pltpu.make_async_remote_copy(
            sx.at[to, h], rx.at[x, h], xs_sem, xr_sem,
            device_id=at(z, to), device_id_type=MESH)

    def x_copy_all(to):
        return pltpu.make_async_remote_copy(
            sx.at[to], rx.at[x], xs_sem, xr_sem,
            device_id=at(z, to), device_id_type=MESH)

    def b_copy(h, d):
        to = xwrap(d)
        return pltpu.make_async_remote_copy(
            cb.at[h, to], rc.at[h, x], bs_sem, br_sem.at[h],
            device_id=at(z, to), device_id_type=MESH)

    def e_copy(j, k, to):
        return pltpu.make_async_remote_copy(
            es.at[j, to], er.at[k, x], es_sem, er_sem,
            device_id=at(j, to), device_id_type=MESH)

    def moved(ref, sem):
        return pltpu.make_async_copy(ref, ref, sem)

    def moved_some(ref, sem, n):
        for m in range(1, ref.shape[0]):
            @pl.when(n == m)
            def _(m=m):
                moved(ref.at[pl.ds(0, m)], sem).wait()

    raw = (
        (1, 1, z <= last_c - 1),
        (0, 2, z <= last_c - 2),
        (3, 3, z == 0),
        (2, -1, (z >= 1) & (z <= last_c + 1)),
    )
    raw_in = ((0, (z >= 2) & (z <= last_c)), (3, z == 3), (1, (z >= 1) & (z <= last_c)), (2, z <= last_c))

    def a_copy(slot, d):
        return pltpu.make_async_remote_copy(
            rtot, rz.at[slot], as_sem.at[slot], ar_sem.at[slot],
            device_id=at(z + d, x), device_id_type=MESH)

    def w_copy(j):
        return pltpu.make_async_remote_copy(
            win, rw.at[j], ws_sem.at[j], wr_sem.at[j],
            device_id=at(z + (2 + 4 * j), x), device_id_type=MESH)

    def f_copy(zz):
        return pltpu.make_async_remote_copy(
            fs.at[zz], fr.at[z], fs_sem, fr_sem,
            device_id=at(zz, x), device_id_type=MESH)

    readies = ((1, (z >= 1) & (z <= last_c)), (2, z >= 2), (3, z == 3)) + tuple(
        (2 + 4 * j, z >= 2 + 4 * j) for j in range(1, 4))
    slot_of = {d: i for i, (d, _) in enumerate(readies)}

    def ready_wait(d):
        @pl.when(jnp.logical_not(first))
        def _():
            pl.semaphore_wait(ready.at[slot_of[d]], 1)

    far = (4, 3, 5, 2, 6, 1, 7)

    for h in range(nh):
        cols = pl.ds(h * DH, DH)
        tail = jnp.exp((tokens - 1 - r_iota(tokens)) * lds[h]) * scale
        with jax.named_scope(f"load{h}"):
            kv_wait(h)
        with jax.named_scope(f"state{h}"):
            kd = (k_v[:, cols].astype(F32) * tail).astype(BF16)
            st[h] = lax.dot_general(kd, v_v[:, cols], (((0,), (0,)), ((), ())), preferred_element_type=F32)
            for xx in range(NX):
                sx[xx, h] = st[h, pl.ds(xx, rows, stride=NX), :]
        for d in far:
            @pl.when((key_of(xwrap(d)) < key) & (z < nz - 2))
            def _(d=d, h=h):
                x_copy(h, xwrap(d)).start()

    for r in range(nh, es.shape[2]):
        es[:, :, r, :] = jnp.zeros((2, NX, DH), F32)

    @pl.when(z >= nz - 2)
    def _():
        for h in range(nh):
            w = (NX - 1 - x + NX * (nz - 1 - z)).astype(F32) * (lds[h] * float(tokens))
            for j in range(2):
                es[j, :, h, :] = st[h, pl.ds(j * NX, NX), :] * jnp.exp(w)
        for j, k in express:
            for d in far + (0,):
                to = xwrap(d)
                ok = z == nz - 1 - k
                if j == 0:
                    ok = ok & jnp.logical_not(plane & (to == 0))

                @pl.when(ok)
                def _(j=j, k=k, to=to):
                    e_copy(j, k, to).start()
        for d in far:
            @pl.when(key_of(xwrap(d)) < key)
            def _(d=d):
                x_copy_all(xwrap(d)).start()
    for d, ok in readies:
        @pl.when(ok & jnp.logical_not(column & (z == d)))
        def _(d=d):
            pl.semaphore_signal(ready.at[slot_of[d]], inc=1, device_id=at(z - d, x), device_id_type=MESH)

    zero = jnp.zeros((nh, rows, DH), F32)

    @pl.when(z < 2)
    def _():
        rz[0] = zero

    @pl.when(z < 1)
    def _():
        rz[1] = zero

    @pl.when(z != 3)
    def _():
        rz[3] = zero

    for j in range(1, 4):
        @pl.when((z > 0) & (z < 2 + 4 * j))
        def _(j=j):
            rw[j] = zero

    for zz in range(nz):
        ok = zz <= z
        for j, k in express:
            if zz == nz - 1 - k:
                ok = ok | ((z == j) & jnp.logical_not(first))

        @pl.when(ok)
        def _(zz=zz):
            fr[zz] = jnp.zeros(fr.shape[1:], F32)
    for r in range(nh, fs.shape[1]):
        fs[:, r, :] = jnp.zeros((nz, DH), F32)
    rx[x] = sx[x]
    with jax.named_scope("xready"):
        for k in range(1, NX + 1):
            to = x_of(k)

            @pl.when((key < k) & (z == 0) & plane if k == NX else key < k)
            def _(to=to):
                pl.semaphore_wait(xready.at[lax.rem(to + NX - x, NX)], 1)
                x_copy_all(to).start()

    ri = lax.broadcasted_iota(jnp.int32, (SUB, SUB), 0)
    ci = lax.broadcasted_iota(jnp.int32, (SUB, SUB), 1)

    def inner_of(h):
        cols = pl.ds(h * DH, DH)
        base = jnp.exp((ri - ci).astype(F32) * lds[h]) * scale
        for i in range(nb):
            qi = q_v[pl.ds(i * SUB, SUB), cols]
            parts = []
            for j in range(i + 1):
                s = lax.dot_general(qi, k_v[pl.ds(j * SUB, SUB), cols], (((1,), (1,)), ((), ())),
                                    preferred_element_type=F32)
                if j == i:
                    w = jnp.where(ri >= ci, s * base, 0.0)
                else:
                    w = s * (base * jnp.exp(lds[h] * float((i - j) * SUB)))
                parts.append(w.astype(BF16))
            w = parts[0] if i == 0 else jnp.concatenate(parts, axis=1)
            inner[h, pl.ds(i * SUB, SUB), :] = jnp.dot(
                w, v_v[pl.ds(0, (i + 1) * SUB), cols], preferred_element_type=F32)

    def gate_of(h):
        cols = pl.ds(h * DH, DH)
        gain = gain_v[pl.ds(h * DH, DH)].reshape(1, DH)
        u = g_v[:, cols].astype(F32)
        gs[h] = u / (1.0 + jnp.exp(-u)) * gain

    def local_work():
        with jax.named_scope("local"):
            for c in whole:
                c.wait()
            for h in range(nh):
                inner_of(h)
                gate_of(h)

    with jax.named_scope("xwait"):
        moved(rx.at[pl.ds(0, NX - 1)], xr_sem).wait()
    with jax.named_scope("prefix"):
        for h in range(nh):
            d1 = jnp.exp(lds[h] * float(tokens))
            acc = rx[0, h]
            for xx in range(1, NX):
                xp[h, xx] = acc
                acc = acc * d1 + rx[xx, h]
            rtot[h] = acc
            fs[:, h, :] = acc * jnp.exp((nz - 1 - z).astype(F32) * (lds[h] * float(tokens * NX)))

    for zz in range(nz - 1):
        ok = z > zz
        for j, k in express:
            if zz == j:
                ok = ok & ((z != nz - 1 - k) | column if j == 0 else z != nz - 1 - k)
        if zz == 0:
            ok = ok & jnp.logical_not(inner_col)

        @pl.when(ok)
        def _(zz=zz):
            f_copy(zz).start()
    for slot, d, ok in raw:
        @pl.when(ok)
        def _(slot=slot, d=d):
            if d > 0:
                ready_wait(d)
            else:
                @pl.when(column & (z == 1))
                def _():
                    pl.semaphore_wait(xready.at[0], 1)
            a_copy(slot, d).start()

    def back(h):
        for d in far:
            b_copy(h, d).start()
        rc[h, x] = cb[h, x]

    @pl.when(z == 0)
    def _():
        for h in range(nh):
            cb[h, 0] = jnp.zeros((rows, DH), F32)
            for xx in range(1, NX):
                cb[h, xx] = xp[h, xx]
            back(h)

    early = (z >= 1) & (z < nz // 2)

    @pl.when(early)
    def _():
        local_work()

    @pl.when(z <= last_c)
    def _():
        with jax.named_scope("windows"):
            @pl.when(z > last_c - 2)
            def _():
                ready_wait(2)
            for slot, ok in raw_in:
                @pl.when(ok)
                def _(slot=slot):
                    moved(rz.at[slot], ar_sem.at[slot]).wait()
            for h in range(nh):
                dd = [jnp.exp(lds[h] * float(tokens * NX * k)) for k in range(5)]
                win[h] = (rz[2, h] + dd[1] * rtot[h] + dd[2] * rz[1, h]
                          + dd[3] * rz[0, h] + dd[4] * rz[3, h])
            w_copy(0).start()

    with jax.named_scope("wwait"):
        for j in range(4):
            @pl.when(z >= 2 + 4 * j)
            def _(j=j):
                moved(rw.at[j], wr_sem.at[j]).wait()

    @pl.when(z == 1)
    def _():
        rw[0] = rz[1]
    @pl.when(z > 0)
    def _():
        for h in range(nh):
            ee = rw[0, h]
            for j in range(1, 4):
                ee = ee + rw[j, h] * jnp.exp(lds[h] * float(tokens * NX * 4 * j))
            cb[h, 0] = ee
            for xx in range(1, NX):
                cb[h, xx] = xp[h, xx] + ee * jnp.exp(lds[h] * float(tokens * xx))
            back(h)

    @pl.when(inner_col)
    def _():
        @pl.when(z > 1)
        def _():
            pl.semaphore_wait(xready.at[0], 1)
        f_copy(0).start()

    for j in range(1, 4):
        @pl.when(z + 2 + 4 * j < nz)
        def _(j=j):
            ready_wait(2 + 4 * j)
            w_copy(j).start()

    @pl.when(jnp.logical_not(early))
    def _():
        local_work()

    for h in range(nh):
        cols = pl.ds(h * DH, DH)
        lead = jnp.exp((r_iota(SUB) + 1.0) * lds[h])
        with jax.named_scope(f"bwait{h}"):
            moved(rc.at[h, pl.ds(0, NX - 1)], br_sem.at[h]).wait()
        with jax.named_scope(f"outer{h}"):
            for xx in range(NX):
                carr[h, pl.ds(xx, rows, stride=NX), :] = rc[h, xx]
            low = carr[h].astype(BF16)
            for i in range(nb):
                rs = pl.ds(i * SUB, SUB)
                o = jnp.dot(q_v[rs, cols], low, preferred_element_type=F32)
                mix = inner[h, rs, :] + o * (lead * jnp.exp(lds[h] * float(i * SUB)))
                mean = jnp.sum(mix, axis=1, keepdims=True) * (1.0 / DH)
                cen = mix - mean
                var = jnp.sum(cen * cen, axis=1, keepdims=True) * (1.0 / DH)
                out_ref[rs, cols] = (cen * lax.rsqrt(var + 1e-05) * gs[h, rs, :]).astype(BF16)

    ahead = (nz - 1 - z).astype(F32)
    mine = []
    for h in range(nh):
        one = lds[h] * float(tokens * NX)
        mine.append(jnp.exp((ahead + 1.0) * one) * cb[h, 0, pl.ds(z, 1), :]
                    + jnp.exp(ahead * one) * rtot[h, pl.ds(z, 1), :])
    with jax.named_scope("fwait"):
        less = jnp.where(first, 0, jnp.where(z == 0, 2, jnp.where(z == 1, 1, 0)))
        moved_some(fr, fr_sem, nz - 1 - z - less)

        @pl.when((z == 0) & jnp.logical_not(first))
        def _():
            moved(er, er_sem).wait()

        @pl.when(z == 1)
        def _():
            moved(er.at[0], er_sem).wait()
    for h in range(nh):
        fin_ref[h] = mine[h] + jnp.sum(fr[:, h, :], axis=0, keepdims=True)

    @pl.when((z <= 1) & jnp.logical_not(first))
    def _():
        for h in range(nh):
            fin_ref[h] = fin_ref[h] + jnp.sum(er[0, :, h, :], axis=0, keepdims=True)

    @pl.when((z == 0) & jnp.logical_not(first))
    def _():
        for h in range(nh):
            fin_ref[h] = fin_ref[h] + jnp.sum(er[1, :, h, :], axis=0, keepdims=True)

    with jax.named_scope("ends"):
        less = jnp.where(last, 2, jnp.where(z == nz - 2, 1, 0))
        moved_some(fs, fs_sem, z - less + jnp.where(column & (z >= nz - 2), 1, 0))
        late = jnp.where(last, 2 * NX, jnp.where(z == nz - 2, NX, 0))
        moved_some(fs, es_sem, late - jnp.where(plane & (z >= nz - 2), 1, 0))

        @pl.when(last & jnp.logical_not(plane))
        def _():
            moved(fs, es_sem).wait()
        moved(sx.at[pl.ds(0, NX - 1)], xs_sem).wait()
        moved(cb.at[:, pl.ds(0, NX - 1)], bs_sem).wait()
        for slot, d, ok in raw:
            @pl.when(ok)
            def _(slot=slot):
                moved(rtot, as_sem.at[slot]).wait()
        for j in range(4):
            @pl.when(z + 2 + 4 * j < nz)
            def _(j=j):
                moved(win, ws_sem.at[j]).wait()


def body(table, nz, queries, key_rows, value_rows, gate_input, norm_gain):
    tokens, width = queries.shape
    nh = width // DH
    rows = DH // NX
    anyspace = pl.BlockSpec(memory_space=pl.ANY)
    vmem = pl.BlockSpec(memory_space=pltpu.VMEM)
    dma = pltpu.SemaphoreType.DMA
    wide = pltpu.VMEM((tokens, width), BF16)
    spread = pltpu.VMEM((NX, nh, rows, DH), F32)
    eight = pltpu.VMEM((nh, NX, rows, DH), F32)
    four = pltpu.VMEM((4, nh, rows, DH), F32)
    one = pltpu.VMEM((nh, rows, DH), F32)
    square = pltpu.VMEM((nh, DH, DH), F32)
    tall = pltpu.VMEM((nh, tokens, DH), F32)
    few = pltpu.VMEM((2, NX, pl.next_power_of_2(nh), DH), F32)
    line = pltpu.VMEM((nz, pl.next_power_of_2(nh), DH), F32)
    retained, final = pl.pallas_call(
        functools.partial(kernel, table, nz),
        out_shape=(pltpu.VMEM((tokens, width), BF16), pltpu.VMEM((nh, 1, DH), F32)),
        in_specs=[anyspace] * 5,
        out_specs=(vmem, vmem),
        scratch_shapes=[
            wide, wide, wide, wide, pltpu.VMEM((width,), F32),
            square, spread, spread, eight, one, four, one, four, eight, eight, square, tall, tall, line, line, few, few,
            dma((nh,)), dma((3,)), dma, dma, dma((4,)), dma((4,)), dma((4,)), dma((4,)), dma, dma((nh,)), dma, dma, dma, dma,
            pltpu.SemaphoreType.REGULAR((6,)), pltpu.SemaphoreType.REGULAR((NX,)),
        ],
        compiler_params=pltpu.CompilerParams(collective_id=0, has_side_effects=True),
        name="retention",
    )(queries, key_rows, value_rows, gate_input, norm_gain)
    return retained, final.reshape(1, nh, DH)


def solution(mesh):
    table = log_decays(mesh.shape["head"])
    rows = ("grp", "seq")
    placed = (P(rows, "head"),) * 4 + (P("head"),)
    return jax.shard_map(
        functools.partial(body, table, mesh.shape["seq"] // NX),
        mesh=mesh,
        in_specs=placed,
        out_specs=(P(rows, "head"), P(rows, "head", None)),
        check_vma=False,
    )
```

```python
import functools
import math

import jax
import jax.numpy as jnp
import numpy as np
from jax import lax
from jax.experimental import pallas as pl
from jax.experimental.pallas import tpu as pltpu
from jax.sharding import PartitionSpec as P

ALL_HEADS = 10
HEADS = 6
DH = 128
NX = 8
MESH = pl.DeviceIdType.MESH
F32 = jnp.float32
BF16 = jnp.bfloat16
SUB = 128


def log_decays(shards):
    per = HEADS // shards
    ids = ALL_HEADS - HEADS + np.arange(HEADS, dtype=np.float64)
    table = np.log1p(-np.exp2(-5.0 - ids)).reshape(shards, per)
    return [[float(np.float32(v)) for v in row] for row in table]


def kernel(
    table, nz,
    q_hbm, k_hbm, v_hbm, g_hbm, gain_hbm,
    out_ref, fin_ref,
    q_v, k_v, v_v, g_v, gain_v,
    st, sx, rx, xp, rtot, rz, win, rw, cb, rc, carr, inner, gs, fs, fr, es, er,
    kv_sem, in_sem, xs_sem, xr_sem, as_sem, ar_sem, ws_sem, wr_sem, bs_sem, br_sem, fs_sem, fr_sem, es_sem, er_sem, ready, xready,
):
    tokens = q_v.shape[0]
    nh = q_v.shape[1] // DH
    rows = DH // NX
    nb = tokens // SUB
    scale = DH ** (-0.5)
    me = lax.axis_index("seq")
    z = lax.div(me, NX)
    x = lax.rem(me, NX)
    hd = lax.axis_index("head")
    plane = (lax.axis_index("grp") == 0) & (hd == 0)
    column = plane & (x == 0)
    first = column & (z == 0)
    inner_col = column & (z > 0) & (z < nz - 1)
    last_c = nz - 3

    lds = []
    for h in range(nh):
        ld = jnp.float32(table[0][h])
        for s in range(1, len(table)):
            ld = jnp.where(hd == s, jnp.float32(table[s][h]), ld)
        lds.append(ld)

    def at(zz, xx):
        return {"seq": zz * NX + xx}

    def xwrap(d):
        return lax.rem(x + (d % NX), NX)

    def r_iota(n):
        return lax.broadcasted_iota(jnp.int32, (n, DH), 0).astype(F32)

    def load(src, dst, h):
        cols = pl.ds(h * DH, DH)
        return pltpu.make_async_copy(src.at[:, cols], dst.at[:, cols], kv_sem.at[h])

    def kv_wait(h):
        two = pl.ds(0, 2 * DH)
        pltpu.make_async_copy(k_hbm.at[:, two], k_v.at[:, two], kv_sem.at[h]).wait()

    whole = (
        pltpu.make_async_copy(q_hbm, q_v, in_sem.at[0]),
        pltpu.make_async_copy(g_hbm, g_v, in_sem.at[1]),
        pltpu.make_async_copy(gain_hbm, gain_v, in_sem.at[2]),
    )

    for h in range(nh):
        load(k_hbm, k_v, h).start()
        load(v_hbm, v_v, h).start()

    def key_of(xx):
        k = jnp.where(xx < NX // 2, xx, 3 * NX // 2 - 1 - xx)
        return jnp.where((xx == 0) & (z == 0) & plane, NX, k)

    def x_of(k):
        if k == NX:
            return 0
        return k if k < NX // 2 else 3 * NX // 2 - 1 - k

    key = key_of(x)

    barrier = pltpu.get_barrier_semaphore()
    for d in range(1, NX):
        @pl.when(key_of(xwrap(d)) > key)
        def _(d=d):
            pl.semaphore_signal(barrier, inc=1, device_id=at(z, xwrap(d)), device_id_type=MESH)
    last = z == nz - 1
    express = ((0, 0), (1, 0), (0, 1))

    def tell_later():
        for zz in range(1, nz):
            ok = z < zz
            if zz < nz - 1:
                ok = ok & jnp.logical_not(first)

            @pl.when(ok)
            def _(zz=zz):
                pl.semaphore_signal(barrier, inc=1, device_id=at(zz, x), device_id_type=MESH)

    @pl.when(z > 0)
    def _():
        tell_later()

    @pl.when(inner_col)
    def _():
        pl.semaphore_signal(barrier, inc=1, device_id=at(0, x), device_id_type=MESH)
    owed = jnp.where(plane, NX - 1 - jnp.where(x == 0, 0, 1), NX - 1)
    count = key + z + jnp.where(last, owed + NX - 1, jnp.where(z == nz - 2, owed, 0))
    count = jnp.where((z == 0) & plane, key - 1, count)
    count = jnp.where(first, NX + nz - 3, count) - jnp.where(inner_col, 1, 0)
    for h in range(nh):
        inner[h] = jnp.exp((tokens - 1 - r_iota(tokens)) * lds[h]) * scale
    with jax.named_scope("barrier"):
        @pl.when(count > 0)
        def _():
            pl.semaphore_wait(barrier, count)
    for d in range(1, NX):
        @pl.when(key_of(xwrap(d)) < key)
        def _(d=d):
            pl.semaphore_signal(xready.at[NX - d], inc=1, device_id=at(z, xwrap(d)), device_id_type=MESH)

    @pl.when(z == 0)
    def _():
        tell_later()

    @pl.when(first)
    def _():
        for zz in range(1, nz - 1):
            pl.semaphore_signal(xready.at[0], inc=1, device_id=at(zz, x), device_id_type=MESH)
    for j, k in express:
        @pl.when((z == j) & jnp.logical_not(first))
        def _(k=k):
            for d in range(1, NX):
                pl.semaphore_signal(barrier, inc=1, device_id=at(nz - 1 - k, xwrap(d)), device_id_type=MESH)
    for c in whole:
        c.start()

    def x_copy(to):
        return pltpu.make_async_remote_copy(
            sx.at[to], rx.at[x], xs_sem, xr_sem,
            device_id=at(z, to), device_id_type=MESH)

    def b_copy(h, d):
        to = xwrap(d)
        return pltpu.make_async_remote_copy(
            cb.at[h, to], rc.at[h, x], bs_sem, br_sem.at[h],
            device_id=at(z, to), device_id_type=MESH)

    def e_copy(j, k, to):
        return pltpu.make_async_remote_copy(
            es.at[j, to], er.at[k, x], es_sem, er_sem,
            device_id=at(j, to), device_id_type=MESH)

    def moved(ref, sem):
        return pltpu.make_async_copy(ref, ref, sem)

    def moved_some(ref, sem, n):
        for m in range(1, ref.shape[0] + 1):
            @pl.when(n == m)
            def _(m=m):
                moved(ref.at[pl.ds(0, m)], sem).wait()

    raw = (
        (1, 1, z <= last_c - 1),
        (0, 2, z <= last_c - 2),
        (3, 3, z == 0),
        (2, -1, (z >= 1) & (z <= last_c + 1)),
    )
    def a_copy(slot, d):
        return pltpu.make_async_remote_copy(
            rtot, rz.at[slot], as_sem, ar_sem,
            device_id=at(z + d, x), device_id_type=MESH)

    def w_copy(j):
        return pltpu.make_async_remote_copy(
            win, rw.at[j], ws_sem, wr_sem,
            device_id=at(z + (2 + 4 * j), x), device_id_type=MESH)

    def f_copy(zz):
        return pltpu.make_async_remote_copy(
            fs.at[zz], fr.at[z], fs_sem, fr_sem,
            device_id=at(zz, x), device_id_type=MESH)

    readies = ((1, (z >= 1) & (z <= last_c)), (2, z >= 2), (3, z == 3)) + tuple(
        (2 + 4 * j, z >= 2 + 4 * j) for j in range(1, 4))
    slot_of = {d: i for i, (d, _) in enumerate(readies)}

    def ready_wait(d):
        @pl.when(jnp.logical_not(first))
        def _():
            pl.semaphore_wait(ready.at[slot_of[d]], 1)

    far = (4, 3, 5, 2, 6, 1, 7)

    for h in range(nh):
        cols = pl.ds(h * DH, DH)
        with jax.named_scope(f"load{h}"):
            kv_wait(h)
        with jax.named_scope(f"state{h}"):
            kd = (k_v[:, cols].astype(F32) * inner[h]).astype(BF16)
            st[h] = lax.dot_general(kd, v_v[:, cols], (((0,), (0,)), ((), ())), preferred_element_type=F32)
            for xx in range(NX):
                sx[xx, h] = st[h, pl.ds(xx, rows, stride=NX), :]

    for r in range(nh, es.shape[2]):
        es[:, :, r, :] = jnp.zeros((2, NX, DH), F32)

    @pl.when(z >= nz - 2)
    def _():
        for h in range(nh):
            w = (NX - 1 - x + NX * (nz - 1 - z)).astype(F32) * (lds[h] * float(tokens))
            for j in range(2):
                es[j, :, h, :] = st[h, pl.ds(j * NX, NX), :] * jnp.exp(w)
        for j, k in express:
            for d in far + (0,):
                to = xwrap(d)
                ok = z == nz - 1 - k
                if j == 0:
                    ok = ok & jnp.logical_not(plane & (to == 0))

                @pl.when(ok)
                def _(j=j, k=k, to=to):
                    e_copy(j, k, to).start()

    for d in far:
        @pl.when(key_of(xwrap(d)) < key)
        def _(d=d):
            x_copy(xwrap(d)).start()
    for d, ok in readies:
        @pl.when(ok & jnp.logical_not(column & (z == d)))
        def _(d=d):
            pl.semaphore_signal(ready.at[slot_of[d]], inc=1, device_id=at(z - d, x), device_id_type=MESH)

    zero = jnp.zeros((nh, rows, DH), F32)

    @pl.when(z < 2)
    def _():
        rz[0] = zero

    @pl.when(z < 1)
    def _():
        rz[1] = zero

    @pl.when(z != 3)
    def _():
        rz[3] = zero

    for j in range(1, 4):
        @pl.when((z > 0) & (z < 2 + 4 * j))
        def _(j=j):
            rw[j] = zero

    for zz in range(nz):
        ok = zz <= z
        for j, k in express:
            if zz == nz - 1 - k:
                ok = ok | ((z == j) & jnp.logical_not(first))

        @pl.when(ok)
        def _(zz=zz):
            fr[zz] = jnp.zeros(fr.shape[1:], F32)
    for r in range(nh, fs.shape[1]):
        fs[:, r, :] = jnp.zeros((nz, DH), F32)
    rx[x] = sx[x]
    with jax.named_scope("xready"):
        for k in range(1, NX + 1):
            to = x_of(k)

            @pl.when((key < k) & (z == 0) & plane if k == NX else key < k)
            def _(to=to):
                pl.semaphore_wait(xready.at[lax.rem(to + NX - x, NX)], 1)
                x_copy(to).start()

    ri = lax.broadcasted_iota(jnp.int32, (SUB, SUB), 0)
    ci = lax.broadcasted_iota(jnp.int32, (SUB, SUB), 1)

    def inner_of(h):
        cols = pl.ds(h * DH, DH)
        base = jnp.exp((ri - ci).astype(F32) * lds[h]) * scale
        for i in range(nb):
            qi = q_v[pl.ds(i * SUB, SUB), cols]
            parts = []
            for j in range(i + 1):
                s = lax.dot_general(qi, k_v[pl.ds(j * SUB, SUB), cols], (((1,), (1,)), ((), ())),
                                    preferred_element_type=F32)
                if j == i:
                    w = jnp.where(ri >= ci, s * base, 0.0)
                else:
                    w = s * (base * jnp.exp(lds[h] * float((i - j) * SUB)))
                parts.append(w.astype(BF16))
            w = parts[0] if i == 0 else jnp.concatenate(parts, axis=1)
            inner[h, pl.ds(i * SUB, SUB), :] = jnp.dot(
                w, v_v[pl.ds(0, (i + 1) * SUB), cols], preferred_element_type=F32)

    def gate_of(h):
        cols = pl.ds(h * DH, DH)
        gain = gain_v[pl.ds(h * DH, DH)].reshape(1, DH)
        u = g_v[:, cols].astype(F32)
        gs[h] = u / (1.0 + jnp.exp(-u)) * gain

    def local_work():
        with jax.named_scope("local"):
            for c in whole:
                c.wait()
            for h in range(nh):
                inner_of(h)
                gate_of(h)

    with jax.named_scope("xwait"):
        moved(rx.at[pl.ds(0, NX - 1)], xr_sem).wait()
    with jax.named_scope("prefix"):
        for h in range(nh):
            d1 = jnp.exp(lds[h] * float(tokens))
            acc = rx[0, h]
            for xx in range(1, NX):
                xp[h, xx] = acc
                acc = acc * d1 + rx[xx, h]
            rtot[h] = acc
            fs[:, h, :] = acc * jnp.exp((nz - 1 - z).astype(F32) * (lds[h] * float(tokens * NX)))

    for zz in range(nz - 1):
        ok = z > zz
        for j, k in express:
            if zz == j:
                ok = ok & ((z != nz - 1 - k) | column if j == 0 else z != nz - 1 - k)
        if zz == 0:
            ok = ok & jnp.logical_not(inner_col)

        @pl.when(ok)
        def _(zz=zz):
            f_copy(zz).start()
    for slot, d, ok in raw:
        @pl.when(ok)
        def _(slot=slot, d=d):
            if d > 0:
                ready_wait(d)
            else:
                @pl.when(column & (z == 1))
                def _():
                    pl.semaphore_wait(xready.at[0], 1)
            a_copy(slot, d).start()

    def back(h):
        for d in far:
            b_copy(h, d).start()
        rc[h, x] = cb[h, x]

    @pl.when(z == 0)
    def _():
        for h in range(nh):
            cb[h, 0] = jnp.zeros((rows, DH), F32)
            for xx in range(1, NX):
                cb[h, xx] = xp[h, xx]
            back(h)

    early = (z >= 1) & (z < nz // 2)

    @pl.when(early)
    def _():
        local_work()

    @pl.when(z <= last_c)
    def _():
        with jax.named_scope("windows"):
            @pl.when(z > last_c - 2)
            def _():
                ready_wait(2)
            n = 1 + jnp.where(z >= 1, 1, 0) + jnp.where(z >= 2, 1, 0) + jnp.where(z == 3, 1, 0)
            moved_some(rz, ar_sem, n)
            for h in range(nh):
                dd = [jnp.exp(lds[h] * float(tokens * NX * k)) for k in range(5)]
                win[h] = (rz[2, h] + dd[1] * rtot[h] + dd[2] * rz[1, h]
                          + dd[3] * rz[0, h] + dd[4] * rz[3, h])
            w_copy(0).start()

    with jax.named_scope("wwait"):
        moved_some(rw, wr_sem, lax.div(z + 2, 4))

    @pl.when(z == 1)
    def _():
        rw[0] = rz[1]
    @pl.when(z > 0)
    def _():
        for h in range(nh):
            ee = rw[0, h]
            for j in range(1, 4):
                ee = ee + rw[j, h] * jnp.exp(lds[h] * float(tokens * NX * 4 * j))
            cb[h, 0] = ee
            for xx in range(1, NX):
                cb[h, xx] = xp[h, xx] + ee * jnp.exp(lds[h] * float(tokens * xx))
            back(h)

    @pl.when(inner_col)
    def _():
        @pl.when(z > 1)
        def _():
            pl.semaphore_wait(xready.at[0], 1)
        f_copy(0).start()

    for j in range(1, 4):
        @pl.when(z + 2 + 4 * j < nz)
        def _(j=j):
            ready_wait(2 + 4 * j)
            w_copy(j).start()

    @pl.when(jnp.logical_not(early))
    def _():
        local_work()

    for h in range(nh):
        cols = pl.ds(h * DH, DH)
        lead = jnp.exp((r_iota(SUB) + 1.0) * lds[h])
        with jax.named_scope(f"bwait{h}"):
            moved(rc.at[h, pl.ds(0, NX - 1)], br_sem.at[h]).wait()
        with jax.named_scope(f"outer{h}"):
            for xx in range(NX):
                carr[h, pl.ds(xx, rows, stride=NX), :] = rc[h, xx]
            low = carr[h].astype(BF16)
            for i in range(nb):
                rs = pl.ds(i * SUB, SUB)
                o = jnp.dot(q_v[rs, cols], low, preferred_element_type=F32)
                mix = inner[h, rs, :] + o * (lead * jnp.exp(lds[h] * float(i * SUB)))
                mean = jnp.sum(mix, axis=1, keepdims=True) * (1.0 / DH)
                cen = mix - mean
                var = jnp.sum(cen * cen, axis=1, keepdims=True) * (1.0 / DH)
                out_ref[rs, cols] = (cen * lax.rsqrt(var + 1e-05) * gs[h, rs, :]).astype(BF16)

    ahead = (nz - 1 - z).astype(F32)
    mine = []
    for h in range(nh):
        one = lds[h] * float(tokens * NX)
        mine.append(jnp.exp((ahead + 1.0) * one) * cb[h, 0, pl.ds(z, 1), :]
                    + jnp.exp(ahead * one) * rtot[h, pl.ds(z, 1), :])
    with jax.named_scope("fwait"):
        less = jnp.where(first, 0, jnp.where(z == 0, 2, jnp.where(z == 1, 1, 0)))
        moved_some(fr, fr_sem, nz - 1 - z - less)

        @pl.when((z == 0) & jnp.logical_not(first))
        def _():
            moved(er, er_sem).wait()

        @pl.when(z == 1)
        def _():
            moved(er.at[0], er_sem).wait()
    for h in range(nh):
        fin_ref[h] = mine[h] + jnp.sum(fr[:, h, :], axis=0, keepdims=True)

    @pl.when((z <= 1) & jnp.logical_not(first))
    def _():
        for h in range(nh):
            fin_ref[h] = fin_ref[h] + jnp.sum(er[0, :, h, :], axis=0, keepdims=True)

    @pl.when((z == 0) & jnp.logical_not(first))
    def _():
        for h in range(nh):
            fin_ref[h] = fin_ref[h] + jnp.sum(er[1, :, h, :], axis=0, keepdims=True)

    with jax.named_scope("ends"):
        less = jnp.where(last, 2, jnp.where(z == nz - 2, 1, 0))
        moved_some(fs, fs_sem, z - less + jnp.where(column & (z >= nz - 2), 1, 0))
        late = jnp.where(last, 2 * NX, jnp.where(z == nz - 2, NX, 0))
        moved_some(fs, es_sem, late - jnp.where(plane & (z >= nz - 2), 1, 0))
        moved(sx.at[pl.ds(0, NX - 1)], xs_sem).wait()
        moved(cb.at[:, pl.ds(0, NX - 1)], bs_sem).wait()
        for slot, d, ok in raw:
            @pl.when(ok)
            def _(slot=slot):
                moved(rtot, as_sem).wait()
        for j in range(4):
            @pl.when(z + 2 + 4 * j < nz)
            def _(j=j):
                moved(win, ws_sem).wait()


def body(table, nz, queries, key_rows, value_rows, gate_input, norm_gain):
    tokens, width = queries.shape
    nh = width // DH
    rows = DH // NX
    anyspace = pl.BlockSpec(memory_space=pl.ANY)
    vmem = pl.BlockSpec(memory_space=pltpu.VMEM)
    dma = pltpu.SemaphoreType.DMA
    wide = pltpu.VMEM((tokens, width), BF16)
    spread = pltpu.VMEM((NX, nh, rows, DH), F32)
    eight = pltpu.VMEM((nh, NX, rows, DH), F32)
    four = pltpu.VMEM((4, nh, rows, DH), F32)
    one = pltpu.VMEM((nh, rows, DH), F32)
    square = pltpu.VMEM((nh, DH, DH), F32)
    tall = pltpu.VMEM((nh, tokens, DH), F32)
    few = pltpu.VMEM((2, NX, pl.next_power_of_2(nh), DH), F32)
    line = pltpu.VMEM((nz, pl.next_power_of_2(nh), DH), F32)
    retained, final = pl.pallas_call(
        functools.partial(kernel, table, nz),
        out_shape=(pltpu.VMEM((tokens, width), BF16), pltpu.VMEM((nh, 1, DH), F32)),
        in_specs=[anyspace] * 5,
        out_specs=(vmem, vmem),
        scratch_shapes=[
            wide, wide, wide, wide, pltpu.VMEM((width,), F32),
            square, spread, spread, eight, one, four, one, four, eight, eight, square, tall, tall, line, line, few, few,
            dma((nh,)), dma((3,)), dma, dma, dma, dma, dma, dma, dma, dma((nh,)), dma, dma, dma, dma,
            pltpu.SemaphoreType.REGULAR((6,)), pltpu.SemaphoreType.REGULAR((NX,)),
        ],
        compiler_params=pltpu.CompilerParams(collective_id=0, has_side_effects=True),
        name="retention",
    )(queries, key_rows, value_rows, gate_input, norm_gain)
    return retained, final.reshape(1, nh, DH)


def solution(mesh):
    table = log_decays(mesh.shape["head"])
    rows = ("grp", "seq")
    placed = (P(rows, "head"),) * 4 + (P("head"),)
    return jax.shard_map(
        functools.partial(body, table, mesh.shape["seq"] // NX),
        mesh=mesh,
        in_specs=placed,
        out_specs=(P(rows, "head"), P(rows, "head", None)),
        check_vma=False,
    )
```

```python
import functools
import math

import jax
import jax.numpy as jnp
import numpy as np
from jax import lax
from jax.experimental import pallas as pl
from jax.experimental.pallas import tpu as pltpu
from jax.sharding import PartitionSpec as P

ALL_HEADS = 10
HEADS = 6
DH = 128
NX = 8
MESH = pl.DeviceIdType.MESH
F32 = jnp.float32
BF16 = jnp.bfloat16
SUB = 128


def log_decays(shards):
    per = HEADS // shards
    ids = ALL_HEADS - HEADS + np.arange(HEADS, dtype=np.float64)
    table = np.log1p(-np.exp2(-5.0 - ids)).reshape(shards, per)
    return [[float(np.float32(v)) for v in row] for row in table]


def kernel(
    table, nz,
    q_hbm, k_hbm, v_hbm, g_hbm, gain_hbm,
    out_ref, fin_ref,
    q_v, k_v, v_v, g_v, gain_v,
    st, sx, rx, xp, rtot, rz, win, rw, cb, rc, carr, inner, gs, fs, fr, es, er,
    kv_sem, in_sem, xs_sem, xr_sem, as_sem, ar_sem, ws_sem, wr_sem, bs_sem, br_sem, fs_sem, fr_sem, es_sem, er_sem, ready, xready,
):
    tokens = q_v.shape[0]
    nh = q_v.shape[1] // DH
    rows = DH // NX
    nb = tokens // SUB
    scale = DH ** (-0.5)
    me = lax.axis_index("seq")
    z = lax.div(me, NX)
    x = lax.rem(me, NX)
    hd = lax.axis_index("head")
    plane = (lax.axis_index("grp") == 0) & (hd == 0)
    column = plane & (x == 0)
    first = column & (z == 0)
    inner_col = column & (z > 0) & (z < nz - 2)
    last_c = nz - 3

    lds = []
    for h in range(nh):
        ld = jnp.float32(table[0][h])
        for s in range(1, len(table)):
            ld = jnp.where(hd == s, jnp.float32(table[s][h]), ld)
        lds.append(ld)

    def at(zz, xx):
        return {"seq": zz * NX + xx}

    def xwrap(d):
        return lax.rem(x + (d % NX), NX)

    def r_iota(n):
        return lax.broadcasted_iota(jnp.int32, (n, DH), 0).astype(F32)

    def load(src, dst, h):
        cols = pl.ds(h * DH, DH)
        return pltpu.make_async_copy(src.at[:, cols], dst.at[:, cols], kv_sem.at[h])

    def kv_wait(h):
        two = pl.ds(0, 2 * DH)
        pltpu.make_async_copy(k_hbm.at[:, two], k_v.at[:, two], kv_sem.at[h]).wait()

    whole = (
        pltpu.make_async_copy(q_hbm, q_v, in_sem.at[0]),
        pltpu.make_async_copy(g_hbm, g_v, in_sem.at[1]),
        pltpu.make_async_copy(gain_hbm, gain_v, in_sem.at[2]),
    )

    def key_of(xx):
        k = jnp.where(xx < NX // 2, xx, 3 * NX // 2 - 1 - xx)
        k = jnp.where(xx == NX // 2, NX - 2, jnp.where(xx == NX // 2 + 1, NX - 1, k))
        return jnp.where((xx == 0) & (z == 0) & plane, NX, k)

    def x_of(k):
        if k == NX:
            return 0
        if k >= NX - 2:
            return k - NX // 2 + 2
        return k if k < NX // 2 else 3 * NX // 2 - 1 - k

    key = key_of(x)

    barrier = pltpu.get_barrier_semaphore()
    for d in range(1, NX):
        @pl.when(key_of(xwrap(d)) > key)
        def _(d=d):
            pl.semaphore_signal(barrier, inc=1, device_id=at(z, xwrap(d)), device_id_type=MESH)
    for h in range(nh):
        load(k_hbm, k_v, h).start()
        load(v_hbm, v_v, h).start()

    last = z == nz - 1
    express = ((0, 0), (1, 0), (0, 1), (0, 2))

    def tell_later():
        for zz in range(1, nz):
            ok = z < zz
            if zz < nz - 2:
                ok = ok & jnp.logical_not(first)

            @pl.when(ok)
            def _(zz=zz):
                pl.semaphore_signal(barrier, inc=1, device_id=at(zz, x), device_id_type=MESH)

    @pl.when(z > 0)
    def _():
        tell_later()

    @pl.when(inner_col)
    def _():
        pl.semaphore_signal(barrier, inc=1, device_id=at(0, x), device_id_type=MESH)
    owed = jnp.where(plane, NX - 1 - jnp.where(x == 0, 0, 1), NX - 1)
    count = key + z + jnp.where(last, owed + NX - 1, jnp.where((z == nz - 2) | (z == nz - 3), owed, 0))
    count = jnp.where((z == 0) & plane, key - 1, count)
    count = jnp.where(first, NX + nz - 4, count) - jnp.where(inner_col, 1, 0)
    for h in range(nh):
        inner[h] = jnp.exp((tokens - 1 - r_iota(tokens)) * lds[h]) * scale
    with jax.named_scope("barrier"):
        @pl.when(count > 0)
        def _():
            pl.semaphore_wait(barrier, count)
    for d in range(1, NX):
        @pl.when(key_of(xwrap(d)) < key)
        def _(d=d):
            pl.semaphore_signal(xready.at[NX - d], inc=1, device_id=at(z, xwrap(d)), device_id_type=MESH)

    @pl.when(z == 0)
    def _():
        tell_later()

    @pl.when(first)
    def _():
        for zz in range(1, nz - 2):
            pl.semaphore_signal(xready.at[0], inc=1, device_id=at(zz, x), device_id_type=MESH)
    for j, k in express:
        @pl.when((z == j) & jnp.logical_not(first))
        def _(k=k):
            for d in range(1, NX):
                pl.semaphore_signal(barrier, inc=1, device_id=at(nz - 1 - k, xwrap(d)), device_id_type=MESH)
    for c in whole:
        c.start()

    def x_copy(to):
        return pltpu.make_async_remote_copy(
            sx.at[to], rx.at[x], xs_sem, xr_sem,
            device_id=at(z, to), device_id_type=MESH)

    def b_copy(h, d):
        to = xwrap(d)
        return pltpu.make_async_remote_copy(
            cb.at[h, to], rc.at[h, x], bs_sem, br_sem.at[h],
            device_id=at(z, to), device_id_type=MESH)

    def e_copy(j, k, to):
        return pltpu.make_async_remote_copy(
            es.at[j, to], er.at[k, x], es_sem, er_sem,
            device_id=at(j, to), device_id_type=MESH)

    def moved(ref, sem):
        return pltpu.make_async_copy(ref, ref, sem)

    def moved_some(ref, sem, n):
        for m in range(1, ref.shape[0] + 1):
            @pl.when(n == m)
            def _(m=m):
                moved(ref.at[pl.ds(0, m)], sem).wait()

    raw = (
        (1, 1, z <= last_c - 1),
        (0, 2, z <= last_c - 2),
        (3, 3, z == 0),
        (2, -1, (z >= 1) & (z <= last_c + 1)),
    )
    def a_copy(slot, d):
        return pltpu.make_async_remote_copy(
            rtot, rz.at[slot], as_sem, ar_sem,
            device_id=at(z + d, x), device_id_type=MESH)

    def w_copy(j):
        return pltpu.make_async_remote_copy(
            win, rw.at[j], ws_sem, wr_sem,
            device_id=at(z + (2 + 4 * j), x), device_id_type=MESH)

    def f_copy(zz):
        return pltpu.make_async_remote_copy(
            fs.at[zz], fr.at[z], fs_sem, fr_sem,
            device_id=at(zz, x), device_id_type=MESH)

    readies = ((1, (z >= 1) & (z <= last_c)), (2, z >= 2), (3, z == 3)) + tuple(
        (2 + 4 * j, z >= 2 + 4 * j) for j in range(1, 4))
    slot_of = {d: i for i, (d, _) in enumerate(readies)}

    def ready_wait(d):
        @pl.when(jnp.logical_not(first) if d < nz - 2 else z >= 0)
        def _():
            pl.semaphore_wait(ready.at[slot_of[d]], 1)

    far = (4, 3, 5, 2, 6, 1, 7)

    for h in range(nh):
        cols = pl.ds(h * DH, DH)
        with jax.named_scope(f"load{h}"):
            kv_wait(h)
        with jax.named_scope(f"state{h}"):
            kd = (k_v[:, cols].astype(F32) * inner[h]).astype(BF16)
            st[h] = lax.dot_general(kd, v_v[:, cols], (((0,), (0,)), ((), ())), preferred_element_type=F32)
            for xx in range(NX):
                sx[xx, h] = st[h, pl.ds(xx, rows, stride=NX), :]

    for r in range(nh, es.shape[2]):
        es[:, :, r, :] = jnp.zeros((2, NX, DH), F32)

    @pl.when(z >= nz - 3)
    def _():
        for h in range(nh):
            w = (NX - 1 - x + NX * (nz - 1 - z)).astype(F32) * (lds[h] * float(tokens))
            for j in range(2):
                es[j, :, h, :] = st[h, pl.ds(j * NX, NX), :] * jnp.exp(w)
        for j, k in express:
            for d in far + (0,):
                to = xwrap(d)
                ok = z == nz - 1 - k
                if j == 0:
                    ok = ok & jnp.logical_not(plane & (to == 0))

                @pl.when(ok)
                def _(j=j, k=k, to=to):
                    e_copy(j, k, to).start()

    for d in far:
        @pl.when(key_of(xwrap(d)) < key)
        def _(d=d):
            x_copy(xwrap(d)).start()
    for d, ok in readies:
        @pl.when(ok & jnp.logical_not(inner_col & (z == d)))
        def _(d=d):
            pl.semaphore_signal(ready.at[slot_of[d]], inc=1, device_id=at(z - d, x), device_id_type=MESH)

    zero = jnp.zeros((nh, rows, DH), F32)

    @pl.when(z < 2)
    def _():
        rz[0] = zero

    @pl.when(z < 1)
    def _():
        rz[1] = zero

    @pl.when(z != 3)
    def _():
        rz[3] = zero

    for j in range(1, 4):
        @pl.when((z > 0) & (z < 2 + 4 * j))
        def _(j=j):
            rw[j] = zero

    for zz in range(nz):
        ok = zz <= z
        for j, k in express:
            if zz == nz - 1 - k:
                ok = ok | ((z == j) & jnp.logical_not(first))

        @pl.when(ok)
        def _(zz=zz):
            fr[zz] = jnp.zeros(fr.shape[1:], F32)
    for r in range(nh, fs.shape[1]):
        fs[:, r, :] = jnp.zeros((nz, DH), F32)
    rx[x] = sx[x]
    with jax.named_scope("xready"):
        for k in range(1, NX + 1):
            to = x_of(k)

            @pl.when((key < k) & (z == 0) & plane if k == NX else key < k)
            def _(to=to):
                pl.semaphore_wait(xready.at[lax.rem(to + NX - x, NX)], 1)
                x_copy(to).start()

    ri = lax.broadcasted_iota(jnp.int32, (SUB, SUB), 0)
    ci = lax.broadcasted_iota(jnp.int32, (SUB, SUB), 1)

    def inner_of(h):
        cols = pl.ds(h * DH, DH)
        base = jnp.exp((ri - ci).astype(F32) * lds[h]) * scale
        for i in range(nb):
            qi = q_v[pl.ds(i * SUB, SUB), cols]
            parts = []
            for j in range(i + 1):
                s = lax.dot_general(qi, k_v[pl.ds(j * SUB, SUB), cols], (((1,), (1,)), ((), ())),
                                    preferred_element_type=F32)
                if j == i:
                    w = jnp.where(ri >= ci, s * base, 0.0)
                else:
                    w = s * (base * jnp.exp(lds[h] * float((i - j) * SUB)))
                parts.append(w.astype(BF16))
            w = parts[0] if i == 0 else jnp.concatenate(parts, axis=1)
            inner[h, pl.ds(i * SUB, SUB), :] = jnp.dot(
                w, v_v[pl.ds(0, (i + 1) * SUB), cols], preferred_element_type=F32)

    def gate_of(h):
        cols = pl.ds(h * DH, DH)
        gain = gain_v[pl.ds(h * DH, DH)].reshape(1, DH)
        u = g_v[:, cols].astype(F32)
        gs[h] = u / (1.0 + jnp.exp(-u)) * gain

    def local_work():
        with jax.named_scope("local"):
            for c in whole:
                c.wait()
            for h in range(nh):
                inner_of(h)
                gate_of(h)

    with jax.named_scope("xwait"):
        moved(rx.at[pl.ds(0, NX - 1)], xr_sem).wait()
    with jax.named_scope("prefix"):
        for h in range(nh):
            d1 = jnp.exp(lds[h] * float(tokens))
            acc = rx[0, h]
            for xx in range(1, NX):
                xp[h, xx] = acc
                acc = acc * d1 + rx[xx, h]
            rtot[h] = acc
            fs[:, h, :] = acc * jnp.exp((nz - 1 - z).astype(F32) * (lds[h] * float(tokens * NX)))

    for zz in range(nz - 1):
        ok = z > zz
        for j, k in express:
            if zz == j:
                ok = ok & ((z != nz - 1 - k) | column if j == 0 else z != nz - 1 - k)
        if zz == 0:
            ok = ok & jnp.logical_not(inner_col)

        @pl.when(ok)
        def _(zz=zz):
            f_copy(zz).start()
    for slot, d, ok in raw:
        @pl.when(ok)
        def _(slot=slot, d=d):
            if d > 0:
                ready_wait(d)
            else:
                @pl.when(column & (z == 1))
                def _():
                    pl.semaphore_wait(xready.at[0], 1)
            a_copy(slot, d).start()

    def back(h):
        for d in far:
            b_copy(h, d).start()
        rc[h, x] = cb[h, x]

    @pl.when(z == 0)
    def _():
        for h in range(nh):
            cb[h, 0] = jnp.zeros((rows, DH), F32)
            for xx in range(1, NX):
                cb[h, xx] = xp[h, xx]
            back(h)

    early = (z >= 1) & (z < nz // 2)

    @pl.when(early)
    def _():
        local_work()

    @pl.when(z <= last_c)
    def _():
        with jax.named_scope("windows"):
            @pl.when(z > last_c - 2)
            def _():
                ready_wait(2)
            n = 1 + jnp.where(z >= 1, 1, 0) + jnp.where(z >= 2, 1, 0) + jnp.where(z == 3, 1, 0)
            moved_some(rz, ar_sem, n)
            for h in range(nh):
                dd = [jnp.exp(lds[h] * float(tokens * NX * k)) for k in range(5)]
                win[h] = (rz[2, h] + dd[1] * rtot[h] + dd[2] * rz[1, h]
                          + dd[3] * rz[0, h] + dd[4] * rz[3, h])
            w_copy(0).start()

    with jax.named_scope("wwait"):
        moved_some(rw, wr_sem, lax.div(z + 2, 4))

    @pl.when(z == 1)
    def _():
        rw[0] = rz[1]
    @pl.when(z > 0)
    def _():
        for h in range(nh):
            ee = rw[0, h]
            for j in range(1, 4):
                ee = ee + rw[j, h] * jnp.exp(lds[h] * float(tokens * NX * 4 * j))
            cb[h, 0] = ee
            for xx in range(1, NX):
                cb[h, xx] = xp[h, xx] + ee * jnp.exp(lds[h] * float(tokens * xx))
            back(h)

    @pl.when(inner_col)
    def _():
        @pl.when(z > 1)
        def _():
            pl.semaphore_wait(xready.at[0], 1)
        f_copy(0).start()

    for j in range(1, 4):
        @pl.when(z + 2 + 4 * j < nz)
        def _(j=j):
            ready_wait(2 + 4 * j)
            w_copy(j).start()

    @pl.when(jnp.logical_not(early))
    def _():
        local_work()

    def outer_of(h):
        cols = pl.ds(h * DH, DH)
        lead = jnp.exp((r_iota(SUB) + 1.0) * lds[h])
        for xx in range(NX):
            carr[h, pl.ds(xx, rows, stride=NX), :] = rc[h, xx]
        low = carr[h].astype(BF16)
        o = jnp.dot(q_v[:, cols], low, preferred_element_type=F32)
        for i in range(nb):
            rs = pl.ds(i * SUB, SUB)
            inner[h, rs, :] = (inner[h, rs, :]
                               + o[i * SUB:(i + 1) * SUB] * (lead * jnp.exp(lds[h] * float(i * SUB))))

    def norm_of(h):
        cols = pl.ds(h * DH, DH)
        for i in range(nb):
            rs = pl.ds(i * SUB, SUB)
            mix = inner[h, rs, :]
            mean = jnp.sum(mix, axis=1, keepdims=True) * (1.0 / DH)
            cen = mix - mean
            var = jnp.sum(cen * cen, axis=1, keepdims=True) * (1.0 / DH)
            out_ref[rs, cols] = (cen * lax.rsqrt(var + 1e-05) * gs[h, rs, :]).astype(BF16)

    for h in range(nh):
        with jax.named_scope(f"bwait{h}"):
            moved(rc.at[h, pl.ds(0, NX - 1)], br_sem.at[h]).wait()
        with jax.named_scope(f"outer{h}"):
            outer_of(h)
            if h > 0:
                norm_of(h - 1)
    with jax.named_scope("norm"):
        norm_of(nh - 1)

    ahead = (nz - 1 - z).astype(F32)
    mine = []
    for h in range(nh):
        one = lds[h] * float(tokens * NX)
        mine.append(jnp.exp((ahead + 1.0) * one) * cb[h, 0, pl.ds(z, 1), :]
                    + jnp.exp(ahead * one) * rtot[h, pl.ds(z, 1), :])
    with jax.named_scope("fwait"):
        less = jnp.where(first, 0, jnp.where(z == 0, 3, jnp.where(z == 1, 1, 0)))
        moved_some(fr, fr_sem, nz - 1 - z - less)

        @pl.when((z == 0) & jnp.logical_not(first))
        def _():
            moved(er, er_sem).wait()

        @pl.when(z == 1)
        def _():
            moved(er.at[0], er_sem).wait()
    for h in range(nh):
        fin_ref[h] = mine[h] + jnp.sum(fr[:, h, :], axis=0, keepdims=True)

    @pl.when((z <= 1) & jnp.logical_not(first))
    def _():
        for h in range(nh):
            fin_ref[h] = fin_ref[h] + jnp.sum(er[0, :, h, :], axis=0, keepdims=True)

    @pl.when((z == 0) & jnp.logical_not(first))
    def _():
        for h in range(nh):
            for k in range(1, 3):
                fin_ref[h] = fin_ref[h] + jnp.sum(er[k, :, h, :], axis=0, keepdims=True)

    with jax.named_scope("ends"):
        less = jnp.where(last, 2, jnp.where(z >= nz - 3, 1, 0))
        moved_some(fs, fs_sem, z - less + jnp.where(column & (z >= nz - 3), 1, 0))
        late = jnp.where(last, 2 * NX, jnp.where(z >= nz - 3, NX, 0))
        moved_some(fs, es_sem, late - jnp.where(plane & (z >= nz - 3), 1, 0))
        moved(sx.at[pl.ds(0, NX - 1)], xs_sem).wait()
        moved(cb.at[:, pl.ds(0, NX - 1)], bs_sem).wait()
        for slot, d, ok in raw:
            @pl.when(ok)
            def _(slot=slot):
                moved(rtot, as_sem).wait()
        for j in range(4):
            @pl.when(z + 2 + 4 * j < nz)
            def _(j=j):
                moved(win, ws_sem).wait()


def put(a_ref, b_ref, a_out, b_out, sem):
    one = pltpu.make_async_copy(a_ref, a_out, sem.at[0])
    two = pltpu.make_async_copy(b_ref, b_out, sem.at[1])
    one.start()
    two.start()
    one.wait()
    two.wait()


def body(table, nz, queries, key_rows, value_rows, gate_input, norm_gain):
    tokens, width = queries.shape
    nh = width // DH
    rows = DH // NX
    anyspace = pl.BlockSpec(memory_space=pl.ANY)
    vmem = pl.BlockSpec(memory_space=pltpu.VMEM)
    dma = pltpu.SemaphoreType.DMA
    wide = pltpu.VMEM((tokens, width), BF16)
    spread = pltpu.VMEM((NX, nh, rows, DH), F32)
    eight = pltpu.VMEM((nh, NX, rows, DH), F32)
    four = pltpu.VMEM((4, nh, rows, DH), F32)
    one = pltpu.VMEM((nh, rows, DH), F32)
    square = pltpu.VMEM((nh, DH, DH), F32)
    tall = pltpu.VMEM((nh, tokens, DH), F32)
    few = pltpu.VMEM((3, NX, pl.next_power_of_2(nh), DH), F32)
    line = pltpu.VMEM((nz, pl.next_power_of_2(nh), DH), F32)
    retained, final = pl.pallas_call(
        functools.partial(kernel, table, nz),
        out_shape=(pltpu.VMEM((tokens, width), BF16), pltpu.VMEM((nh, 1, DH), F32)),
        in_specs=[anyspace] * 5,
        out_specs=(vmem, vmem),
        scratch_shapes=[
            wide, wide, wide, wide, pltpu.VMEM((width,), F32),
            square, spread, spread, eight, one, four, one, four, eight, eight, square, tall, tall, line, line, pltpu.VMEM((2, NX, pl.next_power_of_2(nh), DH), F32), few,
            dma((nh,)), dma((3,)), dma, dma, dma, dma, dma, dma, dma, dma((nh,)), dma, dma, dma, dma,
            pltpu.SemaphoreType.REGULAR((6,)), pltpu.SemaphoreType.REGULAR((NX,)),
        ],
        compiler_params=pltpu.CompilerParams(collective_id=0, has_side_effects=True),
        name="retention",
    )(queries, key_rows, value_rows, gate_input, norm_gain)
    retained, final = (pltpu.with_memory_space_constraint(a, pltpu.VMEM) for a in (retained, final))
    retained, final = pl.pallas_call(
        put,
        out_shape=(jax.ShapeDtypeStruct((tokens, width), BF16), jax.ShapeDtypeStruct((nh, 1, DH), F32)),
        in_specs=[vmem, vmem],
        out_specs=(anyspace, anyspace),
        scratch_shapes=[dma((2,))],
        name="put",
    )(retained, final)
    return retained, final.reshape(1, nh, DH)


def solution(mesh):
    table = log_decays(mesh.shape["head"])
    rows = ("grp", "seq")
    placed = (P(rows, "head"),) * 4 + (P("head"),)
    return jax.shard_map(
        functools.partial(body, table, mesh.shape["seq"] // NX),
        mesh=mesh,
        in_specs=placed,
        out_specs=(P(rows, "head"), P(rows, "head", None)),
        check_vma=False,
    )
```

```python
import functools
import math

import jax
import jax.numpy as jnp
import numpy as np
from jax import lax
from jax.experimental import pallas as pl
from jax.experimental.pallas import tpu as pltpu
from jax.sharding import PartitionSpec as P

ALL_HEADS = 10
HEADS = 6
DH = 128
NX = 8
MESH = pl.DeviceIdType.MESH
F32 = jnp.float32
BF16 = jnp.bfloat16
SUB = 128


def log_decays(shards):
    per = HEADS // shards
    ids = ALL_HEADS - HEADS + np.arange(HEADS, dtype=np.float64)
    table = np.log1p(-np.exp2(-5.0 - ids)).reshape(shards, per)
    return [[float(np.float32(v)) for v in row] for row in table]


def kernel(
    table, nz,
    q_hbm, k_hbm, v_hbm, g_hbm, gain_hbm,
    out_ref, fin_ref,
    q_v, k_v, v_v, g_v, gain_v,
    st, sx, rx, xp, rtot, rz, win, rw, cb, rc, carr, inner, gs, fs, fr, es, er, r2, cb2,
    kv_sem, in_sem, xs_sem, xr_sem, ar_sem, wr_sem, br_sem, fr_sem, er_sem, r2_sem, ready, xready, two,
):
    tokens = q_v.shape[0]
    nh = q_v.shape[1] // DH
    rows = DH // NX
    nb = tokens // SUB
    scale = DH ** (-0.5)
    me = lax.axis_index("seq")
    z = lax.div(me, NX)
    x = lax.rem(me, NX)
    hd = lax.axis_index("head")
    plane = (lax.axis_index("grp") == 0) & (hd == 0)
    column = plane & (x == 0)
    first = column & (z == 0)
    row0 = plane & (z == 0)
    row1 = plane & (z == 1)
    inner_col = column & (z > 0) & (z < nz - 2)
    last_c = nz - 3

    lds = []
    for h in range(nh):
        ld = jnp.float32(table[0][h])
        for s in range(1, len(table)):
            ld = jnp.where(hd == s, jnp.float32(table[s][h]), ld)
        lds.append(ld)

    def at(zz, xx):
        return {"seq": zz * NX + xx}

    def xwrap(d):
        return lax.rem(x + (d % NX), NX)

    def r_iota(n):
        return lax.broadcasted_iota(jnp.int32, (n, DH), 0).astype(F32)

    def load(src, dst, h):
        cols = pl.ds(h * DH, DH)
        return pltpu.make_async_copy(src.at[:, cols], dst.at[:, cols], kv_sem.at[h])

    def kv_wait(h):
        two = pl.ds(0, 2 * DH)
        pltpu.make_async_copy(k_hbm.at[:, two], k_v.at[:, two], kv_sem.at[h]).wait()

    whole = (
        pltpu.make_async_copy(q_hbm, q_v, in_sem.at[0]),
        pltpu.make_async_copy(g_hbm, g_v, in_sem.at[1]),
        pltpu.make_async_copy(gain_hbm, gain_v, in_sem.at[2]),
    )

    for h in range(nh):
        load(k_hbm, k_v, h).start()
        load(v_hbm, v_v, h).start()

    def key_of(xx):
        k = jnp.where(xx < NX // 2, xx, 3 * NX // 2 - 1 - xx)
        k = jnp.where(xx == NX // 2, NX - 2, jnp.where(xx == NX // 2 + 1, NX - 1, k))
        return jnp.where((xx == 0) & (z == 0) & plane, NX, k)

    def x_of(k):
        if k == NX:
            return 0
        if k >= NX - 2:
            return k - NX // 2 + 2
        return k if k < NX // 2 else 3 * NX // 2 - 1 - k

    key = key_of(x)

    barrier = pltpu.get_barrier_semaphore()
    for d in range(1, NX):
        @pl.when(key_of(xwrap(d)) > key)
        def _(d=d):
            pl.semaphore_signal(barrier, inc=1, device_id=at(z, xwrap(d)), device_id_type=MESH)
    last = z == nz - 1
    express = ((0, 0), (1, 0), (0, 1), (0, 2), (1, 1))

    def tell_later():
        for zz in range(1, nz):
            ok = z < zz
            if zz < nz - 2:
                ok = ok & jnp.logical_not(first)

            @pl.when(ok)
            def _(zz=zz):
                pl.semaphore_signal(barrier, inc=1, device_id=at(zz, x), device_id_type=MESH)

    @pl.when(z > 0)
    def _():
        tell_later()

    @pl.when(inner_col)
    def _():
        pl.semaphore_signal(barrier, inc=1, device_id=at(0, x), device_id_type=MESH)

    @pl.when(row1 & (x > 0))
    def _():
        pl.semaphore_signal(barrier, inc=1, device_id=at(0, 0), device_id_type=MESH)
    owed = jnp.where(plane, NX - 1 - jnp.where(x == 0, 0, 1), NX - 1)
    count = key + z + jnp.where(z >= nz - 2, owed + NX - 1, jnp.where((z == nz - 3) | row1, owed, 0))
    count = jnp.where((z == 0) & plane, key - 1, count)
    count = jnp.where(first, 2 * NX + nz - 5, count) - jnp.where(inner_col, 1, 0)
    for h in range(nh):
        inner[h] = jnp.exp((tokens - 1 - r_iota(tokens)) * lds[h]) * scale
    with jax.named_scope("barrier"):
        @pl.when(count > 0)
        def _():
            pl.semaphore_wait(barrier, count)
    for d in range(1, NX):
        @pl.when(key_of(xwrap(d)) < key)
        def _(d=d):
            pl.semaphore_signal(xready.at[NX - d], inc=1, device_id=at(z, xwrap(d)), device_id_type=MESH)

    @pl.when(z == 0)
    def _():
        tell_later()

    @pl.when(first)
    def _():
        for zz in range(1, nz - 2):
            pl.semaphore_signal(xready.at[0], inc=1, device_id=at(zz, x), device_id_type=MESH)
    @pl.when(row0 & jnp.logical_not(first))
    def _():
        for d in range(1, NX):
            pl.semaphore_signal(barrier, inc=1, device_id=at(1, xwrap(d)), device_id_type=MESH)
    for to in range(1, NX):
        @pl.when(row1)
        def _(to=to):
            pl.semaphore_signal(two, inc=1, device_id=at(0, to), device_id_type=MESH)
    for j, k in express:
        @pl.when((z == j) & jnp.logical_not(first))
        def _(k=k):
            for d in range(1, NX):
                pl.semaphore_signal(barrier, inc=1, device_id=at(nz - 1 - k, xwrap(d)), device_id_type=MESH)
    for c in whole:
        c.start()

    def x_copy(to):
        return pltpu.make_async_remote_copy(
            sx.at[to], rx.at[x], xs_sem, xr_sem,
            device_id=at(z, to), device_id_type=MESH)

    def b_copy(h, d):
        return b_to(h, xwrap(d))

    def b_to(h, to):
        return pltpu.make_async_remote_copy(
            cb.at[h, to], rc.at[h, x], xs_sem, br_sem.at[h],
            device_id=at(z, to), device_id_type=MESH)

    def d_copy(to):
        return pltpu.make_async_remote_copy(
            sx.at[to], r2.at[x], xs_sem, r2_sem,
            device_id=at(1, to), device_id_type=MESH)

    def s_copy(h, to):
        return pltpu.make_async_remote_copy(
            cb2.at[h, to], rc.at[h, 0], xs_sem, br_sem.at[h],
            device_id=at(0, to), device_id_type=MESH)

    def e_copy(j, k, to):
        return pltpu.make_async_remote_copy(
            es.at[j, to], er.at[k, x], xs_sem, er_sem,
            device_id=at(j, to), device_id_type=MESH)

    def moved(ref, sem):
        return pltpu.make_async_copy(ref, ref, sem)

    def moved_some(ref, sem, n):
        for m in range(1, ref.shape[0] + 1):
            @pl.when(n == m)
            def _(m=m):
                moved(ref.at[pl.ds(0, m)], sem).wait()

    raw = (
        (1, 1, (z <= last_c - 1) & jnp.logical_not(row0)),
        (0, 2, z <= last_c - 2),
        (3, 3, z == 0),
        (2, -1, (z >= 1) & (z <= last_c + 1)),
    )
    def a_copy(slot, d):
        return pltpu.make_async_remote_copy(
            rtot, rz.at[slot], xs_sem, ar_sem,
            device_id=at(z + d, x), device_id_type=MESH)

    def w_copy(j):
        return pltpu.make_async_remote_copy(
            win, rw.at[j], xs_sem, wr_sem,
            device_id=at(z + (2 + 4 * j), x), device_id_type=MESH)

    def f_copy(zz):
        return pltpu.make_async_remote_copy(
            fs.at[zz], fr.at[z], xs_sem, fr_sem,
            device_id=at(zz, x), device_id_type=MESH)

    readies = ((1, (z >= 1) & (z <= last_c)), (2, z >= 2), (3, z == 3)) + tuple(
        (2 + 4 * j, z >= 2 + 4 * j) for j in range(1, 4))
    slot_of = {d: i for i, (d, _) in enumerate(readies)}

    def ready_wait(d):
        @pl.when(jnp.logical_not(first) if d < nz - 2 else z >= 0)
        def _():
            pl.semaphore_wait(ready.at[slot_of[d]], 1)

    far = (4, 3, 5, 2, 6, 1, 7)

    with jax.named_scope("load"):
        for h in range(nh):
            kv_wait(h)
    with jax.named_scope("state"):
        for h in range(nh):
            cols = pl.ds(h * DH, DH)
            kd = (k_v[:, cols].astype(F32) * inner[h]).astype(BF16)
            st[h] = lax.dot_general(kd, v_v[:, cols], (((0,), (0,)), ((), ())), preferred_element_type=F32)
            for xx in range(NX):
                sx[xx, h] = st[h, pl.ds(xx, rows, stride=NX), :]

    for r in range(nh, es.shape[2]):
        es[:, :, r, :] = jnp.zeros((2, NX, DH), F32)

    @pl.when(z >= nz - 3)
    def _():
        for h in range(nh):
            w = (NX - 1 - x + NX * (nz - 1 - z)).astype(F32) * (lds[h] * float(tokens))
            for j in range(2):
                es[j, :, h, :] = st[h, pl.ds(j * NX, NX), :] * jnp.exp(w)
        for j, k in express:
            for d in far + (0,):
                to = xwrap(d)
                ok = z == nz - 1 - k
                if j == 0:
                    ok = ok & jnp.logical_not(plane & (to == 0))

                @pl.when(ok)
                def _(j=j, k=k, to=to):
                    e_copy(j, k, to).start()

    @pl.when(first)
    def _():
        for d in far:
            x_copy(xwrap(d)).start()
            d_copy(xwrap(d)).start()
        d_copy(x).start()
    for d in far:
        @pl.when((key_of(xwrap(d)) < key) & jnp.logical_not(first))
        def _(d=d):
            x_copy(xwrap(d)).start()
    for d, ok in readies:
        @pl.when(ok & jnp.logical_not((plane if d == 1 else inner_col) & (z == d)))
        def _(d=d):
            pl.semaphore_signal(ready.at[slot_of[d]], inc=1, device_id=at(z - d, x), device_id_type=MESH)

    zero = jnp.zeros((nh, rows, DH), F32)

    @pl.when(z < 2)
    def _():
        rz[0] = zero

    @pl.when(z < 1)
    def _():
        rz[1] = zero

    @pl.when(z != 3)
    def _():
        rz[3] = zero

    for j in range(1, 4):
        @pl.when((z > 0) & (z < 2 + 4 * j))
        def _(j=j):
            rw[j] = zero

    for zz in range(nz):
        ok = zz <= z
        for j, k in express:
            if zz == nz - 1 - k:
                ok = ok | ((z == j) & jnp.logical_not(first))

        @pl.when(ok)
        def _(zz=zz):
            fr[zz] = jnp.zeros(fr.shape[1:], F32)
    for r in range(nh, fs.shape[1]):
        fs[:, r, :] = jnp.zeros((nz, DH), F32)
    rx[x] = sx[x]

    @pl.when(row0 & jnp.logical_not(first))
    def _():
        pl.semaphore_wait(two, NX)
        for d in far + (0,):
            d_copy(xwrap(d)).start()
    with jax.named_scope("xready"):
        for k in range(1, NX + 1):
            to = x_of(k)

            @pl.when((key < k) & (z == 0) & plane if k == NX else key < k)
            def _(to=to):
                pl.semaphore_wait(xready.at[lax.rem(to + NX - x, NX)], 1)
                x_copy(to).start()

    ri = lax.broadcasted_iota(jnp.int32, (SUB, SUB), 0)
    ci = lax.broadcasted_iota(jnp.int32, (SUB, SUB), 1)

    def inner_of(h):
        cols = pl.ds(h * DH, DH)
        base = jnp.exp((ri - ci).astype(F32) * lds[h]) * scale
        for i in range(nb):
            qi = q_v[pl.ds(i * SUB, SUB), cols]
            parts = []
            for j in range(i + 1):
                s = lax.dot_general(qi, k_v[pl.ds(j * SUB, SUB), cols], (((1,), (1,)), ((), ())),
                                    preferred_element_type=F32)
                if j == i:
                    w = jnp.where(ri >= ci, s * base, 0.0)
                else:
                    w = s * (base * jnp.exp(lds[h] * float((i - j) * SUB)))
                parts.append(w.astype(BF16))
            w = parts[0] if i == 0 else jnp.concatenate(parts, axis=1)
            inner[h, pl.ds(i * SUB, SUB), :] = jnp.dot(
                w, v_v[pl.ds(0, (i + 1) * SUB), cols], preferred_element_type=F32)

    def gate_of(h):
        cols = pl.ds(h * DH, DH)
        gain = gain_v[pl.ds(h * DH, DH)].reshape(1, DH)
        u = g_v[:, cols].astype(F32)
        gs[h] = u / (1.0 + jnp.exp(-u)) * gain

    def local_work():
        with jax.named_scope("local"):
            for c in whole:
                c.wait()
            for h in range(nh):
                inner_of(h)
                gate_of(h)

    with jax.named_scope("xwait"):
        moved(rx.at[pl.ds(0, NX - 1)], xr_sem).wait()
    with jax.named_scope("prefix"):
        for h in range(nh):
            d1 = jnp.exp(lds[h] * float(tokens))
            acc = rx[0, h]
            for xx in range(1, NX):
                xp[h, xx] = acc
                acc = acc * d1 + rx[xx, h]
            rtot[h] = acc
            fs[:, h, :] = acc * jnp.exp((nz - 1 - z).astype(F32) * (lds[h] * float(tokens * NX)))

    for zz in range(nz - 1):
        ok = z > zz
        for j, k in express:
            if zz == j:
                ok = ok & ((z != nz - 1 - k) | column if j == 0 else z != nz - 1 - k)
        if zz == 0:
            ok = ok & jnp.logical_not(inner_col)

        @pl.when(ok)
        def _(zz=zz):
            f_copy(zz).start()
    for slot, d, ok in raw:
        @pl.when(ok)
        def _(slot=slot, d=d):
            if d > 0:
                ready_wait(d)
            else:
                @pl.when(column & (z == 1))
                def _():
                    pl.semaphore_wait(xready.at[0], 1)
            a_copy(slot, d).start()

    def back(h):
        for d in far:
            b_copy(h, d).start()
        rc[h, x] = cb[h, x]

    @pl.when(z == 0)
    def _():
        for h in range(nh):
            cb[h, 0] = jnp.zeros((rows, DH), F32)
            for xx in range(1, NX):
                cb[h, xx] = xp[h, xx]
            rc[h, x] = cb[h, x]
        for to in (1, 2, 3, 7, 6, 5, 4, 0):
            @pl.when((x != to) & jnp.logical_not(first))
            def _(to=to):
                for h in range(nh):
                    b_to(h, to).start()

    early = (z >= 1) & (z < nz // 2)

    @pl.when(early)
    def _():
        local_work()

    @pl.when(row1)
    def _():
        with jax.named_scope("row0"):
            moved(r2, r2_sem).wait()
            for h in range(nh):
                d1 = jnp.exp(lds[h] * float(tokens))
                acc = r2[0, h]
                for xx in range(1, NX):
                    cb2[h, xx] = acc
                    acc = acc * d1 + r2[xx, h]
                rz[1, h] = acc

                @pl.when(x == 0)
                def _(h=h):
                    for to in (4, 5, 3, 6, 2, 7, 1):
                        s_copy(h, to).start()

    @pl.when(z <= last_c)
    def _():
        with jax.named_scope("windows"):
            @pl.when(z > last_c - 2)
            def _():
                ready_wait(2)
            n = 1 + jnp.where((z >= 1) & jnp.logical_not(row1), 1, 0) + jnp.where(z >= 2, 1, 0) + jnp.where(z == 3, 1, 0)
            moved_some(rz, ar_sem, n)
            for h in range(nh):
                dd = [jnp.exp(lds[h] * float(tokens * NX * k)) for k in range(5)]
                win[h] = (rz[2, h] + dd[1] * rtot[h] + dd[2] * rz[1, h]
                          + dd[3] * rz[0, h] + dd[4] * rz[3, h])
            w_copy(0).start()

    with jax.named_scope("wwait"):
        moved_some(rw, wr_sem, lax.div(z + 2, 4))

    @pl.when(z == 1)
    def _():
        rw[0] = rz[1]
    @pl.when(z > 0)
    def _():
        for h in range(nh):
            ee = rw[0, h]
            for j in range(1, 4):
                ee = ee + rw[j, h] * jnp.exp(lds[h] * float(tokens * NX * 4 * j))
            cb[h, 0] = ee
            for xx in range(1, NX):
                cb[h, xx] = xp[h, xx] + ee * jnp.exp(lds[h] * float(tokens * xx))
            back(h)

    @pl.when(inner_col)
    def _():
        @pl.when(z > 1)
        def _():
            pl.semaphore_wait(xready.at[0], 1)
        f_copy(0).start()

    for j in range(1, 4):
        @pl.when(z + 2 + 4 * j < nz)
        def _(j=j):
            ready_wait(2 + 4 * j)
            w_copy(j).start()

    @pl.when(jnp.logical_not(early))
    def _():
        local_work()

    def outer_of(h):
        cols = pl.ds(h * DH, DH)
        lead = jnp.exp((r_iota(SUB) + 1.0) * lds[h])
        for xx in range(NX):
            carr[h, pl.ds(xx, rows, stride=NX), :] = rc[h, xx]
        low = carr[h].astype(BF16)
        o = jnp.dot(q_v[:, cols], low, preferred_element_type=F32)
        for i in range(nb):
            rs = pl.ds(i * SUB, SUB)
            inner[h, rs, :] = (inner[h, rs, :]
                               + o[i * SUB:(i + 1) * SUB] * (lead * jnp.exp(lds[h] * float(i * SUB))))

    def norm_of(h):
        cols = pl.ds(h * DH, DH)
        for i in range(nb):
            rs = pl.ds(i * SUB, SUB)
            mix = inner[h, rs, :]
            mean = jnp.sum(mix, axis=1, keepdims=True) * (1.0 / DH)
            cen = mix - mean
            var = jnp.sum(cen * cen, axis=1, keepdims=True) * (1.0 / DH)
            out_ref[rs, cols] = (cen * lax.rsqrt(var + 1e-05) * gs[h, rs, :]).astype(BF16)

    for h in range(nh):
        with jax.named_scope(f"bwait{h}"):
            moved(rc.at[h, pl.ds(0, NX - 1)], br_sem.at[h]).wait()
        with jax.named_scope(f"outer{h}"):
            outer_of(h)
            if h > 0:
                norm_of(h - 1)
    with jax.named_scope("norm"):
        norm_of(nh - 1)

    ahead = (nz - 1 - z).astype(F32)
    mine = []
    for h in range(nh):
        one = lds[h] * float(tokens * NX)
        mine.append(jnp.exp((ahead + 1.0) * one) * cb[h, 0, pl.ds(z, 1), :]
                    + jnp.exp(ahead * one) * rtot[h, pl.ds(z, 1), :])
    with jax.named_scope("fwait"):
        less = jnp.where(first, 0, jnp.where(z == 0, 3, jnp.where(z == 1, 2, 0)))
        moved_some(fr, fr_sem, nz - 1 - z - less)

        @pl.when((z == 0) & jnp.logical_not(first))
        def _():
            moved(er, er_sem).wait()

        @pl.when(z == 1)
        def _():
            moved(er.at[pl.ds(0, 2)], er_sem).wait()
    for h in range(nh):
        fin_ref[h] = mine[h] + jnp.sum(fr[:, h, :], axis=0, keepdims=True)

    @pl.when((z <= 1) & jnp.logical_not(first))
    def _():
        for h in range(nh):
            for k in range(2):
                fin_ref[h] = fin_ref[h] + jnp.sum(er[k, :, h, :], axis=0, keepdims=True)

    @pl.when((z == 0) & jnp.logical_not(first))
    def _():
        for h in range(nh):
            fin_ref[h] = fin_ref[h] + jnp.sum(er[2, :, h, :], axis=0, keepdims=True)

    with jax.named_scope("ends"):
        less = jnp.where(z >= nz - 2, 2, jnp.where(z == nz - 3, 1, 0))
        moved_some(fs, xs_sem, z - less + jnp.where(column & (z >= nz - 3), 1, 0))
        late = jnp.where(z >= nz - 2, 2 * NX, jnp.where(z == nz - 3, NX, 0))
        moved_some(fs, xs_sem, late - jnp.where(plane & (z >= nz - 3), 1, 0))
        moved(sx.at[pl.ds(0, NX - 1)], xs_sem).wait()

        @pl.when(row0)
        def _():
            moved(sx, xs_sem).wait()

        @pl.when(jnp.logical_not(first))
        def _():
            moved(cb.at[:, pl.ds(0, NX - 1)], xs_sem).wait()

        @pl.when(row1 & (x == 0))
        def _():
            moved(cb2.at[:, pl.ds(0, NX - 1)], xs_sem).wait()
        for slot, d, ok in raw:
            @pl.when(ok)
            def _(slot=slot):
                moved(rtot, xs_sem).wait()
        for j in range(4):
            @pl.when(z + 2 + 4 * j < nz)
            def _(j=j):
                moved(win, xs_sem).wait()


def put(a_ref, b_ref, a_out, b_out, sem):
    one = pltpu.make_async_copy(a_ref, a_out, sem.at[0])
    two = pltpu.make_async_copy(b_ref, b_out, sem.at[1])
    one.start()
    two.start()
    one.wait()
    two.wait()


def body(table, nz, queries, key_rows, value_rows, gate_input, norm_gain):
    tokens, width = queries.shape
    nh = width // DH
    rows = DH // NX
    anyspace = pl.BlockSpec(memory_space=pl.ANY)
    vmem = pl.BlockSpec(memory_space=pltpu.VMEM)
    dma = pltpu.SemaphoreType.DMA
    wide = pltpu.VMEM((tokens, width), BF16)
    spread = pltpu.VMEM((NX, nh, rows, DH), F32)
    eight = pltpu.VMEM((nh, NX, rows, DH), F32)
    four = pltpu.VMEM((4, nh, rows, DH), F32)
    one = pltpu.VMEM((nh, rows, DH), F32)
    square = pltpu.VMEM((nh, DH, DH), F32)
    tall = pltpu.VMEM((nh, tokens, DH), F32)
    few = pltpu.VMEM((3, NX, pl.next_power_of_2(nh), DH), F32)
    line = pltpu.VMEM((nz, pl.next_power_of_2(nh), DH), F32)
    retained, final = pl.pallas_call(
        functools.partial(kernel, table, nz),
        out_shape=(pltpu.VMEM((tokens, width), BF16), pltpu.VMEM((nh, 1, DH), F32)),
        in_specs=[anyspace] * 5,
        out_specs=(vmem, vmem),
        scratch_shapes=[
            wide, wide, wide, wide, pltpu.VMEM((width,), F32),
            square, spread, spread, eight, one, four, one, four, eight, eight, square, tall, tall, line, line,
            pltpu.VMEM((2, NX, pl.next_power_of_2(nh), DH), F32), few, spread, eight,
            dma((nh,)), dma((3,)), dma, dma, dma, dma, dma((nh,)), dma, dma, dma,
            pltpu.SemaphoreType.REGULAR((6,)), pltpu.SemaphoreType.REGULAR((NX,)),
            pltpu.SemaphoreType.REGULAR,
        ],
        compiler_params=pltpu.CompilerParams(collective_id=0, has_side_effects=True),
        name="retention",
    )(queries, key_rows, value_rows, gate_input, norm_gain)
    retained, final = (pltpu.with_memory_space_constraint(a, pltpu.VMEM) for a in (retained, final))
    retained, final = pl.pallas_call(
        put,
        out_shape=(jax.ShapeDtypeStruct((tokens, width), BF16), jax.ShapeDtypeStruct((nh, 1, DH), F32)),
        in_specs=[vmem, vmem],
        out_specs=(anyspace, anyspace),
        scratch_shapes=[dma((2,))],
        name="put",
    )(retained, final)
    return retained, final.reshape(1, nh, DH)


def solution(mesh):
    table = log_decays(mesh.shape["head"])
    rows = ("grp", "seq")
    placed = (P(rows, "head"),) * 4 + (P("head"),)
    return jax.shard_map(
        functools.partial(body, table, mesh.shape["seq"] // NX),
        mesh=mesh,
        in_specs=placed,
        out_specs=(P(rows, "head"), P(rows, "head", None)),
        check_vma=False,
    )
```

```python
import functools
import math

import jax
import jax.numpy as jnp
import numpy as np
from jax import lax
from jax.experimental import pallas as pl
from jax.experimental.pallas import tpu as pltpu
from jax.sharding import PartitionSpec as P

ALL_HEADS = 10
HEADS = 6
DH = 128
NX = 8
MESH = pl.DeviceIdType.MESH
F32 = jnp.float32
BF16 = jnp.bfloat16
SUB = 128


def log_decays(shards):
    per = HEADS // shards
    ids = ALL_HEADS - HEADS + np.arange(HEADS, dtype=np.float64)
    table = np.log1p(-np.exp2(-5.0 - ids)).reshape(shards, per)
    return [[float(np.float32(v)) for v in row] for row in table]


def kernel(
    table, nz,
    q_hbm, k_hbm, v_hbm, g_hbm, gain_hbm,
    out_ref, fin_ref,
    q_v, k_v, v_v, g_v, gain_v,
    st, sx, rx, xp, rtot, rz, win, rw, cb, rc, carr, inner, gs, fs, fr, es, er, r2, cb2,
    kv_sem, in_sem, xs_sem, xr_sem, ar_sem, wr_sem, br_sem, fr_sem, er_sem, r2_sem, ready, xready, two,
):
    tokens = q_v.shape[0]
    nh = q_v.shape[1] // DH
    rows = DH // NX
    nb = tokens // SUB
    scale = DH ** (-0.5)
    me = lax.axis_index("seq")
    z = lax.div(me, NX)
    x = lax.rem(me, NX)
    hd = lax.axis_index("head")
    plane = (lax.axis_index("grp") == 0) & (hd == 0)
    column = plane & (x == 0)
    first = column & (z == 0)
    row0 = plane & (z == 0)
    row1 = plane & (z == 1)
    inner_col = column & (z > 0) & (z < nz - 2)
    last_c = nz - 3

    lds = []
    for h in range(nh):
        ld = jnp.float32(table[0][h])
        for s in range(1, len(table)):
            ld = jnp.where(hd == s, jnp.float32(table[s][h]), ld)
        lds.append(ld)

    def at(zz, xx):
        return {"seq": zz * NX + xx}

    def xwrap(d):
        return lax.rem(x + (d % NX), NX)

    def r_iota(n):
        return lax.broadcasted_iota(jnp.int32, (n, DH), 0).astype(F32)

    def load(src, dst, h):
        cols = pl.ds(h * DH, DH)
        return pltpu.make_async_copy(src.at[:, cols], dst.at[:, cols], kv_sem.at[h])

    def kv_wait(h):
        two = pl.ds(0, 2 * DH)
        pltpu.make_async_copy(k_hbm.at[:, two], k_v.at[:, two], kv_sem.at[h]).wait()

    whole = (
        pltpu.make_async_copy(q_hbm, q_v, in_sem.at[0]),
        pltpu.make_async_copy(g_hbm, g_v, in_sem.at[1]),
        pltpu.make_async_copy(gain_hbm, gain_v, in_sem.at[2]),
    )

    for h in range(nh):
        load(k_hbm, k_v, h).start()
        load(v_hbm, v_v, h).start()

    def key_of(xx):
        k = jnp.where(xx < NX // 2, xx, 3 * NX // 2 - 1 - xx)
        k = jnp.where(xx == NX // 2, NX - 2, jnp.where(xx == NX // 2 + 1, NX - 1, k))
        return jnp.where((xx == 0) & (z == 0) & plane, NX, k)

    def x_of(k):
        if k == NX:
            return 0
        if k >= NX - 2:
            return k - NX // 2 + 2
        return k if k < NX // 2 else 3 * NX // 2 - 1 - k

    key = key_of(x)

    barrier = pltpu.get_barrier_semaphore()
    for d in range(1, NX):
        @pl.when(key_of(xwrap(d)) > key)
        def _(d=d):
            pl.semaphore_signal(barrier, inc=1, device_id=at(z, xwrap(d)), device_id_type=MESH)
    last = z == nz - 1
    express = ((0, 0), (1, 0), (0, 1), (0, 2), (1, 1))

    def tell_later():
        for zz in range(1, nz):
            ok = z < zz
            if zz < nz - 2:
                ok = ok & jnp.logical_not(first)

            @pl.when(ok)
            def _(zz=zz):
                pl.semaphore_signal(barrier, inc=1, device_id=at(zz, x), device_id_type=MESH)

    @pl.when(z > 0)
    def _():
        tell_later()

    @pl.when(inner_col)
    def _():
        pl.semaphore_signal(barrier, inc=1, device_id=at(0, x), device_id_type=MESH)

    @pl.when(row1 & (x > 0))
    def _():
        pl.semaphore_signal(barrier, inc=1, device_id=at(0, 0), device_id_type=MESH)
    owed = jnp.where(plane, NX - 1 - jnp.where(x == 0, 0, 1), NX - 1)
    count = key + z + jnp.where(z >= nz - 2, owed + NX - 1, jnp.where((z == nz - 3) | row1, owed, 0))
    count = jnp.where((z == 0) & plane, key - 1, count)
    count = jnp.where(first, 2 * NX + nz - 5, count) - jnp.where(inner_col, 1, 0)
    for h in range(nh):
        inner[h] = jnp.exp((tokens - 1 - r_iota(tokens)) * lds[h]) * scale
    with jax.named_scope("barrier"):
        @pl.when(count > 0)
        def _():
            pl.semaphore_wait(barrier, count)
    for d in range(1, NX):
        @pl.when(key_of(xwrap(d)) < key)
        def _(d=d):
            pl.semaphore_signal(xready.at[NX - d], inc=1, device_id=at(z, xwrap(d)), device_id_type=MESH)

    @pl.when(z == 0)
    def _():
        tell_later()

    @pl.when(first)
    def _():
        for zz in range(1, nz - 2):
            pl.semaphore_signal(xready.at[0], inc=1, device_id=at(zz, x), device_id_type=MESH)
    @pl.when(row0 & jnp.logical_not(first))
    def _():
        for d in range(1, NX):
            pl.semaphore_signal(barrier, inc=1, device_id=at(1, xwrap(d)), device_id_type=MESH)
    for to in range(1, NX):
        @pl.when(row1)
        def _(to=to):
            pl.semaphore_signal(two, inc=1, device_id=at(0, to), device_id_type=MESH)
    for j, k in express:
        @pl.when((z == j) & jnp.logical_not(first))
        def _(k=k):
            for d in range(1, NX):
                pl.semaphore_signal(barrier, inc=1, device_id=at(nz - 1 - k, xwrap(d)), device_id_type=MESH)
    def x_copy(to):
        return pltpu.make_async_remote_copy(
            sx.at[to], rx.at[x], xs_sem, xr_sem,
            device_id=at(z, to), device_id_type=MESH)

    def b_copy(h, d):
        return b_to(h, xwrap(d))

    def b_to(h, to):
        return pltpu.make_async_remote_copy(
            cb.at[h, to], rc.at[h, x], xs_sem, br_sem.at[h],
            device_id=at(z, to), device_id_type=MESH)

    def d_copy(to):
        return pltpu.make_async_remote_copy(
            sx.at[to], r2.at[x], xs_sem, r2_sem,
            device_id=at(1, to), device_id_type=MESH)

    def s_copy(h, to):
        return pltpu.make_async_remote_copy(
            cb2.at[h, to], rc.at[h, 0], xs_sem, br_sem.at[h],
            device_id=at(0, to), device_id_type=MESH)

    def e_copy(j, k, to):
        return pltpu.make_async_remote_copy(
            es.at[j, to], er.at[k, x], xs_sem, er_sem,
            device_id=at(j, to), device_id_type=MESH)

    def moved(ref, sem):
        return pltpu.make_async_copy(ref, ref, sem)

    def moved_some(ref, sem, n):
        for m in range(1, ref.shape[0] + 1):
            @pl.when(n == m)
            def _(m=m):
                moved(ref.at[pl.ds(0, m)], sem).wait()

    raw = (
        (1, 1, (z <= last_c - 1) & jnp.logical_not(row0)),
        (0, 2, z <= last_c - 2),
        (3, 3, z == 0),
        (2, -1, (z >= 1) & (z <= last_c + 1)),
    )
    def a_copy(slot, d):
        return pltpu.make_async_remote_copy(
            rtot, rz.at[slot], xs_sem, ar_sem,
            device_id=at(z + d, x), device_id_type=MESH)

    def w_copy(j):
        return pltpu.make_async_remote_copy(
            win, rw.at[j], xs_sem, wr_sem,
            device_id=at(z + (2 + 4 * j), x), device_id_type=MESH)

    def f_copy(zz):
        return pltpu.make_async_remote_copy(
            fs.at[zz], fr.at[z], xs_sem, fr_sem,
            device_id=at(zz, x), device_id_type=MESH)

    readies = ((1, (z >= 1) & (z <= last_c)), (2, z >= 2), (3, z == 3)) + tuple(
        (2 + 4 * j, z >= 2 + 4 * j) for j in range(1, 4))
    slot_of = {d: i for i, (d, _) in enumerate(readies)}

    def ready_wait(d):
        @pl.when(jnp.logical_not(first) if d < nz - 2 else z >= 0)
        def _():
            pl.semaphore_wait(ready.at[slot_of[d]], 1)

    far = (4, 3, 5, 2, 6, 1, 7)

    with jax.named_scope("load"):
        for h in range(nh):
            kv_wait(h)
    with jax.named_scope("state"):
        for h in range(nh):
            cols = pl.ds(h * DH, DH)
            kd = (k_v[:, cols].astype(F32) * inner[h]).astype(BF16)
            st[h] = lax.dot_general(kd, v_v[:, cols], (((0,), (0,)), ((), ())), preferred_element_type=F32)
            for xx in range(NX):
                sx[xx, h] = st[h, pl.ds(xx, rows, stride=NX), :]

    for r in range(nh, es.shape[2]):
        es[:, :, r, :] = jnp.zeros((2, NX, DH), F32)

    @pl.when(z >= nz - 3)
    def _():
        for h in range(nh):
            w = (NX - 1 - x + NX * (nz - 1 - z)).astype(F32) * (lds[h] * float(tokens))
            for j in range(2):
                es[j, :, h, :] = st[h, pl.ds(j * NX, NX), :] * jnp.exp(w)
        for j, k in express:
            for d in far + (0,):
                to = xwrap(d)
                ok = z == nz - 1 - k
                if j == 0:
                    ok = ok & jnp.logical_not(plane & (to == 0))

                @pl.when(ok)
                def _(j=j, k=k, to=to):
                    e_copy(j, k, to).start()

    @pl.when(first)
    def _():
        for d in far:
            x_copy(xwrap(d)).start()
            d_copy(xwrap(d)).start()
        d_copy(x).start()
    for d in far:
        @pl.when((key_of(xwrap(d)) < key) & jnp.logical_not(first))
        def _(d=d):
            x_copy(xwrap(d)).start()
    for d, ok in readies:
        @pl.when(ok & jnp.logical_not((plane if d == 1 else inner_col) & (z == d)))
        def _(d=d):
            pl.semaphore_signal(ready.at[slot_of[d]], inc=1, device_id=at(z - d, x), device_id_type=MESH)
    for c in whole:
        c.start()

    zero = jnp.zeros((nh, rows, DH), F32)

    @pl.when(z < 2)
    def _():
        rz[0] = zero

    @pl.when(z < 1)
    def _():
        rz[1] = zero

    @pl.when(z != 3)
    def _():
        rz[3] = zero

    for j in range(1, 4):
        @pl.when((z > 0) & (z < 2 + 4 * j))
        def _(j=j):
            rw[j] = zero

    for zz in range(nz):
        ok = zz <= z
        for j, k in express:
            if zz == nz - 1 - k:
                ok = ok | ((z == j) & jnp.logical_not(first))

        @pl.when(ok)
        def _(zz=zz):
            fr[zz] = jnp.zeros(fr.shape[1:], F32)
    for r in range(nh, fs.shape[1]):
        fs[:, r, :] = jnp.zeros((nz, DH), F32)
    rx[x] = sx[x]

    @pl.when(row0 & jnp.logical_not(first))
    def _():
        pl.semaphore_wait(two, NX)
        for d in far + (0,):
            d_copy(xwrap(d)).start()
    with jax.named_scope("xready"):
        for k in range(1, NX + 1):
            to = x_of(k)

            @pl.when((key < k) & (z == 0) & plane if k == NX else key < k)
            def _(to=to):
                pl.semaphore_wait(xready.at[lax.rem(to + NX - x, NX)], 1)
                x_copy(to).start()

    ri = lax.broadcasted_iota(jnp.int32, (SUB, SUB), 0)
    ci = lax.broadcasted_iota(jnp.int32, (SUB, SUB), 1)

    def inner_of(h):
        cols = pl.ds(h * DH, DH)
        base = jnp.exp((ri - ci).astype(F32) * lds[h]) * scale
        for i in range(nb):
            qi = q_v[pl.ds(i * SUB, SUB), cols]
            parts = []
            for j in range(i + 1):
                s = lax.dot_general(qi, k_v[pl.ds(j * SUB, SUB), cols], (((1,), (1,)), ((), ())),
                                    preferred_element_type=F32)
                if j == i:
                    w = jnp.where(ri >= ci, s * base, 0.0)
                else:
                    w = s * (base * jnp.exp(lds[h] * float((i - j) * SUB)))
                parts.append(w.astype(BF16))
            w = parts[0] if i == 0 else jnp.concatenate(parts, axis=1)
            inner[h, pl.ds(i * SUB, SUB), :] = jnp.dot(
                w, v_v[pl.ds(0, (i + 1) * SUB), cols], preferred_element_type=F32)

    def gate_of(h):
        cols = pl.ds(h * DH, DH)
        gain = gain_v[pl.ds(h * DH, DH)].reshape(1, DH)
        u = g_v[:, cols].astype(F32)
        gs[h] = u / (1.0 + jnp.exp(-u)) * gain

    def local_work():
        with jax.named_scope("local"):
            for c in whole:
                c.wait()
            for h in range(nh):
                inner_of(h)
                gate_of(h)

    with jax.named_scope("xwait"):
        moved(rx.at[pl.ds(0, NX - 1)], xr_sem).wait()
    with jax.named_scope("prefix"):
        for h in range(nh):
            d1 = jnp.exp(lds[h] * float(tokens))
            acc = rx[0, h]
            for xx in range(1, NX):
                xp[h, xx] = acc
                acc = acc * d1 + rx[xx, h]
            rtot[h] = acc

    @pl.when(z == 0)
    def _():
        for h in range(nh):
            xp[h, 0] = jnp.zeros((rows, DH), F32)
            cb[h, 0] = jnp.zeros((rows, DH), F32)
            rc[h, x] = xp[h, x]
        for to in (1, 2, 3, 7, 6, 5, 4, 0):
            @pl.when((x != to) & jnp.logical_not(first))
            def _(to=to):
                for h in range(nh):
                    pltpu.make_async_remote_copy(
                        xp.at[h, to], rc.at[h, x], xs_sem, br_sem.at[h],
                        device_id=at(z, to), device_id_type=MESH).start()

    @pl.when(z > 0)
    def _():
        for h in range(nh):
            fs[:, h, :] = rtot[h] * jnp.exp((nz - 1 - z).astype(F32) * (lds[h] * float(tokens * NX)))

    for zz in range(nz - 1):
        ok = z > zz
        for j, k in express:
            if zz == j:
                ok = ok & ((z != nz - 1 - k) | column if j == 0 else z != nz - 1 - k)
        if zz == 0:
            ok = ok & jnp.logical_not(inner_col)

        @pl.when(ok)
        def _(zz=zz):
            f_copy(zz).start()
    for slot, d, ok in raw:
        @pl.when(ok)
        def _(slot=slot, d=d):
            if d > 0:
                ready_wait(d)
            else:
                @pl.when(column & (z == 1))
                def _():
                    pl.semaphore_wait(xready.at[0], 1)
            a_copy(slot, d).start()

    def back(h):
        for d in far:
            b_copy(h, d).start()
        rc[h, x] = cb[h, x]

    early = (z >= 1) & (z < nz // 2)

    @pl.when(early)
    def _():
        local_work()

    @pl.when(row1)
    def _():
        with jax.named_scope("row0"):
            moved(r2, r2_sem).wait()
            for h in range(nh):
                d1 = jnp.exp(lds[h] * float(tokens))
                acc = r2[0, h]
                for xx in range(1, NX):
                    cb2[h, xx] = acc
                    acc = acc * d1 + r2[xx, h]
                rz[1, h] = acc

            @pl.when(x == 0)
            def _():
                for to in (1, 2, 3, 7, 6, 5, 4):
                    for h in range(nh):
                        s_copy(h, to).start()

    @pl.when(z <= last_c)
    def _():
        with jax.named_scope("windows"):
            @pl.when(z > last_c - 2)
            def _():
                ready_wait(2)
            n = 1 + jnp.where((z >= 1) & jnp.logical_not(row1), 1, 0) + jnp.where(z >= 2, 1, 0) + jnp.where(z == 3, 1, 0)
            moved_some(rz, ar_sem, n)
            for h in range(nh):
                dd = [jnp.exp(lds[h] * float(tokens * NX * k)) for k in range(5)]
                win[h] = (rz[2, h] + dd[1] * rtot[h] + dd[2] * rz[1, h]
                          + dd[3] * rz[0, h] + dd[4] * rz[3, h])
            w_copy(0).start()

    with jax.named_scope("wwait"):
        moved_some(rw, wr_sem, lax.div(z + 2, 4))

    @pl.when(z == 1)
    def _():
        rw[0] = rz[1]
    @pl.when(z > 0)
    def _():
        for h in range(nh):
            ee = rw[0, h]
            for j in range(1, 4):
                ee = ee + rw[j, h] * jnp.exp(lds[h] * float(tokens * NX * 4 * j))
            cb[h, 0] = ee
            for xx in range(1, NX):
                cb[h, xx] = xp[h, xx] + ee * jnp.exp(lds[h] * float(tokens * xx))
            back(h)

    @pl.when(inner_col)
    def _():
        @pl.when(z > 1)
        def _():
            pl.semaphore_wait(xready.at[0], 1)
        f_copy(0).start()

    for j in range(1, 4):
        @pl.when(z + 2 + 4 * j < nz)
        def _(j=j):
            ready_wait(2 + 4 * j)
            w_copy(j).start()

    @pl.when(jnp.logical_not(early))
    def _():
        local_work()

    def outer_of(h):
        cols = pl.ds(h * DH, DH)
        lead = jnp.exp((r_iota(SUB) + 1.0) * lds[h])
        for xx in range(NX):
            carr[h, pl.ds(xx, rows, stride=NX), :] = rc[h, xx]
        low = carr[h].astype(BF16)
        o = jnp.dot(q_v[:, cols], low, preferred_element_type=F32)
        for i in range(nb):
            rs = pl.ds(i * SUB, SUB)
            inner[h, rs, :] = (inner[h, rs, :]
                               + o[i * SUB:(i + 1) * SUB] * (lead * jnp.exp(lds[h] * float(i * SUB))))

    def norm_of(h):
        cols = pl.ds(h * DH, DH)
        for i in range(nb):
            rs = pl.ds(i * SUB, SUB)
            mix = inner[h, rs, :]
            mean = jnp.sum(mix, axis=1, keepdims=True) * (1.0 / DH)
            cen = mix - mean
            var = jnp.sum(cen * cen, axis=1, keepdims=True) * (1.0 / DH)
            out_ref[rs, cols] = (cen * lax.rsqrt(var + 1e-05) * gs[h, rs, :]).astype(BF16)

    for h in range(nh):
        with jax.named_scope(f"bwait{h}"):
            moved(rc.at[h, pl.ds(0, NX - 1)], br_sem.at[h]).wait()
        with jax.named_scope(f"outer{h}"):
            outer_of(h)
            if h > 0:
                norm_of(h - 1)
    with jax.named_scope("norm"):
        norm_of(nh - 1)

    ahead = (nz - 1 - z).astype(F32)
    mine = []
    for h in range(nh):
        one = lds[h] * float(tokens * NX)
        mine.append(jnp.exp((ahead + 1.0) * one) * cb[h, 0, pl.ds(z, 1), :]
                    + jnp.exp(ahead * one) * rtot[h, pl.ds(z, 1), :])
    with jax.named_scope("fwait"):
        less = jnp.where(first, 0, jnp.where(z == 0, 3, jnp.where(z == 1, 2, 0)))
        moved_some(fr, fr_sem, nz - 1 - z - less)

        @pl.when((z == 0) & jnp.logical_not(first))
        def _():
            moved(er, er_sem).wait()

        @pl.when(z == 1)
        def _():
            moved(er.at[pl.ds(0, 2)], er_sem).wait()
    for h in range(nh):
        fin_ref[h] = mine[h] + jnp.sum(fr[:, h, :], axis=0, keepdims=True)

    @pl.when((z <= 1) & jnp.logical_not(first))
    def _():
        for h in range(nh):
            for k in range(2):
                fin_ref[h] = fin_ref[h] + jnp.sum(er[k, :, h, :], axis=0, keepdims=True)

    @pl.when((z == 0) & jnp.logical_not(first))
    def _():
        for h in range(nh):
            fin_ref[h] = fin_ref[h] + jnp.sum(er[2, :, h, :], axis=0, keepdims=True)

    with jax.named_scope("ends"):
        less = jnp.where(z >= nz - 2, 2, jnp.where(z == nz - 3, 1, 0))
        moved_some(fs, xs_sem, z - less + jnp.where(column & (z >= nz - 3), 1, 0))
        late = jnp.where(z >= nz - 2, 2 * NX, jnp.where(z == nz - 3, NX, 0))
        moved_some(fs, xs_sem, late - jnp.where(plane & (z >= nz - 3), 1, 0))
        moved(sx.at[pl.ds(0, NX - 1)], xs_sem).wait()

        @pl.when(row0)
        def _():
            moved(sx, xs_sem).wait()

        @pl.when(jnp.logical_not(first))
        def _():
            moved(cb.at[:, pl.ds(0, NX - 1)], xs_sem).wait()

        @pl.when(row1 & (x == 0))
        def _():
            moved(cb2.at[:, pl.ds(0, NX - 1)], xs_sem).wait()
        for slot, d, ok in raw:
            @pl.when(ok)
            def _(slot=slot):
                moved(rtot, xs_sem).wait()
        for j in range(4):
            @pl.when(z + 2 + 4 * j < nz)
            def _(j=j):
                moved(win, xs_sem).wait()


def put(a_ref, b_ref, a_out, b_out, sem):
    one = pltpu.make_async_copy(a_ref, a_out, sem.at[0])
    two = pltpu.make_async_copy(b_ref, b_out, sem.at[1])
    one.start()
    two.start()
    one.wait()
    two.wait()


def body(table, nz, queries, key_rows, value_rows, gate_input, norm_gain):
    tokens, width = queries.shape
    nh = width // DH
    rows = DH // NX
    anyspace = pl.BlockSpec(memory_space=pl.ANY)
    vmem = pl.BlockSpec(memory_space=pltpu.VMEM)
    dma = pltpu.SemaphoreType.DMA
    wide = pltpu.VMEM((tokens, width), BF16)
    spread = pltpu.VMEM((NX, nh, rows, DH), F32)
    eight = pltpu.VMEM((nh, NX, rows, DH), F32)
    four = pltpu.VMEM((4, nh, rows, DH), F32)
    one = pltpu.VMEM((nh, rows, DH), F32)
    square = pltpu.VMEM((nh, DH, DH), F32)
    tall = pltpu.VMEM((nh, tokens, DH), F32)
    few = pltpu.VMEM((3, NX, pl.next_power_of_2(nh), DH), F32)
    line = pltpu.VMEM((nz, pl.next_power_of_2(nh), DH), F32)
    retained, final = pl.pallas_call(
        functools.partial(kernel, table, nz),
        out_shape=(pltpu.VMEM((tokens, width), BF16), pltpu.VMEM((nh, 1, DH), F32)),
        in_specs=[anyspace] * 5,
        out_specs=(vmem, vmem),
        scratch_shapes=[
            wide, wide, wide, wide, pltpu.VMEM((width,), F32),
            square, spread, spread, eight, one, four, one, four, eight, eight, square, tall, tall, line, line,
            pltpu.VMEM((2, NX, pl.next_power_of_2(nh), DH), F32), few, spread, eight,
            dma((nh,)), dma((3,)), dma, dma, dma, dma, dma((nh,)), dma, dma, dma,
            pltpu.SemaphoreType.REGULAR((6,)), pltpu.SemaphoreType.REGULAR((NX,)),
            pltpu.SemaphoreType.REGULAR,
        ],
        compiler_params=pltpu.CompilerParams(collective_id=0, has_side_effects=True),
        name="retention",
    )(queries, key_rows, value_rows, gate_input, norm_gain)
    retained, final = (pltpu.with_memory_space_constraint(a, pltpu.VMEM) for a in (retained, final))
    retained, final = pl.pallas_call(
        put,
        out_shape=(jax.ShapeDtypeStruct((tokens, width), BF16), jax.ShapeDtypeStruct((nh, 1, DH), F32)),
        in_specs=[vmem, vmem],
        out_specs=(anyspace, anyspace),
        scratch_shapes=[dma((2,))],
        name="put",
    )(retained, final)
    return retained, final.reshape(1, nh, DH)


def solution(mesh):
    table = log_decays(mesh.shape["head"])
    rows = ("grp", "seq")
    placed = (P(rows, "head"),) * 4 + (P("head"),)
    return jax.shard_map(
        functools.partial(body, table, mesh.shape["seq"] // NX),
        mesh=mesh,
        in_specs=placed,
        out_specs=(P(rows, "head"), P(rows, "head", None)),
        check_vma=False,
    )
```

```python
import functools
import math

import jax
import jax.numpy as jnp
import numpy as np
from jax import lax
from jax.experimental import pallas as pl
from jax.experimental.pallas import tpu as pltpu
from jax.sharding import PartitionSpec as P

ALL_HEADS = 10
HEADS = 6
DH = 128
NX = 8
MESH = pl.DeviceIdType.MESH
F32 = jnp.float32
BF16 = jnp.bfloat16
SUB = 128


def log_decays(shards):
    per = HEADS // shards
    ids = ALL_HEADS - HEADS + np.arange(HEADS, dtype=np.float64)
    table = np.log1p(-np.exp2(-5.0 - ids)).reshape(shards, per)
    return [[float(np.float32(v)) for v in row] for row in table]


def kernel(
    table, nz,
    q_hbm, k_hbm, v_hbm, g_hbm, gain_hbm,
    out_ref, fin_ref,
    q_v, k_v, v_v, g_v, gain_v,
    st, sx, rx, xp, rtot, rz, win, rw, cb, rc, carr, inner, gs, fs, fr, es, er, r2, cb2,
    kv_sem, in_sem, xs_sem, xr_sem, ar_sem, wr_sem, br_sem, fr_sem, er_sem, r2_sem, ready, xready, two,
):
    tokens = q_v.shape[0]
    nh = q_v.shape[1] // DH
    rows = DH // NX
    nb = tokens // SUB
    scale = DH ** (-0.5)
    me = lax.axis_index("seq")
    z = lax.div(me, NX)
    x = lax.rem(me, NX)
    hd = lax.axis_index("head")
    plane = (lax.axis_index("grp") == 0) & (hd == 0)
    column = plane & (x == 0)
    first = column & (z == 0)
    row0 = plane & (z == 0)
    row1 = plane & (z == 1)
    inner_col = column & (z > 0) & (z < nz - 2)
    last_c = nz - 3

    lds = []
    for h in range(nh):
        ld = jnp.float32(table[0][h])
        for s in range(1, len(table)):
            ld = jnp.where(hd == s, jnp.float32(table[s][h]), ld)
        lds.append(ld)

    def at(zz, xx):
        return {"seq": zz * NX + xx}

    def xwrap(d):
        return lax.rem(x + (d % NX), NX)

    def r_iota(n):
        return lax.broadcasted_iota(jnp.int32, (n, DH), 0).astype(F32)

    def load(src, dst, h):
        cols = pl.ds(h * DH, DH)
        return pltpu.make_async_copy(src.at[:, cols], dst.at[:, cols], kv_sem.at[h])

    def kv_wait(h):
        two = pl.ds(0, 2 * DH)
        pltpu.make_async_copy(k_hbm.at[:, two], k_v.at[:, two], kv_sem.at[h]).wait()

    whole = (
        pltpu.make_async_copy(q_hbm, q_v, in_sem.at[0]),
        pltpu.make_async_copy(g_hbm, g_v, in_sem.at[1]),
        pltpu.make_async_copy(gain_hbm, gain_v, in_sem.at[2]),
    )

    for h in range(nh):
        load(k_hbm, k_v, h).start()
        load(v_hbm, v_v, h).start()

    def key_of(xx):
        k = jnp.where(xx < NX // 2, xx, 3 * NX // 2 - 1 - xx)
        k = jnp.where(xx == NX // 2, NX - 2, jnp.where(xx == NX // 2 + 1, NX - 1, k))
        return jnp.where((xx == 0) & (z == 0) & plane, NX, k)

    def x_of(k):
        if k == NX:
            return 0
        if k >= NX - 2:
            return k - NX // 2 + 2
        return k if k < NX // 2 else 3 * NX // 2 - 1 - k

    key = key_of(x)

    barrier = pltpu.get_barrier_semaphore()
    for d in range(1, NX):
        @pl.when(key_of(xwrap(d)) > key)
        def _(d=d):
            pl.semaphore_signal(barrier, inc=1, device_id=at(z, xwrap(d)), device_id_type=MESH)
    last = z == nz - 1
    express = ((0, 0), (1, 0), (0, 1), (0, 2), (1, 1))

    def tell_later():
        for zz in range(1, nz):
            ok = z < zz
            if zz < nz - 2:
                ok = ok & jnp.logical_not(first)

            @pl.when(ok)
            def _(zz=zz):
                pl.semaphore_signal(barrier, inc=1, device_id=at(zz, x), device_id_type=MESH)

    @pl.when(z > 0)
    def _():
        tell_later()

    @pl.when(inner_col)
    def _():
        pl.semaphore_signal(barrier, inc=1, device_id=at(0, x), device_id_type=MESH)

    @pl.when(row1 & (x > 0))
    def _():
        pl.semaphore_signal(barrier, inc=1, device_id=at(0, 0), device_id_type=MESH)
    owed = jnp.where(plane, NX - 1 - jnp.where(x == 0, 0, 1), NX - 1)
    count = key + z + jnp.where(z >= nz - 2, owed + NX - 1, jnp.where((z == nz - 3) | row1, owed, 0))
    count = jnp.where((z == 0) & plane, key - 1, count)
    count = jnp.where(first, 2 * NX + nz - 5, count) - jnp.where(inner_col, 1, 0)
    for h in range(nh):
        inner[h] = jnp.exp((tokens - 1 - r_iota(tokens)) * lds[h]) * scale
    with jax.named_scope("barrier"):
        @pl.when(count > 0)
        def _():
            pl.semaphore_wait(barrier, count)
    for d in range(1, NX):
        @pl.when(key_of(xwrap(d)) < key)
        def _(d=d):
            pl.semaphore_signal(xready.at[NX - d], inc=1, device_id=at(z, xwrap(d)), device_id_type=MESH)

    @pl.when(z == 0)
    def _():
        tell_later()

    @pl.when(first)
    def _():
        for zz in range(1, nz - 2):
            pl.semaphore_signal(xready.at[0], inc=1, device_id=at(zz, x), device_id_type=MESH)
    @pl.when(row0 & jnp.logical_not(first))
    def _():
        for d in range(1, NX):
            pl.semaphore_signal(barrier, inc=1, device_id=at(1, xwrap(d)), device_id_type=MESH)
    for to in range(1, NX):
        @pl.when(row1)
        def _(to=to):
            pl.semaphore_signal(two, inc=1, device_id=at(0, to), device_id_type=MESH)
    for j, k in express:
        @pl.when((z == j) & jnp.logical_not(first))
        def _(k=k):
            for d in range(1, NX):
                pl.semaphore_signal(barrier, inc=1, device_id=at(nz - 1 - k, xwrap(d)), device_id_type=MESH)
    def x_copy(to):
        return pltpu.make_async_remote_copy(
            sx.at[to], rx.at[x], xs_sem, xr_sem,
            device_id=at(z, to), device_id_type=MESH)

    def b_copy(h, d):
        return b_to(h, xwrap(d))

    def b_to(h, to):
        return pltpu.make_async_remote_copy(
            cb.at[h, to], rc.at[h, x], xs_sem, br_sem.at[h],
            device_id=at(z, to), device_id_type=MESH)

    def d_copy(to):
        return pltpu.make_async_remote_copy(
            sx.at[to], r2.at[x], xs_sem, r2_sem,
            device_id=at(1, to), device_id_type=MESH)

    def s_copy(h, to):
        return pltpu.make_async_remote_copy(
            cb2.at[h, to], rc.at[h, 0], xs_sem, br_sem.at[h],
            device_id=at(0, to), device_id_type=MESH)

    def e_copy(j, k, to):
        return pltpu.make_async_remote_copy(
            es.at[j, to], er.at[k, x], xs_sem, er_sem,
            device_id=at(j, to), device_id_type=MESH)

    def moved(ref, sem):
        return pltpu.make_async_copy(ref, ref, sem)

    def moved_some(ref, sem, n):
        for m in range(1, ref.shape[0] + 1):
            @pl.when(n == m)
            def _(m=m):
                moved(ref.at[pl.ds(0, m)], sem).wait()

    raw = (
        (1, 1, (z <= last_c - 1) & jnp.logical_not(row0)),
        (0, 2, z <= last_c - 2),
        (3, 3, z == 0),
        (2, -1, (z >= 1) & (z <= last_c + 1)),
    )
    def a_copy(slot, d):
        return pltpu.make_async_remote_copy(
            rtot, rz.at[slot], xs_sem, ar_sem,
            device_id=at(z + d, x), device_id_type=MESH)

    def w_copy(j):
        return pltpu.make_async_remote_copy(
            win, rw.at[j], xs_sem, wr_sem,
            device_id=at(z + (2 + 4 * j), x), device_id_type=MESH)

    def f_copy(zz):
        return pltpu.make_async_remote_copy(
            fs.at[zz], fr.at[z], xs_sem, fr_sem,
            device_id=at(zz, x), device_id_type=MESH)

    readies = ((1, (z >= 1) & (z <= last_c)), (2, z >= 2), (3, z == 3)) + tuple(
        (2 + 4 * j, z >= 2 + 4 * j) for j in range(1, 4))
    slot_of = {d: i for i, (d, _) in enumerate(readies)}

    def ready_wait(d):
        @pl.when(jnp.logical_not(first) if d < nz - 2 else z >= 0)
        def _():
            pl.semaphore_wait(ready.at[slot_of[d]], 1)

    far = (4, 3, 5, 2, 6, 1, 7)

    with jax.named_scope("load"):
        for h in range(nh):
            kv_wait(h)
    with jax.named_scope("state"):
        for h in range(nh):
            cols = pl.ds(h * DH, DH)
            kd = (k_v[:, cols].astype(F32) * inner[h]).astype(BF16)
            st[h] = lax.dot_general(kd, v_v[:, cols], (((0,), (0,)), ((), ())), preferred_element_type=F32)
            for xx in range(NX):
                sx[xx, h] = st[h, pl.ds(xx, rows, stride=NX), :]

    for r in range(nh, es.shape[2]):
        es[:, :, r, :] = jnp.zeros((2, NX, DH), F32)

    @pl.when(z >= nz - 3)
    def _():
        for h in range(nh):
            w = (NX - 1 - x + NX * (nz - 1 - z)).astype(F32) * (lds[h] * float(tokens))
            for j in range(2):
                es[j, :, h, :] = st[h, pl.ds(j * NX, NX), :] * jnp.exp(w)
        for j, k in express:
            for d in far + (0,):
                to = xwrap(d)
                ok = z == nz - 1 - k
                if j == 0:
                    ok = ok & jnp.logical_not(plane & (to == 0))

                @pl.when(ok)
                def _(j=j, k=k, to=to):
                    e_copy(j, k, to).start()

    @pl.when(first)
    def _():
        for d in (5, 4, 3, 6, 2, 7, 1):
            x_copy(xwrap(d)).start()
        for d in far + (0,):
            d_copy(xwrap(d)).start()
    for d in far:
        @pl.when((key_of(xwrap(d)) < key) & jnp.logical_not(first))
        def _(d=d):
            x_copy(xwrap(d)).start()
    for d, ok in readies:
        @pl.when(ok & jnp.logical_not((plane if d == 1 else inner_col) & (z == d)))
        def _(d=d):
            pl.semaphore_signal(ready.at[slot_of[d]], inc=1, device_id=at(z - d, x), device_id_type=MESH)
    for c in whole:
        c.start()

    zero = jnp.zeros((nh, rows, DH), F32)

    @pl.when(z < 2)
    def _():
        rz[0] = zero

    @pl.when(z < 1)
    def _():
        rz[1] = zero

    @pl.when(z != 3)
    def _():
        rz[3] = zero

    for j in range(1, 4):
        @pl.when((z > 0) & (z < 2 + 4 * j))
        def _(j=j):
            rw[j] = zero

    for zz in range(nz):
        ok = zz <= z
        for j, k in express:
            if zz == nz - 1 - k:
                ok = ok | ((z == j) & jnp.logical_not(first))

        @pl.when(ok)
        def _(zz=zz):
            fr[zz] = jnp.zeros(fr.shape[1:], F32)
    for r in range(nh, fs.shape[1]):
        fs[:, r, :] = jnp.zeros((nz, DH), F32)
    rx[x] = sx[x]

    @pl.when(row0 & jnp.logical_not(first))
    def _():
        pl.semaphore_wait(two, NX)
        for d in far + (0,):
            d_copy(xwrap(d)).start()
    with jax.named_scope("xready"):
        for k in range(1, NX + 1):
            to = x_of(k)

            @pl.when((key < k) & (z == 0) & plane if k == NX else key < k)
            def _(to=to):
                pl.semaphore_wait(xready.at[lax.rem(to + NX - x, NX)], 1)
                x_copy(to).start()

    ri = lax.broadcasted_iota(jnp.int32, (SUB, SUB), 0)
    ci = lax.broadcasted_iota(jnp.int32, (SUB, SUB), 1)

    def inner_of(h):
        cols = pl.ds(h * DH, DH)
        base = jnp.exp((ri - ci).astype(F32) * lds[h]) * scale
        for i in range(nb):
            qi = q_v[pl.ds(i * SUB, SUB), cols]
            parts = []
            for j in range(i + 1):
                s = lax.dot_general(qi, k_v[pl.ds(j * SUB, SUB), cols], (((1,), (1,)), ((), ())),
                                    preferred_element_type=F32)
                if j == i:
                    w = jnp.where(ri >= ci, s * base, 0.0)
                else:
                    w = s * (base * jnp.exp(lds[h] * float((i - j) * SUB)))
                parts.append(w.astype(BF16))
            w = parts[0] if i == 0 else jnp.concatenate(parts, axis=1)
            inner[h, pl.ds(i * SUB, SUB), :] = jnp.dot(
                w, v_v[pl.ds(0, (i + 1) * SUB), cols], preferred_element_type=F32)

    def gate_of(h):
        cols = pl.ds(h * DH, DH)
        gain = gain_v[pl.ds(h * DH, DH)].reshape(1, DH)
        u = g_v[:, cols].astype(F32)
        gs[h] = u / (1.0 + jnp.exp(-u)) * gain

    def local_work():
        with jax.named_scope("local"):
            for c in whole:
                c.wait()
            for h in range(nh):
                inner_of(h)
                gate_of(h)

    with jax.named_scope("xwait"):
        moved(rx.at[pl.ds(0, NX - 1)], xr_sem).wait()
    with jax.named_scope("prefix"):
        for h in range(nh):
            d1 = jnp.exp(lds[h] * float(tokens))
            acc = rx[0, h]
            for xx in range(1, NX):
                xp[h, xx] = acc
                acc = acc * d1 + rx[xx, h]
            rtot[h] = acc

    @pl.when(z == 0)
    def _():
        for h in range(nh):
            xp[h, 0] = jnp.zeros((rows, DH), F32)
            cb[h, 0] = jnp.zeros((rows, DH), F32)
            rc[h, x] = xp[h, x]
        for to in (1, 2, 3, 7, 6, 5, 4, 0):
            @pl.when((x != to) & jnp.logical_not(first))
            def _(to=to):
                for h in range(nh):
                    pltpu.make_async_remote_copy(
                        xp.at[h, to], rc.at[h, x], xs_sem, br_sem.at[h],
                        device_id=at(z, to), device_id_type=MESH).start()

    @pl.when(z > 0)
    def _():
        for h in range(nh):
            fs[:, h, :] = rtot[h] * jnp.exp((nz - 1 - z).astype(F32) * (lds[h] * float(tokens * NX)))

    for zz in range(nz - 1):
        ok = z > zz
        for j, k in express:
            if zz == j:
                ok = ok & ((z != nz - 1 - k) | column if j == 0 else z != nz - 1 - k)
        if zz == 0:
            ok = ok & jnp.logical_not(inner_col)

        @pl.when(ok)
        def _(zz=zz):
            f_copy(zz).start()
    for slot, d, ok in raw:
        @pl.when(ok)
        def _(slot=slot, d=d):
            if d > 0:
                ready_wait(d)
            else:
                @pl.when(column & (z == 1))
                def _():
                    pl.semaphore_wait(xready.at[0], 1)
            a_copy(slot, d).start()

    def back(h):
        for d in far:
            b_copy(h, d).start()
        rc[h, x] = cb[h, x]

    early = (z >= 1) & (z < nz // 2)

    @pl.when(early)
    def _():
        local_work()

    @pl.when(row1)
    def _():
        with jax.named_scope("row0"):
            moved(r2, r2_sem).wait()
            for h in range(nh):
                d1 = jnp.exp(lds[h] * float(tokens))
                acc = r2[0, h]
                for xx in range(1, NX):
                    cb2[h, xx] = acc
                    acc = acc * d1 + r2[xx, h]
                rz[1, h] = acc

            @pl.when(x == 0)
            def _():
                for to in (1, 2, 3, 7, 6, 5, 4):
                    for h in range(nh):
                        s_copy(h, to).start()

    @pl.when(z <= last_c)
    def _():
        with jax.named_scope("windows"):
            @pl.when(z > last_c - 2)
            def _():
                ready_wait(2)
            n = 1 + jnp.where((z >= 1) & jnp.logical_not(row1), 1, 0) + jnp.where(z >= 2, 1, 0) + jnp.where(z == 3, 1, 0)
            moved_some(rz, ar_sem, n)
            for h in range(nh):
                dd = [jnp.exp(lds[h] * float(tokens * NX * k)) for k in range(5)]
                win[h] = (rz[2, h] + dd[1] * rtot[h] + dd[2] * rz[1, h]
                          + dd[3] * rz[0, h] + dd[4] * rz[3, h])
            w_copy(0).start()

    with jax.named_scope("wwait"):
        moved_some(rw, wr_sem, lax.div(z + 2, 4))

    @pl.when(z == 1)
    def _():
        rw[0] = rz[1]
    @pl.when(z > 0)
    def _():
        for h in range(nh):
            ee = rw[0, h]
            for j in range(1, 4):
                ee = ee + rw[j, h] * jnp.exp(lds[h] * float(tokens * NX * 4 * j))
            cb[h, 0] = ee
            for xx in range(1, NX):
                cb[h, xx] = xp[h, xx] + ee * jnp.exp(lds[h] * float(tokens * xx))
            back(h)

    @pl.when(inner_col)
    def _():
        @pl.when(z > 1)
        def _():
            pl.semaphore_wait(xready.at[0], 1)
        f_copy(0).start()

    for j in range(1, 4):
        @pl.when(z + 2 + 4 * j < nz)
        def _(j=j):
            ready_wait(2 + 4 * j)
            w_copy(j).start()

    @pl.when(jnp.logical_not(early))
    def _():
        local_work()

    def outer_of(h):
        cols = pl.ds(h * DH, DH)
        lead = jnp.exp((r_iota(SUB) + 1.0) * lds[h])
        for xx in range(NX):
            carr[h, pl.ds(xx, rows, stride=NX), :] = rc[h, xx]
        low = carr[h].astype(BF16)
        o = jnp.dot(q_v[:, cols], low, preferred_element_type=F32)
        for i in range(nb):
            rs = pl.ds(i * SUB, SUB)
            inner[h, rs, :] = (inner[h, rs, :]
                               + o[i * SUB:(i + 1) * SUB] * (lead * jnp.exp(lds[h] * float(i * SUB))))

    def norm_of(h):
        cols = pl.ds(h * DH, DH)
        for i in range(nb):
            rs = pl.ds(i * SUB, SUB)
            mix = inner[h, rs, :]
            mean = jnp.sum(mix, axis=1, keepdims=True) * (1.0 / DH)
            cen = mix - mean
            var = jnp.sum(cen * cen, axis=1, keepdims=True) * (1.0 / DH)
            out_ref[rs, cols] = (cen * lax.rsqrt(var + 1e-05) * gs[h, rs, :]).astype(BF16)

    for h in range(nh):
        with jax.named_scope(f"bwait{h}"):
            moved(rc.at[h, pl.ds(0, NX - 1)], br_sem.at[h]).wait()
        with jax.named_scope(f"outer{h}"):
            outer_of(h)
            if h > 0:
                norm_of(h - 1)
    with jax.named_scope("norm"):
        norm_of(nh - 1)

    ahead = (nz - 1 - z).astype(F32)
    mine = []
    for h in range(nh):
        one = lds[h] * float(tokens * NX)
        mine.append(jnp.exp((ahead + 1.0) * one) * cb[h, 0, pl.ds(z, 1), :]
                    + jnp.exp(ahead * one) * rtot[h, pl.ds(z, 1), :])
    with jax.named_scope("fwait"):
        less = jnp.where(first, 0, jnp.where(z == 0, 3, jnp.where(z == 1, 2, 0)))
        moved_some(fr, fr_sem, nz - 1 - z - less)

        @pl.when((z == 0) & jnp.logical_not(first))
        def _():
            moved(er, er_sem).wait()

        @pl.when(z == 1)
        def _():
            moved(er.at[pl.ds(0, 2)], er_sem).wait()
    for h in range(nh):
        fin_ref[h] = mine[h] + jnp.sum(fr[:, h, :], axis=0, keepdims=True)

    @pl.when((z <= 1) & jnp.logical_not(first))
    def _():
        for h in range(nh):
            for k in range(2):
                fin_ref[h] = fin_ref[h] + jnp.sum(er[k, :, h, :], axis=0, keepdims=True)

    @pl.when((z == 0) & jnp.logical_not(first))
    def _():
        for h in range(nh):
            fin_ref[h] = fin_ref[h] + jnp.sum(er[2, :, h, :], axis=0, keepdims=True)

    with jax.named_scope("ends"):
        less = jnp.where(z >= nz - 2, 2, jnp.where(z == nz - 3, 1, 0))
        lines = z - less + jnp.where(column & (z >= nz - 3), 1, 0)
        late = jnp.where(z >= nz - 2, 2 * NX, jnp.where(z == nz - 3, NX, 0))
        lines = lines + late - jnp.where(plane & (z >= nz - 3), 1, 0)
        totals = lax.div(nz + 1 - z, 4)
        for slot, d, ok in raw:
            totals = totals + jnp.where(ok, 1, 0)
        for ref, n in ((fs, lines), (rw, totals)):
            m = ref.shape[0]
            while m > 0:
                @pl.when(lax.rem(lax.div(n, m), 2) == 1)
                def _(ref=ref, m=m):
                    moved(ref.at[pl.ds(0, m)], xs_sem).wait()
                m = m // 2
        moved(sx.at[pl.ds(0, NX - 1)], xs_sem).wait()

        @pl.when(row0)
        def _():
            moved(sx, xs_sem).wait()

        @pl.when(jnp.logical_not(first))
        def _():
            moved(cb.at[:, pl.ds(0, NX - 1)], xs_sem).wait()

        @pl.when(row1 & (x == 0))
        def _():
            moved(cb2.at[:, pl.ds(0, NX - 1)], xs_sem).wait()


def put(a_ref, b_ref, a_out, b_out, sem):
    one = pltpu.make_async_copy(a_ref, a_out, sem.at[0])
    two = pltpu.make_async_copy(b_ref, b_out, sem.at[1])
    one.start()
    two.start()
    one.wait()
    two.wait()


def body(table, nz, queries, key_rows, value_rows, gate_input, norm_gain):
    tokens, width = queries.shape
    nh = width // DH
    rows = DH // NX
    anyspace = pl.BlockSpec(memory_space=pl.ANY)
    vmem = pl.BlockSpec(memory_space=pltpu.VMEM)
    dma = pltpu.SemaphoreType.DMA
    wide = pltpu.VMEM((tokens, width), BF16)
    spread = pltpu.VMEM((NX, nh, rows, DH), F32)
    eight = pltpu.VMEM((nh, NX, rows, DH), F32)
    four = pltpu.VMEM((4, nh, rows, DH), F32)
    one = pltpu.VMEM((nh, rows, DH), F32)
    square = pltpu.VMEM((nh, DH, DH), F32)
    tall = pltpu.VMEM((nh, tokens, DH), F32)
    few = pltpu.VMEM((3, NX, pl.next_power_of_2(nh), DH), F32)
    line = pltpu.VMEM((nz, pl.next_power_of_2(nh), DH), F32)
    retained, final = pl.pallas_call(
        functools.partial(kernel, table, nz),
        out_shape=(pltpu.VMEM((tokens, width), BF16), pltpu.VMEM((nh, 1, DH), F32)),
        in_specs=[anyspace] * 5,
        out_specs=(vmem, vmem),
        scratch_shapes=[
            wide, wide, wide, wide, pltpu.VMEM((width,), F32),
            square, spread, spread, eight, one, four, one, four, eight, eight, square, tall, tall, line, line,
            pltpu.VMEM((2, NX, pl.next_power_of_2(nh), DH), F32), few, spread, eight,
            dma((nh,)), dma((3,)), dma, dma, dma, dma, dma((nh,)), dma, dma, dma,
            pltpu.SemaphoreType.REGULAR((6,)), pltpu.SemaphoreType.REGULAR((NX,)),
            pltpu.SemaphoreType.REGULAR,
        ],
        compiler_params=pltpu.CompilerParams(collective_id=0, has_side_effects=True),
        name="retention",
    )(queries, key_rows, value_rows, gate_input, norm_gain)
    retained, final = (pltpu.with_memory_space_constraint(a, pltpu.VMEM) for a in (retained, final))
    retained, final = pl.pallas_call(
        put,
        out_shape=(jax.ShapeDtypeStruct((tokens, width), BF16), jax.ShapeDtypeStruct((nh, 1, DH), F32)),
        in_specs=[vmem, vmem],
        out_specs=(anyspace, anyspace),
        scratch_shapes=[dma((2,))],
        name="put",
    )(retained, final)
    return retained, final.reshape(1, nh, DH)


def solution(mesh):
    table = log_decays(mesh.shape["head"])
    rows = ("grp", "seq")
    placed = (P(rows, "head"),) * 4 + (P("head"),)
    return jax.shard_map(
        functools.partial(body, table, mesh.shape["seq"] // NX),
        mesh=mesh,
        in_specs=placed,
        out_specs=(P(rows, "head"), P(rows, "head", None)),
        check_vma=False,
    )
```

```python
import functools
import math

import jax
import jax.numpy as jnp
import numpy as np
from jax import lax
from jax.experimental import pallas as pl
from jax.experimental.pallas import tpu as pltpu
from jax.sharding import PartitionSpec as P

ALL_HEADS = 10
HEADS = 6
DH = 128
NX = 8
MESH = pl.DeviceIdType.MESH
F32 = jnp.float32
BF16 = jnp.bfloat16
SUB = 128


def log_decays(shards):
    per = HEADS // shards
    ids = ALL_HEADS - HEADS + np.arange(HEADS, dtype=np.float64)
    table = np.log1p(-np.exp2(-5.0 - ids)).reshape(shards, per)
    return [[float(np.float32(v)) for v in row] for row in table]


def kernel(
    table, nz,
    q_hbm, k_hbm, v_hbm, g_hbm, gain_hbm,
    out_ref, fin_ref,
    q_v, k_v, v_v, g_v, gain_v,
    st, sx, rx, xp, rtot, rz, win, rw, cb, rc, carr, inner, gs, fs, fr, es, er, r2, cb2,
    kv_sem, in_sem, xs_sem, xr_sem, ar_sem, wr_sem, br_sem, fr_sem, er_sem, r2_sem, ready, xready, two,
):
    tokens = q_v.shape[0]
    nh = q_v.shape[1] // DH
    rows = DH // NX
    nb = tokens // SUB
    scale = DH ** (-0.5)
    me = lax.axis_index("seq")
    z = lax.div(me, NX)
    x = lax.rem(me, NX)
    hd = lax.axis_index("head")
    plane = (lax.axis_index("grp") == 0) & (hd == 0)
    column = plane & (x == 0)
    first = column & (z == 0)
    row0 = plane & (z == 0)
    row1 = plane & (z == 1)
    inner_col = column & (z > 0) & (z < nz - 2)
    last_c = nz - 3

    lds = []
    for h in range(nh):
        ld = jnp.float32(table[0][h])
        for s in range(1, len(table)):
            ld = jnp.where(hd == s, jnp.float32(table[s][h]), ld)
        lds.append(ld)

    def at(zz, xx):
        return {"seq": zz * NX + xx}

    def xwrap(d):
        return lax.rem(x + (d % NX), NX)

    def r_iota(n):
        return lax.broadcasted_iota(jnp.int32, (n, DH), 0).astype(F32)

    def load(src, dst, h):
        cols = pl.ds(h * DH, DH)
        return pltpu.make_async_copy(src.at[:, cols], dst.at[:, cols], kv_sem.at[h])

    def kv_wait(h):
        two = pl.ds(0, 2 * DH)
        pltpu.make_async_copy(k_hbm.at[:, two], k_v.at[:, two], kv_sem.at[h]).wait()

    whole = (
        pltpu.make_async_copy(q_hbm, q_v, in_sem.at[0]),
        pltpu.make_async_copy(g_hbm, g_v, in_sem.at[1]),
        pltpu.make_async_copy(gain_hbm, gain_v, in_sem.at[2]),
    )

    for h in range(nh):
        load(k_hbm, k_v, h).start()
        load(v_hbm, v_v, h).start()

    def key_of(xx):
        k = jnp.where(xx < NX // 2, xx, 3 * NX // 2 - 1 - xx)
        k = jnp.where(xx == NX // 2, NX - 2, jnp.where(xx == NX // 2 + 1, NX - 1, k))
        return jnp.where((xx == 0) & (z == 0) & plane, NX, k)

    def x_of(k):
        if k == NX:
            return 0
        if k >= NX - 2:
            return k - NX // 2 + 2
        return k if k < NX // 2 else 3 * NX // 2 - 1 - k

    key = key_of(x)

    barrier = pltpu.get_barrier_semaphore()
    for d in range(1, NX):
        @pl.when(key_of(xwrap(d)) > key)
        def _(d=d):
            pl.semaphore_signal(barrier, inc=1, device_id=at(z, xwrap(d)), device_id_type=MESH)
    last = z == nz - 1
    express = ((0, 0), (1, 0), (0, 1), (0, 2), (1, 1))

    def tell_later():
        for zz in range(1, nz):
            ok = z < zz
            if zz < nz - 2:
                ok = ok & jnp.logical_not(first)

            @pl.when(ok)
            def _(zz=zz):
                pl.semaphore_signal(barrier, inc=1, device_id=at(zz, x), device_id_type=MESH)

    @pl.when(z > 0)
    def _():
        tell_later()

    @pl.when(inner_col)
    def _():
        pl.semaphore_signal(barrier, inc=1, device_id=at(0, x), device_id_type=MESH)

    @pl.when(row1 & (x > 0))
    def _():
        pl.semaphore_signal(barrier, inc=1, device_id=at(0, 0), device_id_type=MESH)
    owed = jnp.where(plane, NX - 1 - jnp.where(x == 0, 0, 1), NX - 1)
    count = key + z + jnp.where(z >= nz - 2, owed + NX - 1, jnp.where((z == nz - 3) | row1, owed, 0))
    count = jnp.where((z == 0) & plane, key - 1, count)
    count = jnp.where(first, 2 * NX + nz - 5, count) - jnp.where(inner_col, 1, 0)
    for h in range(nh):
        inner[h] = jnp.exp((tokens - 1 - r_iota(tokens)) * lds[h]) * scale
    with jax.named_scope("barrier"):
        @pl.when(count > 0)
        def _():
            pl.semaphore_wait(barrier, count)
    for d in range(1, NX):
        @pl.when(key_of(xwrap(d)) < key)
        def _(d=d):
            pl.semaphore_signal(xready.at[NX - d], inc=1, device_id=at(z, xwrap(d)), device_id_type=MESH)

    @pl.when(z == 0)
    def _():
        tell_later()

    @pl.when(first)
    def _():
        for zz in range(1, nz - 2):
            pl.semaphore_signal(xready.at[0], inc=1, device_id=at(zz, x), device_id_type=MESH)
    @pl.when(row0 & jnp.logical_not(first))
    def _():
        for d in range(1, NX):
            pl.semaphore_signal(barrier, inc=1, device_id=at(1, xwrap(d)), device_id_type=MESH)
    for to in range(1, NX):
        @pl.when(row1)
        def _(to=to):
            pl.semaphore_signal(two, inc=1, device_id=at(0, to), device_id_type=MESH)
    for j, k in express:
        @pl.when((z == j) & jnp.logical_not(first))
        def _(k=k):
            for d in range(1, NX):
                pl.semaphore_signal(barrier, inc=1, device_id=at(nz - 1 - k, xwrap(d)), device_id_type=MESH)
    def x_copy(to):
        return pltpu.make_async_remote_copy(
            sx.at[to], rx.at[x], xs_sem, xr_sem,
            device_id=at(z, to), device_id_type=MESH)

    def b_copy(h, d):
        return b_to(h, xwrap(d))

    def b_to(h, to):
        return pltpu.make_async_remote_copy(
            cb.at[h, to], rc.at[h, x], xs_sem, br_sem.at[h],
            device_id=at(z, to), device_id_type=MESH)

    def d_copy(to):
        return pltpu.make_async_remote_copy(
            sx.at[to], r2.at[x], xs_sem, r2_sem,
            device_id=at(1, to), device_id_type=MESH)

    def s_copy(h, to):
        return pltpu.make_async_remote_copy(
            cb2.at[h, to], rc.at[h, 0], xs_sem, br_sem.at[h],
            device_id=at(0, to), device_id_type=MESH)

    def e_copy(j, k, to):
        return pltpu.make_async_remote_copy(
            es.at[j, to], er.at[k, x], xs_sem, er_sem,
            device_id=at(j, to), device_id_type=MESH)

    def moved(ref, sem):
        return pltpu.make_async_copy(ref, ref, sem)

    def moved_some(ref, sem, n):
        for m in range(1, ref.shape[0] + 1):
            @pl.when(n == m)
            def _(m=m):
                moved(ref.at[pl.ds(0, m)], sem).wait()

    raw = (
        (1, 1, (z <= last_c - 1) & jnp.logical_not(row0)),
        (0, 2, z <= last_c - 2),
        (3, 3, z == 0),
        (2, -1, (z >= 1) & (z <= last_c + 1)),
    )
    def a_copy(slot, d):
        return pltpu.make_async_remote_copy(
            rtot, rz.at[slot], xs_sem, ar_sem,
            device_id=at(z + d, x), device_id_type=MESH)

    def w_copy(j):
        return pltpu.make_async_remote_copy(
            win, rw.at[j], xs_sem, wr_sem,
            device_id=at(z + (2 + 4 * j), x), device_id_type=MESH)

    def f_copy(zz):
        return pltpu.make_async_remote_copy(
            fs.at[zz], fr.at[z], xs_sem, fr_sem,
            device_id=at(zz, x), device_id_type=MESH)

    readies = ((1, (z >= 1) & (z <= last_c)), (2, z >= 2), (3, z == 3)) + tuple(
        (2 + 4 * j, z >= 2 + 4 * j) for j in range(1, 4))
    slot_of = {d: i for i, (d, _) in enumerate(readies)}

    def ready_wait(d):
        @pl.when(jnp.logical_not(first) if d < nz - 2 else z >= 0)
        def _():
            pl.semaphore_wait(ready.at[slot_of[d]], 1)

    far = (4, 3, 5, 2, 6, 1, 7)

    with jax.named_scope("load"):
        for h in range(nh):
            kv_wait(h)
    with jax.named_scope("state"):
        for h in range(nh):
            cols = pl.ds(h * DH, DH)
            kd = (k_v[:, cols].astype(F32) * inner[h]).astype(BF16)
            st[h] = lax.dot_general(kd, v_v[:, cols], (((0,), (0,)), ((), ())), preferred_element_type=F32)
            for xx in range(NX):
                sx[xx, h] = st[h, pl.ds(xx, rows, stride=NX), :]

    for r in range(nh, es.shape[2]):
        es[:, :, r, :] = jnp.zeros((2, NX, DH), F32)

    @pl.when(z >= nz - 3)
    def _():
        for h in range(nh):
            w = (NX - 1 - x + NX * (nz - 1 - z)).astype(F32) * (lds[h] * float(tokens))
            for j in range(2):
                es[j, :, h, :] = st[h, pl.ds(j * NX, NX), :] * jnp.exp(w)
        for j, k in express:
            for d in far + (0,):
                to = xwrap(d)
                ok = z == nz - 1 - k
                if j == 0:
                    ok = ok & jnp.logical_not(plane & (to == 0))

                @pl.when(ok)
                def _(j=j, k=k, to=to):
                    e_copy(j, k, to).start()

    @pl.when(first)
    def _():
        for d in far:
            x_copy(xwrap(d)).start()
            d_copy(xwrap(d)).start()
        d_copy(x).start()
    for d in far:
        @pl.when((key_of(xwrap(d)) < key) & jnp.logical_not(first))
        def _(d=d):
            x_copy(xwrap(d)).start()
    for d, ok in readies:
        @pl.when(ok & jnp.logical_not((plane if d == 1 else inner_col) & (z == d)))
        def _(d=d):
            pl.semaphore_signal(ready.at[slot_of[d]], inc=1, device_id=at(z - d, x), device_id_type=MESH)
    for c in whole:
        c.start()

    zero = jnp.zeros((nh, rows, DH), F32)

    @pl.when(z < 2)
    def _():
        rz[0] = zero

    @pl.when(z < 1)
    def _():
        rz[1] = zero

    @pl.when(z != 3)
    def _():
        rz[3] = zero

    for j in range(1, 4):
        @pl.when((z > 0) & (z < 2 + 4 * j))
        def _(j=j):
            rw[j] = zero

    for zz in range(nz):
        ok = zz <= z
        for j, k in express:
            if zz == nz - 1 - k:
                ok = ok | ((z == j) & jnp.logical_not(first))

        @pl.when(ok)
        def _(zz=zz):
            fr[zz] = jnp.zeros(fr.shape[1:], F32)
    for r in range(nh, fs.shape[1]):
        fs[:, r, :] = jnp.zeros((nz, DH), F32)
    rx[x] = sx[x]

    @pl.when(row0 & jnp.logical_not(first))
    def _():
        pl.semaphore_wait(two, NX)
        for d in far + (0,):
            d_copy(xwrap(d)).start()
    with jax.named_scope("xready"):
        for k in range(1, NX + 1):
            to = x_of(k)

            @pl.when((key < k) & (z == 0) & plane if k == NX else key < k)
            def _(to=to):
                pl.semaphore_wait(xready.at[lax.rem(to + NX - x, NX)], 1)
                x_copy(to).start()

    ri = lax.broadcasted_iota(jnp.int32, (SUB, SUB), 0)
    ci = lax.broadcasted_iota(jnp.int32, (SUB, SUB), 1)

    def inner_of(h):
        cols = pl.ds(h * DH, DH)
        base = jnp.exp((ri - ci).astype(F32) * lds[h]) * scale
        for i in range(nb):
            qi = q_v[pl.ds(i * SUB, SUB), cols]
            parts = []
            for j in range(i + 1):
                s = lax.dot_general(qi, k_v[pl.ds(j * SUB, SUB), cols], (((1,), (1,)), ((), ())),
                                    preferred_element_type=F32)
                if j == i:
                    w = jnp.where(ri >= ci, s * base, 0.0)
                else:
                    w = s * (base * jnp.exp(lds[h] * float((i - j) * SUB)))
                parts.append(w.astype(BF16))
            w = parts[0] if i == 0 else jnp.concatenate(parts, axis=1)
            inner[h, pl.ds(i * SUB, SUB), :] = jnp.dot(
                w, v_v[pl.ds(0, (i + 1) * SUB), cols], preferred_element_type=F32)

    def gate_of(h):
        cols = pl.ds(h * DH, DH)
        gain = gain_v[pl.ds(h * DH, DH)].reshape(1, DH)
        u = g_v[:, cols].astype(F32)
        gs[h] = u / (1.0 + jnp.exp(-u)) * gain

    def local_work():
        with jax.named_scope("local"):
            for c in whole:
                c.wait()
            for h in range(nh):
                inner_of(h)
                gate_of(h)

    with jax.named_scope("xwait"):
        moved(rx.at[pl.ds(0, NX - 1)], xr_sem).wait()
    with jax.named_scope("prefix"):
        for h in range(nh):
            d1 = jnp.exp(lds[h] * float(tokens))
            acc = rx[0, h]
            for xx in range(1, NX):
                xp[h, xx] = acc
                acc = acc * d1 + rx[xx, h]
            rtot[h] = acc

    @pl.when(z == 0)
    def _():
        for h in range(nh):
            xp[h, 0] = jnp.zeros((rows, DH), F32)
            cb[h, 0] = jnp.zeros((rows, DH), F32)
            rc[h, x] = xp[h, x]
        for to in (1, 2, 3, 7, 6, 5, 4, 0):
            @pl.when((x != to) & jnp.logical_not(first))
            def _(to=to):
                for h in range(nh):
                    pltpu.make_async_remote_copy(
                        xp.at[h, to], rc.at[h, x], xs_sem, br_sem.at[h],
                        device_id=at(z, to), device_id_type=MESH).start()

    @pl.when(z > 0)
    def _():
        for h in range(nh):
            fs[:, h, :] = rtot[h] * jnp.exp((nz - 1 - z).astype(F32) * (lds[h] * float(tokens * NX)))

    for zz in range(nz - 1):
        ok = z > zz
        for j, k in express:
            if zz == j:
                ok = ok & ((z != nz - 1 - k) | column if j == 0 else z != nz - 1 - k)
        if zz == 0:
            ok = ok & jnp.logical_not(inner_col)

        @pl.when(ok)
        def _(zz=zz):
            f_copy(zz).start()
    for slot, d, ok in raw:
        @pl.when(ok)
        def _(slot=slot, d=d):
            if d > 0:
                ready_wait(d)
            else:
                @pl.when(column & (z == 1))
                def _():
                    pl.semaphore_wait(xready.at[0], 1)
            a_copy(slot, d).start()

    def back(h):
        for d in far:
            b_copy(h, d).start()
        rc[h, x] = cb[h, x]

    early = (z >= 1) & (z < nz // 2)

    @pl.when(early)
    def _():
        local_work()

    @pl.when(row1)
    def _():
        with jax.named_scope("row0"):
            moved(r2, r2_sem).wait()
            for h in range(nh):
                d1 = jnp.exp(lds[h] * float(tokens))
                acc = r2[0, h]
                for xx in range(1, NX):
                    cb2[h, xx] = acc
                    acc = acc * d1 + r2[xx, h]
                rz[1, h] = acc

            @pl.when(x == 0)
            def _():
                for to in (1, 2, 3, 7, 6, 5, 4):
                    for h in range(nh):
                        s_copy(h, to).start()

    @pl.when(z <= last_c)
    def _():
        with jax.named_scope("windows"):
            @pl.when(z > last_c - 2)
            def _():
                ready_wait(2)
            n = 1 + jnp.where((z >= 1) & jnp.logical_not(row1), 1, 0) + jnp.where(z >= 2, 1, 0) + jnp.where(z == 3, 1, 0)
            moved_some(rz, ar_sem, n)
            for h in range(nh):
                dd = [jnp.exp(lds[h] * float(tokens * NX * k)) for k in range(5)]
                win[h] = (rz[2, h] + dd[1] * rtot[h] + dd[2] * rz[1, h]
                          + dd[3] * rz[0, h] + dd[4] * rz[3, h])
            w_copy(0).start()

    with jax.named_scope("wwait"):
        moved_some(rw, wr_sem, lax.div(z + 2, 4))

    @pl.when(z == 1)
    def _():
        rw[0] = rz[1]
    @pl.when(z > 0)
    def _():
        for h in range(nh):
            ee = rw[0, h]
            for j in range(1, 4):
                ee = ee + rw[j, h] * jnp.exp(lds[h] * float(tokens * NX * 4 * j))
            cb[h, 0] = ee
            for xx in range(1, NX):
                cb[h, xx] = xp[h, xx] + ee * jnp.exp(lds[h] * float(tokens * xx))
            back(h)

    @pl.when(inner_col)
    def _():
        @pl.when(z > 1)
        def _():
            pl.semaphore_wait(xready.at[0], 1)
        f_copy(0).start()

    for j in range(1, 4):
        @pl.when(z + 2 + 4 * j < nz)
        def _(j=j):
            ready_wait(2 + 4 * j)
            w_copy(j).start()

    @pl.when(jnp.logical_not(early))
    def _():
        local_work()

    def outer_of(h):
        cols = pl.ds(h * DH, DH)
        lead = jnp.exp((r_iota(SUB) + 1.0) * lds[h])
        for xx in range(NX):
            carr[h, pl.ds(xx, rows, stride=NX), :] = rc[h, xx]
        low = carr[h].astype(BF16)
        o = jnp.dot(q_v[:, cols], low, preferred_element_type=F32)
        for i in range(nb):
            rs = pl.ds(i * SUB, SUB)
            inner[h, rs, :] = (inner[h, rs, :]
                               + o[i * SUB:(i + 1) * SUB] * (lead * jnp.exp(lds[h] * float(i * SUB))))

    def norm_of(h):
        cols = pl.ds(h * DH, DH)
        for i in range(nb):
            rs = pl.ds(i * SUB, SUB)
            mix = inner[h, rs, :]
            mean = jnp.sum(mix, axis=1, keepdims=True) * (1.0 / DH)
            cen = mix - mean
            var = jnp.sum(cen * cen, axis=1, keepdims=True) * (1.0 / DH)
            out_ref[rs, cols] = (cen * lax.rsqrt(var + 1e-05) * gs[h, rs, :]).astype(BF16)

    for h in range(nh):
        with jax.named_scope(f"bwait{h}"):
            moved(rc.at[h, pl.ds(0, NX - 1)], br_sem.at[h]).wait()
        with jax.named_scope(f"outer{h}"):
            outer_of(h)
            if h > 0:
                norm_of(h - 1)
    with jax.named_scope("norm"):
        norm_of(nh - 1)

    ahead = (nz - 1 - z).astype(F32)
    mine = []
    for h in range(nh):
        one = lds[h] * float(tokens * NX)
        mine.append(jnp.exp((ahead + 1.0) * one) * cb[h, 0, pl.ds(z, 1), :]
                    + jnp.exp(ahead * one) * rtot[h, pl.ds(z, 1), :])
    with jax.named_scope("fwait"):
        less = jnp.where(first, 0, jnp.where(z == 0, 3, jnp.where(z == 1, 2, 0)))
        moved_some(fr, fr_sem, nz - 1 - z - less)

        @pl.when((z == 0) & jnp.logical_not(first))
        def _():
            moved(er, er_sem).wait()

        @pl.when(z == 1)
        def _():
            moved(er.at[pl.ds(0, 2)], er_sem).wait()
    for h in range(nh):
        fin_ref[h] = mine[h] + jnp.sum(fr[:, h, :], axis=0, keepdims=True)

    @pl.when((z <= 1) & jnp.logical_not(first))
    def _():
        for h in range(nh):
            for k in range(2):
                fin_ref[h] = fin_ref[h] + jnp.sum(er[k, :, h, :], axis=0, keepdims=True)

    @pl.when((z == 0) & jnp.logical_not(first))
    def _():
        for h in range(nh):
            fin_ref[h] = fin_ref[h] + jnp.sum(er[2, :, h, :], axis=0, keepdims=True)

    with jax.named_scope("ends"):
        less = jnp.where(z >= nz - 2, 2, jnp.where(z == nz - 3, 1, 0))
        lines = z - less + jnp.where(column & (z >= nz - 3), 1, 0)
        late = jnp.where(z >= nz - 2, 2 * NX, jnp.where(z == nz - 3, NX, 0))
        lines = lines + late - jnp.where(plane & (z >= nz - 3), 1, 0)
        totals = lax.div(nz + 1 - z, 4)
        for slot, d, ok in raw:
            totals = totals + jnp.where(ok, 1, 0)
        for ref, n in ((fs, lines), (rw, totals)):
            m = ref.shape[0]
            while m > 0:
                @pl.when(lax.rem(lax.div(n, m), 2) == 1)
                def _(ref=ref, m=m):
                    moved(ref.at[pl.ds(0, m)], xs_sem).wait()
                m = m // 2
        moved(sx.at[pl.ds(0, NX - 1)], xs_sem).wait()

        @pl.when(row0)
        def _():
            moved(sx, xs_sem).wait()

        @pl.when(jnp.logical_not(first))
        def _():
            moved(cb.at[:, pl.ds(0, NX - 1)], xs_sem).wait()

        @pl.when(row1 & (x == 0))
        def _():
            moved(cb2.at[:, pl.ds(0, NX - 1)], xs_sem).wait()


def put(a_ref, b_ref, a_out, b_out, sem):
    one = pltpu.make_async_copy(a_ref, a_out, sem.at[0])
    two = pltpu.make_async_copy(b_ref, b_out, sem.at[1])
    one.start()
    two.start()
    one.wait()
    two.wait()


def body(table, nz, queries, key_rows, value_rows, gate_input, norm_gain):
    tokens, width = queries.shape
    nh = width // DH
    rows = DH // NX
    anyspace = pl.BlockSpec(memory_space=pl.ANY)
    vmem = pl.BlockSpec(memory_space=pltpu.VMEM)
    dma = pltpu.SemaphoreType.DMA
    wide = pltpu.VMEM((tokens, width), BF16)
    spread = pltpu.VMEM((NX, nh, rows, DH), F32)
    eight = pltpu.VMEM((nh, NX, rows, DH), F32)
    four = pltpu.VMEM((4, nh, rows, DH), F32)
    one = pltpu.VMEM((nh, rows, DH), F32)
    square = pltpu.VMEM((nh, DH, DH), F32)
    tall = pltpu.VMEM((nh, tokens, DH), F32)
    few = pltpu.VMEM((3, NX, pl.next_power_of_2(nh), DH), F32)
    line = pltpu.VMEM((nz, pl.next_power_of_2(nh), DH), F32)
    retained, final = pl.pallas_call(
        functools.partial(kernel, table, nz),
        out_shape=(pltpu.VMEM((tokens, width), BF16), pltpu.VMEM((nh, 1, DH), F32)),
        in_specs=[anyspace] * 5,
        out_specs=(vmem, vmem),
        scratch_shapes=[
            wide, wide, wide, wide, pltpu.VMEM((width,), F32),
            square, spread, spread, eight, one, four, one, four, eight, eight, square, tall, tall, line, line,
            pltpu.VMEM((2, NX, pl.next_power_of_2(nh), DH), F32), few, spread, eight,
            dma((nh,)), dma((3,)), dma, dma, dma, dma, dma((nh,)), dma, dma, dma,
            pltpu.SemaphoreType.REGULAR((6,)), pltpu.SemaphoreType.REGULAR((NX,)),
            pltpu.SemaphoreType.REGULAR,
        ],
        compiler_params=pltpu.CompilerParams(collective_id=0, has_side_effects=True),
        name="retention",
    )(queries, key_rows, value_rows, gate_input, norm_gain)
    retained, final = (pltpu.with_memory_space_constraint(a, pltpu.VMEM) for a in (retained, final))
    retained, final = pl.pallas_call(
        put,
        out_shape=(jax.ShapeDtypeStruct((tokens, width), BF16), jax.ShapeDtypeStruct((nh, 1, DH), F32)),
        in_specs=[vmem, vmem],
        out_specs=(anyspace, anyspace),
        scratch_shapes=[dma((2,))],
        name="put",
    )(retained, final)
    return retained, final.reshape(1, nh, DH)


def solution(mesh):
    table = log_decays(mesh.shape["head"])
    rows = ("grp", "seq")
    placed = (P(rows, "head"),) * 4 + (P("head"),)
    return jax.shard_map(
        functools.partial(body, table, mesh.shape["seq"] // NX),
        mesh=mesh,
        in_specs=placed,
        out_specs=(P(rows, "head"), P(rows, "head", None)),
        check_vma=False,
    )
```

```python
import functools
import math

import jax
import jax.numpy as jnp
import numpy as np
from jax import lax
from jax.experimental import pallas as pl
from jax.experimental.pallas import tpu as pltpu
from jax.sharding import PartitionSpec as P

ALL_HEADS = 10
HEADS = 6
DH = 128
NX = 8
MESH = pl.DeviceIdType.MESH
F32 = jnp.float32
BF16 = jnp.bfloat16
SUB = 128


def log_decays(shards):
    per = HEADS // shards
    ids = ALL_HEADS - HEADS + np.arange(HEADS, dtype=np.float64)
    table = np.log1p(-np.exp2(-5.0 - ids)).reshape(shards, per)
    return [[float(np.float32(v)) for v in row] for row in table]


def kernel(
    table, nz,
    q_hbm, k_hbm, v_hbm, g_hbm, gain_hbm,
    out_ref, fin_ref,
    q_v, k_v, v_v, g_v, gain_v,
    st, sx, rx, xp, rtot, rz, win, rw, cb, rc, carr, inner, gs, fs, fr, es, er, r2, cb2,
    kv_sem, in_sem, xs_sem, xr_sem, ar_sem, wr_sem, br_sem, fr_sem, er_sem, r2_sem, ready, xready, two,
):
    tokens = q_v.shape[0]
    nh = q_v.shape[1] // DH
    rows = DH // NX
    nb = tokens // SUB
    scale = DH ** (-0.5)
    me = lax.axis_index("seq")
    z = lax.div(me, NX)
    x = lax.rem(me, NX)
    hd = lax.axis_index("head")
    plane = (lax.axis_index("grp") == 0) & (hd == 0)
    column = plane & (x == 0)
    first = column & (z == 0)
    row0 = plane & (z == 0)
    row1 = plane & (z == 1)
    inner_col = column & (z > 0) & (z < nz - 2)
    last_c = nz - 3

    lds = []
    for h in range(nh):
        ld = jnp.float32(table[0][h])
        for s in range(1, len(table)):
            ld = jnp.where(hd == s, jnp.float32(table[s][h]), ld)
        lds.append(ld)

    def at(zz, xx):
        return {"seq": zz * NX + xx}

    def xwrap(d):
        return lax.rem(x + (d % NX), NX)

    def r_iota(n):
        return lax.broadcasted_iota(jnp.int32, (n, DH), 0).astype(F32)

    def load(src, dst, h):
        cols = pl.ds(h * DH, DH)
        return pltpu.make_async_copy(src.at[:, cols], dst.at[:, cols], kv_sem.at[h])

    def kv_wait(h):
        two = pl.ds(0, 2 * DH)
        pltpu.make_async_copy(k_hbm.at[:, two], k_v.at[:, two], kv_sem.at[h]).wait()

    whole = (
        pltpu.make_async_copy(q_hbm, q_v, in_sem.at[0]),
        pltpu.make_async_copy(g_hbm, g_v, in_sem.at[1]),
        pltpu.make_async_copy(gain_hbm, gain_v, in_sem.at[2]),
    )

    for h in range(nh):
        load(k_hbm, k_v, h).start()
        load(v_hbm, v_v, h).start()

    def key_of(xx):
        k = jnp.where(xx < NX // 2, xx, 3 * NX // 2 - 1 - xx)
        k = jnp.where(xx == NX // 2, NX - 2, jnp.where(xx == NX // 2 + 1, NX - 1, k))
        return jnp.where((xx == 0) & (z == 0) & plane, NX, k)

    def x_of(k):
        if k == NX:
            return 0
        if k >= NX - 2:
            return k - NX // 2 + 2
        return k if k < NX // 2 else 3 * NX // 2 - 1 - k

    key = key_of(x)

    barrier = pltpu.get_barrier_semaphore()
    for d in range(1, NX):
        @pl.when(key_of(xwrap(d)) > key)
        def _(d=d):
            pl.semaphore_signal(barrier, inc=1, device_id=at(z, xwrap(d)), device_id_type=MESH)
    last = z == nz - 1
    express = ((0, 0), (1, 0), (0, 1), (0, 2), (1, 1))

    def tell_later():
        for zz in range(1, nz):
            ok = z < zz
            if zz < nz - 2:
                ok = ok & jnp.logical_not(first)

            @pl.when(ok)
            def _(zz=zz):
                pl.semaphore_signal(barrier, inc=1, device_id=at(zz, x), device_id_type=MESH)

    @pl.when(z > 0)
    def _():
        tell_later()

    @pl.when(inner_col)
    def _():
        pl.semaphore_signal(barrier, inc=1, device_id=at(0, x), device_id_type=MESH)

    @pl.when(row1 & (x > 0))
    def _():
        pl.semaphore_signal(barrier, inc=1, device_id=at(0, 0), device_id_type=MESH)
    owed = jnp.where(plane, NX - 1 - jnp.where(x == 0, 0, 1), NX - 1)
    count = key + z + jnp.where(z >= nz - 2, owed + NX - 1, jnp.where((z == nz - 3) | row1, owed, 0))
    count = jnp.where((z == 0) & plane, key - 1, count)
    count = jnp.where(first, 2 * NX + nz - 5, count) - jnp.where(inner_col, 1, 0)
    for h in range(nh):
        inner[h] = jnp.exp((tokens - 1 - r_iota(tokens)) * lds[h]) * scale
    with jax.named_scope("barrier"):
        @pl.when(count > 0)
        def _():
            pl.semaphore_wait(barrier, count)
    for d in range(1, NX):
        @pl.when(key_of(xwrap(d)) < key)
        def _(d=d):
            pl.semaphore_signal(xready.at[NX - d], inc=1, device_id=at(z, xwrap(d)), device_id_type=MESH)

    @pl.when(z == 0)
    def _():
        tell_later()

    @pl.when(first)
    def _():
        for zz in range(1, nz - 2):
            pl.semaphore_signal(xready.at[0], inc=1, device_id=at(zz, x), device_id_type=MESH)
    @pl.when(row0 & jnp.logical_not(first))
    def _():
        for d in range(1, NX):
            pl.semaphore_signal(barrier, inc=1, device_id=at(1, xwrap(d)), device_id_type=MESH)
    for to in range(1, NX):
        @pl.when(row1)
        def _(to=to):
            pl.semaphore_signal(two, inc=1, device_id=at(0, to), device_id_type=MESH)
    for j, k in express:
        @pl.when((z == j) & jnp.logical_not(first))
        def _(k=k):
            for d in range(1, NX):
                pl.semaphore_signal(barrier, inc=1, device_id=at(nz - 1 - k, xwrap(d)), device_id_type=MESH)
    def x_copy(to):
        return pltpu.make_async_remote_copy(
            sx.at[to], rx.at[x], xs_sem, xr_sem,
            device_id=at(z, to), device_id_type=MESH)

    def b_copy(h, d):
        return b_to(h, xwrap(d))

    def b_to(h, to):
        return pltpu.make_async_remote_copy(
            cb.at[h, to], rc.at[h, x], xs_sem, br_sem.at[h],
            device_id=at(z, to), device_id_type=MESH)

    def d_copy(to):
        return pltpu.make_async_remote_copy(
            sx.at[to], r2.at[x], xs_sem, r2_sem,
            device_id=at(1, to), device_id_type=MESH)

    def s_copy(h, to):
        return pltpu.make_async_remote_copy(
            cb2.at[h, to], rc.at[h, 0], xs_sem, br_sem.at[h],
            device_id=at(0, to), device_id_type=MESH)

    def e_copy(j, k, to):
        return pltpu.make_async_remote_copy(
            es.at[j, to], er.at[k, x], xs_sem, er_sem,
            device_id=at(j, to), device_id_type=MESH)

    def moved(ref, sem):
        return pltpu.make_async_copy(ref, ref, sem)

    def moved_some(ref, sem, n):
        for m in range(1, ref.shape[0] + 1):
            @pl.when(n == m)
            def _(m=m):
                moved(ref.at[pl.ds(0, m)], sem).wait()

    raw = (
        (1, 1, (z <= last_c - 1) & jnp.logical_not(row0)),
        (0, 2, z <= last_c - 2),
        (3, 3, z == 0),
        (2, -1, (z >= 1) & (z <= last_c + 1)),
    )
    def a_copy(slot, d):
        return pltpu.make_async_remote_copy(
            rtot, rz.at[slot], xs_sem, ar_sem,
            device_id=at(z + d, x), device_id_type=MESH)

    def w_copy(j):
        return pltpu.make_async_remote_copy(
            win, rw.at[j], xs_sem, wr_sem,
            device_id=at(z + (2 + 4 * j), x), device_id_type=MESH)

    def f_copy(zz):
        return pltpu.make_async_remote_copy(
            fs.at[zz], fr.at[z], xs_sem, fr_sem,
            device_id=at(zz, x), device_id_type=MESH)

    readies = ((1, (z >= 1) & (z <= last_c)), (2, z >= 2), (3, z == 3)) + tuple(
        (2 + 4 * j, z >= 2 + 4 * j) for j in range(1, 4))
    slot_of = {d: i for i, (d, _) in enumerate(readies)}

    def ready_wait(d):
        @pl.when(jnp.logical_not(first) if d < nz - 2 else z >= 0)
        def _():
            pl.semaphore_wait(ready.at[slot_of[d]], 1)

    far = (4, 3, 5, 2, 6, 1, 7)

    with jax.named_scope("load"):
        for h in range(nh):
            kv_wait(h)
    with jax.named_scope("state"):
        for h in range(nh):
            cols = pl.ds(h * DH, DH)
            kd = (k_v[:, cols].astype(F32) * inner[h]).astype(BF16)
            st[h] = lax.dot_general(kd, v_v[:, cols], (((0,), (0,)), ((), ())), preferred_element_type=F32)
            for xx in range(NX):
                sx[xx, h] = st[h, pl.ds(xx, rows, stride=NX), :]

    for r in range(nh, es.shape[2]):
        es[:, :, r, :] = jnp.zeros((2, NX, DH), F32)

    @pl.when(z >= nz - 3)
    def _():
        for h in range(nh):
            w = (NX - 1 - x + NX * (nz - 1 - z)).astype(F32) * (lds[h] * float(tokens))
            for j in range(2):
                es[j, :, h, :] = st[h, pl.ds(j * NX, NX), :] * jnp.exp(w)
        for j, k in express:
            for d in far + (0,):
                to = xwrap(d)
                ok = z == nz - 1 - k
                if j == 0:
                    ok = ok & jnp.logical_not(plane & (to == 0))

                @pl.when(ok)
                def _(j=j, k=k, to=to):
                    e_copy(j, k, to).start()

    @pl.when(first)
    def _():
        for d in far:
            x_copy(xwrap(d)).start()
            d_copy(xwrap(d)).start()
        d_copy(x).start()
    for d in far:
        @pl.when((key_of(xwrap(d)) < key) & jnp.logical_not(first))
        def _(d=d):
            x_copy(xwrap(d)).start()
    for d, ok in readies:
        @pl.when(ok & jnp.logical_not((plane if d == 1 else inner_col) & (z == d)))
        def _(d=d):
            pl.semaphore_signal(ready.at[slot_of[d]], inc=1, device_id=at(z - d, x), device_id_type=MESH)
    for c in whole:
        c.start()

    zero = jnp.zeros((nh, rows, DH), F32)

    @pl.when(z < 2)
    def _():
        rz[0] = zero

    @pl.when(z < 1)
    def _():
        rz[1] = zero

    @pl.when(z != 3)
    def _():
        rz[3] = zero

    for j in range(1, 4):
        @pl.when((z > 0) & (z < 2 + 4 * j))
        def _(j=j):
            rw[j] = zero

    for zz in range(nz):
        ok = zz <= z
        for j, k in express:
            if zz == nz - 1 - k:
                ok = ok | ((z == j) & jnp.logical_not(first))

        @pl.when(ok)
        def _(zz=zz):
            fr[zz] = jnp.zeros(fr.shape[1:], F32)
    for r in range(nh, fs.shape[1]):
        fs[:, r, :] = jnp.zeros((nz, DH), F32)
    rx[x] = sx[x]

    @pl.when(row0 & jnp.logical_not(first))
    def _():
        pl.semaphore_wait(two, NX)
        for d in far + (0,):
            d_copy(xwrap(d)).start()
    with jax.named_scope("xready"):
        for k in range(1, NX + 1):
            to = x_of(k)

            @pl.when((key < k) & (z == 0) & plane if k == NX else key < k)
            def _(to=to):
                pl.semaphore_wait(xready.at[lax.rem(to + NX - x, NX)], 1)
                x_copy(to).start()

    ri = lax.broadcasted_iota(jnp.int32, (SUB, SUB), 0)
    ci = lax.broadcasted_iota(jnp.int32, (SUB, SUB), 1)

    def inner_of(h):
        cols = pl.ds(h * DH, DH)
        base = jnp.exp((ri - ci).astype(F32) * lds[h]) * scale
        for i in range(nb):
            qi = q_v[pl.ds(i * SUB, SUB), cols]
            parts = []
            for j in range(i + 1):
                s = lax.dot_general(qi, k_v[pl.ds(j * SUB, SUB), cols], (((1,), (1,)), ((), ())),
                                    preferred_element_type=F32)
                if j == i:
                    w = jnp.where(ri >= ci, s * base, 0.0)
                else:
                    w = s * (base * jnp.exp(lds[h] * float((i - j) * SUB)))
                parts.append(w.astype(BF16))
            w = parts[0] if i == 0 else jnp.concatenate(parts, axis=1)
            inner[h, pl.ds(i * SUB, SUB), :] = jnp.dot(
                w, v_v[pl.ds(0, (i + 1) * SUB), cols], preferred_element_type=F32)

    def gate_of(h):
        cols = pl.ds(h * DH, DH)
        gain = gain_v[pl.ds(h * DH, DH)].reshape(1, DH)
        u = g_v[:, cols].astype(F32)
        gs[h] = u / (1.0 + jnp.exp(-u)) * gain

    def local_work():
        with jax.named_scope("local"):
            for c in whole:
                c.wait()
            for h in range(nh):
                inner_of(h)
                gate_of(h)

    with jax.named_scope("xwait"):
        moved(rx.at[pl.ds(0, NX - 1)], xr_sem).wait()
    with jax.named_scope("prefix"):
        for h in range(nh):
            d1 = jnp.exp(lds[h] * float(tokens))
            acc = rx[0, h]
            for xx in range(1, NX):
                xp[h, xx] = acc
                acc = acc * d1 + rx[xx, h]
            rtot[h] = acc

    @pl.when(z == 0)
    def _():
        for h in range(nh):
            xp[h, 0] = jnp.zeros((rows, DH), F32)
            cb[h, 0] = jnp.zeros((rows, DH), F32)
            rc[h, x] = xp[h, x]
        for to in (1, 2, 3, 7, 6, 5, 4, 0):
            @pl.when((x != to) & jnp.logical_not(first))
            def _(to=to):
                for h in range(nh):
                    pltpu.make_async_remote_copy(
                        xp.at[h, to], rc.at[h, x], xs_sem, br_sem.at[h],
                        device_id=at(z, to), device_id_type=MESH).start()

    @pl.when(z > 0)
    def _():
        for h in range(nh):
            fs[:, h, :] = rtot[h] * jnp.exp((nz - 1 - z).astype(F32) * (lds[h] * float(tokens * NX)))

    for zz in range(nz - 1):
        ok = z > zz
        for j, k in express:
            if zz == j:
                ok = ok & ((z != nz - 1 - k) | column if j == 0 else z != nz - 1 - k)
        if zz == 0:
            ok = ok & jnp.logical_not(inner_col)

        @pl.when(ok)
        def _(zz=zz):
            f_copy(zz).start()
    for slot, d, ok in raw:
        @pl.when(ok)
        def _(slot=slot, d=d):
            if d > 0:
                ready_wait(d)
            else:
                @pl.when(column & (z == 1))
                def _():
                    pl.semaphore_wait(xready.at[0], 1)
            a_copy(slot, d).start()

    def back(h):
        for d in far:
            b_copy(h, d).start()
        rc[h, x] = cb[h, x]

    early = (z >= 1) & (z < nz // 2)

    @pl.when(early)
    def _():
        local_work()

    @pl.when(row1)
    def _():
        with jax.named_scope("row0"):
            moved(r2, r2_sem).wait()
            for h in range(nh):
                d1 = jnp.exp(lds[h] * float(tokens))
                acc = r2[0, h]
                for xx in range(1, NX):
                    cb2[h, xx] = acc
                    acc = acc * d1 + r2[xx, h]
                rz[1, h] = acc

            @pl.when(x == 0)
            def _():
                for to in (1, 2, 3, 7, 6, 5, 4):
                    for h in range(nh):
                        s_copy(h, to).start()

    @pl.when(z <= last_c)
    def _():
        with jax.named_scope("windows"):
            @pl.when(z > last_c - 2)
            def _():
                ready_wait(2)
            n = 1 + jnp.where((z >= 1) & jnp.logical_not(row1), 1, 0) + jnp.where(z >= 2, 1, 0) + jnp.where(z == 3, 1, 0)
            moved_some(rz, ar_sem, n)
            for h in range(nh):
                dd = [jnp.exp(lds[h] * float(tokens * NX * k)) for k in range(5)]
                win[h] = (rz[2, h] + dd[1] * rtot[h] + dd[2] * rz[1, h]
                          + dd[3] * rz[0, h] + dd[4] * rz[3, h])
            w_copy(0).start()

    with jax.named_scope("wwait"):
        moved_some(rw, wr_sem, lax.div(z + 2, 4))

    @pl.when(z == 1)
    def _():
        rw[0] = rz[1]
    @pl.when(z > 0)
    def _():
        for h in range(nh):
            ee = rw[0, h]
            for j in range(1, 4):
                ee = ee + rw[j, h] * jnp.exp(lds[h] * float(tokens * NX * 4 * j))
            cb[h, 0] = ee
            for xx in range(1, NX):
                cb[h, xx] = xp[h, xx] + ee * jnp.exp(lds[h] * float(tokens * xx))
            back(h)

    @pl.when(inner_col)
    def _():
        @pl.when(z > 1)
        def _():
            pl.semaphore_wait(xready.at[0], 1)
        f_copy(0).start()

    for j in range(1, 4):
        @pl.when(z + 2 + 4 * j < nz)
        def _(j=j):
            ready_wait(2 + 4 * j)
            w_copy(j).start()

    @pl.when(jnp.logical_not(early))
    def _():
        local_work()

    ahead = (nz - 1 - z).astype(F32)
    mine = []
    for h in range(nh):
        one = lds[h] * float(tokens * NX)
        mine.append(jnp.exp((ahead + 1.0) * one) * cb[h, 0, pl.ds(z, 1), :]
                    + jnp.exp(ahead * one) * rtot[h, pl.ds(z, 1), :])

    def outer_of(h):
        cols = pl.ds(h * DH, DH)
        lead = jnp.exp((r_iota(SUB) + 1.0) * lds[h])
        for xx in range(NX):
            carr[h, pl.ds(xx, rows, stride=NX), :] = rc[h, xx]
        low = carr[h].astype(BF16)
        o = jnp.dot(q_v[:, cols], low, preferred_element_type=F32)
        for i in range(nb):
            rs = pl.ds(i * SUB, SUB)
            inner[h, rs, :] = (inner[h, rs, :]
                               + o[i * SUB:(i + 1) * SUB] * (lead * jnp.exp(lds[h] * float(i * SUB))))

    def norm_of(h):
        cols = pl.ds(h * DH, DH)
        for i in range(nb):
            rs = pl.ds(i * SUB, SUB)
            mix = inner[h, rs, :]
            mean = jnp.sum(mix, axis=1, keepdims=True) * (1.0 / DH)
            cen = mix - mean
            var = jnp.sum(cen * cen, axis=1, keepdims=True) * (1.0 / DH)
            out_ref[rs, cols] = (cen * lax.rsqrt(var + 1e-05) * gs[h, rs, :]).astype(BF16)

    for h in range(nh):
        with jax.named_scope(f"bwait{h}"):
            moved(rc.at[h, pl.ds(0, NX - 1)], br_sem.at[h]).wait()
        with jax.named_scope(f"outer{h}"):
            outer_of(h)
            if h > 0:
                norm_of(h - 1)
    with jax.named_scope("norm"):
        norm_of(nh - 1)

    with jax.named_scope("fwait"):
        less = jnp.where(first, 0, jnp.where(z == 0, 3, jnp.where(z == 1, 2, 0)))
        moved_some(fr, fr_sem, nz - 1 - z - less)

        @pl.when((z == 0) & jnp.logical_not(first))
        def _():
            moved(er, er_sem).wait()

        @pl.when(z == 1)
        def _():
            moved(er.at[pl.ds(0, 2)], er_sem).wait()
    for h in range(nh):
        fin_ref[h] = mine[h] + jnp.sum(fr[:, h, :], axis=0, keepdims=True)

    @pl.when((z <= 1) & jnp.logical_not(first))
    def _():
        for h in range(nh):
            for k in range(2):
                fin_ref[h] = fin_ref[h] + jnp.sum(er[k, :, h, :], axis=0, keepdims=True)

    @pl.when((z == 0) & jnp.logical_not(first))
    def _():
        for h in range(nh):
            fin_ref[h] = fin_ref[h] + jnp.sum(er[2, :, h, :], axis=0, keepdims=True)

    with jax.named_scope("ends"):
        less = jnp.where(z >= nz - 2, 2, jnp.where(z == nz - 3, 1, 0))
        moved_some(fs, xs_sem, z - less + jnp.where(column & (z >= nz - 3), 1, 0))
        late = jnp.where(z >= nz - 2, 2 * NX, jnp.where(z == nz - 3, NX, 0))
        moved_some(fs, xs_sem, late - jnp.where(plane & (z >= nz - 3), 1, 0))
        moved(sx.at[pl.ds(0, NX - 1)], xs_sem).wait()

        @pl.when(row0)
        def _():
            moved(sx, xs_sem).wait()

        @pl.when(jnp.logical_not(first))
        def _():
            moved(cb.at[:, pl.ds(0, NX - 1)], xs_sem).wait()

        @pl.when(row1 & (x == 0))
        def _():
            moved(cb2.at[:, pl.ds(0, NX - 1)], xs_sem).wait()
        for slot, d, ok in raw:
            @pl.when(ok)
            def _(slot=slot):
                moved(rtot, xs_sem).wait()
        for j in range(4):
            @pl.when(z + 2 + 4 * j < nz)
            def _(j=j):
                moved(win, xs_sem).wait()


def put(a_ref, b_ref, a_out, b_out, sem):
    one = pltpu.make_async_copy(a_ref, a_out, sem.at[0])
    two = pltpu.make_async_copy(b_ref, b_out, sem.at[1])
    one.start()
    two.start()
    one.wait()
    two.wait()


def body(table, nz, queries, key_rows, value_rows, gate_input, norm_gain):
    tokens, width = queries.shape
    nh = width // DH
    rows = DH // NX
    anyspace = pl.BlockSpec(memory_space=pl.ANY)
    vmem = pl.BlockSpec(memory_space=pltpu.VMEM)
    dma = pltpu.SemaphoreType.DMA
    wide = pltpu.VMEM((tokens, width), BF16)
    spread = pltpu.VMEM((NX, nh, rows, DH), F32)
    eight = pltpu.VMEM((nh, NX, rows, DH), F32)
    four = pltpu.VMEM((4, nh, rows, DH), F32)
    one = pltpu.VMEM((nh, rows, DH), F32)
    square = pltpu.VMEM((nh, DH, DH), F32)
    tall = pltpu.VMEM((nh, tokens, DH), F32)
    few = pltpu.VMEM((3, NX, pl.next_power_of_2(nh), DH), F32)
    line = pltpu.VMEM((nz, pl.next_power_of_2(nh), DH), F32)
    retained, final = pl.pallas_call(
        functools.partial(kernel, table, nz),
        out_shape=(pltpu.VMEM((tokens, width), BF16), pltpu.VMEM((nh, 1, DH), F32)),
        in_specs=[anyspace] * 5,
        out_specs=(vmem, vmem),
        scratch_shapes=[
            wide, wide, wide, wide, pltpu.VMEM((width,), F32),
            square, spread, spread, eight, one, four, one, four, eight, eight, square, tall, tall, line, line,
            pltpu.VMEM((2, NX, pl.next_power_of_2(nh), DH), F32), few, spread, eight,
            dma((nh,)), dma((3,)), dma, dma, dma, dma, dma((nh,)), dma, dma, dma,
            pltpu.SemaphoreType.REGULAR((6,)), pltpu.SemaphoreType.REGULAR((NX,)),
            pltpu.SemaphoreType.REGULAR,
        ],
        compiler_params=pltpu.CompilerParams(collective_id=0, has_side_effects=True),
        name="retention",
    )(queries, key_rows, value_rows, gate_input, norm_gain)
    retained, final = (pltpu.with_memory_space_constraint(a, pltpu.VMEM) for a in (retained, final))
    retained, final = pl.pallas_call(
        put,
        out_shape=(jax.ShapeDtypeStruct((tokens, width), BF16), jax.ShapeDtypeStruct((nh, 1, DH), F32)),
        in_specs=[vmem, vmem],
        out_specs=(anyspace, anyspace),
        scratch_shapes=[dma((2,))],
        name="put",
    )(retained, final)
    return retained, final.reshape(1, nh, DH)


def solution(mesh):
    table = log_decays(mesh.shape["head"])
    rows = ("grp", "seq")
    placed = (P(rows, "head"),) * 4 + (P("head"),)
    return jax.shard_map(
        functools.partial(body, table, mesh.shape["seq"] // NX),
        mesh=mesh,
        in_specs=placed,
        out_specs=(P(rows, "head"), P(rows, "head", None)),
        check_vma=False,
    )
```
